32 devices in a mesh: gx: 2 (over core), gy: 4 (over y, x), gz: 4 (over z).
Axes of the slice: x: 2, y: 2, z: 4, core: 2. Of those that a mesh axis runs over, the one named last changes fastest.
Arguments:
- sources: float32 [1, 32, 64, 512], P(None, 'gx', 'gy', 'gz'), may hold values from -6 to 6
- stiffness: float32 [32, 64, 512], P('gx', 'gy', 'gz'), may hold values from 0.5 to 2
- coarse_inverse: float32 [256, 256], P(('gx', 'gy', 'gz')), may hold values from -6 to 6
Outputs:
- pressure: float32 [1, 32, 64, 512], P(None, 'gx', 'gy', 'gz')
The draws below stay inside these ranges and needn't reach their ends.
All inputs are finite; a program needn't handle non-finite values.
Results may differ from the reference program's by a relative error of at most 0.0001.
Values sent between devices are 32-bit elements; how exact they have to be, the bound alone decides.
No kernel may reach another device: no remote copies, remote signals or barrier semaphores. Data moves between devices by JAX's collectives and lax.ppermute only.
A program may use at most 64 MiB of HBM per device.

```python
import math
import jax
import jax.numpy as jnp
from jax import lax

SYSTEMS = 1
CX = 16
CY = 16
CZ = 128
NX = 32
NY = 64
NZ = 512
NC = 256
N_GX = 2
N_GY = 4
N_GZ = 4


def level_of(own_key, shape, cuts, smallest, largest):
    loudness = 1.0
    for dim, shards_of in cuts:
        steps = jax.random.uniform(jax.random.fold_in(jax.random.fold_in(own_key, 6), dim), (shards_of,), jnp.float32, smallest / len(cuts), largest / len(cuts))
        loudness = loudness * jnp.repeat(jnp.exp(steps), shape[dim] // shards_of).reshape((-1,) + (1,) * (len(shape) - 1 - dim))
    return loudness


def centred(own_key, extent, deviation, most, pieces=(), kind=jnp.bfloat16):
    loudness = level_of(own_key, extent, pieces, -0.22, 0.18) if pieces else 1.0
    values = jax.random.normal(own_key, extent, jnp.float32) * deviation * loudness
    return jnp.minimum(jnp.maximum(values, -most), most).astype(kind)


def setup_inputs(seed: int = 0) -> dict:
    splits = jax.random.split(jax.random.key(seed), 4)
    sources = centred(splits[0], (SYSTEMS, NX, NY, NZ), 1.0, 6.0, ((1, 2), (2, 4), (3, 4)), jnp.float32)
    stiffness = jnp.clip(jnp.exp(math.log(2.0) - 1.3862944 * jax.random.uniform(splits[1], (NX, NY, NZ), jnp.float32) ** level_of(splits[1], (NX, NY, NZ), ((0, 2), (1, 4), (2, 4)), -0.2, 0.2)), 0.5, 2.0)
    coarse_inverse = centred(splits[2], (NC, NC), (max(NC // 400, 1)) ** -0.5, 6.0, ((0, 32),), jnp.float32)
    return {"sources": sources, "stiffness": stiffness, "coarse_inverse": coarse_inverse}


damping = 0.8


def loop_sum(padded):
    total = padded[:, 2:, 1:-1, 1:-1] + padded[:, :-2, 1:-1, 1:-1]
    total = total + padded[:, 1:-1, 2:, 1:-1] + padded[:, 1:-1, :-2, 1:-1]
    total = total + padded[:, 1:-1, 1:-1, 2:] + padded[:, 1:-1, 1:-1, :-2]
    return total


def apply_op(answer, weights):
    scaled = weights * answer
    padded = jnp.pad(scaled, ((0, 0), (1, 1), (1, 1), (1, 1)))
    return weights * (6.0 * scaled - loop_sum(padded))


def pre_smooth(source, weights):
    diagonal = 6.0 * weights * weights
    first = damping * source / diagonal
    second = first + damping * (source - apply_op(first, weights)) / diagonal
    return second, source - apply_op(second, weights)


def post_smooth(answer, source, weights):
    return answer + damping * (source - apply_op(answer, weights)) / (6.0 * weights * weights)


def coarsen(values):
    leading = values.shape[0]
    size_x, size_y, size_z = values.shape[1], values.shape[2], values.shape[3]
    blocks = values.reshape((leading, size_x // 2, 2, size_y // 2, 2, size_z // 2, 2))
    return jnp.mean(blocks, axis=(2, 4, 6))


def refine(values):
    return jnp.repeat(jnp.repeat(jnp.repeat(values, 2, axis=1), 2, axis=2), 2, axis=3)


def reference(sources, stiffness, coarse_inverse):
    weight_list = [stiffness[None]]
    for level in range(3):
        weight_list.append(0.5 * coarsen(weight_list[-1]))
    source_list = []
    answer_list = []
    current = sources
    for level in range(4):
        source_list.append(current)
        answer, resid = pre_smooth(current, weight_list[level])
        answer_list.append(answer)
        current = coarsen(resid)
    coarse_source = current
    block_x = CX // 16
    block_y = CY // 16
    block_z = CZ // 16
    ordered = coarse_source.reshape((SYSTEMS, N_GX, block_x, N_GY, block_y, N_GZ, block_z))
    ordered = ordered.transpose((0, 1, 3, 5, 2, 4, 6)).reshape((SYSTEMS, NC))
    solved = jnp.dot(ordered, coarse_inverse.T, precision=lax.Precision.HIGHEST, preferred_element_type=jnp.float32)
    solved = solved.reshape((SYSTEMS, N_GX, N_GY, N_GZ, block_x, block_y, block_z))
    correction = solved.transpose((0, 1, 4, 2, 5, 3, 6)).reshape(coarse_source.shape)
    for level in range(3, -1, -1):
        correction = post_smooth(answer_list[level] + refine(correction), source_list[level], weight_list[level])
    return correction
```

```python
import functools

import jax
import jax.numpy as jnp
from jax import lax
from jax.experimental import pallas as pl
from jax.experimental.pallas import tpu as pltpu
from jax.sharding import PartitionSpec as P

damping = 0.8
K = damping / 6.0
AXES = ("gx", "gy", "gz")
HALO = 8
F32 = jnp.float32


def swap(values, axis, first):
    count = lax.axis_size(axis)
    partner = list(range(count))
    for i in range(first, count - 1, 2):
        partner[i], partner[i + 1] = i + 1, i
    return lax.ppermute(values, axis, list(enumerate(partner)))


def iota(shape, dim):
    return lax.broadcasted_iota(jnp.int32, shape, dim)


def roll(values, amount):
    size = values.shape[-1]
    if isinstance(amount, int):
        amount = amount % size
        if amount == 0:
            return values
    return pltpu.roll(values, amount, values.ndim - 1)


def z_sum(main, side, step):
    lane = iota(main.shape, main.ndim - 1)
    size = main.shape[-1]
    main_up, side_up = roll(main, -step), roll(side, -step)
    main_dn, side_dn = roll(main, step), roll(side, step)
    last = lane >= size - step
    first = lane < step
    main_sum = jnp.where(last, side_up, main_up) + jnp.where(first, side_dn, main_dn)
    side_sum = jnp.where(last, main_up, side_up) + jnp.where(first, main_dn, side_dn)
    return main_sum, side_sum


def xy_sum(ref, x, row, rows):
    total = ref[x - 1, pl.ds(row, rows), :] + ref[x + 1, pl.ds(row, rows), :]
    return total + ref[x, pl.ds(row - 1, rows), :] + ref[x, pl.ds(row + 1, rows), :]


def neighbours(main_ref, side_ref, x, row, rows, step):
    main = main_ref[x, pl.ds(row, rows), :]
    side = side_ref[x, pl.ds(row, rows), :]
    main_z, side_z = z_sum(main, side, step)
    return main, side, xy_sum(main_ref, x, row, rows) + main_z, xy_sum(side_ref, x, row, rows) + side_z


def global_neighbours(ref, x, row, rows, step):
    main = ref[x, pl.ds(row, rows), :]
    lane = iota(main.shape, 1)
    size = main.shape[-1]
    up = jnp.where(lane >= size - step, 0.0, roll(main, -step))
    dn = jnp.where(lane < step, 0.0, roll(main, step))
    return main, xy_sum(ref, x, row, rows) + up + dn


def lane_pairs(values, step):
    lane = iota(values.shape, values.ndim - 1)
    return values + jnp.where((lane // step) % 2 == 0, roll(values, -step), roll(values, step))


def inverse(weights):
    return jnp.where(weights > 0.0, 1.0 / jnp.where(weights > 0.0, weights, 1.0), 0.0)


def tiled(value):
    return [value[:, t * 128 : (t + 1) * 128] for t in range(value.shape[1] // 128)]


def joined(parts):
    return parts[0] if len(parts) == 1 else jnp.concatenate(parts, axis=1)


def row_pairs(ref, rows):
    return joined([ref[t, pl.ds(0, rows // 2, stride=2), :] + ref[t, pl.ds(1, rows // 2, stride=2), :] for t in range(ref.shape[0])])


def each(count, body, width=1):
    while count % width:
        width -= 1
    if count == width:
        for i in range(count):
            body(i)
        return

    def step(i, carry):
        for j in range(width):
            body(i * width + j)
        return carry

    lax.fori_loop(0, count // width, step, 0)


def pair_places(axis, count, own, tall):
    index = lax.axis_index(axis)
    odd = index % 2
    first = dict(place=jnp.where(odd == 0, own + tall, 0), high=odd == 0, valid=jnp.where(odd == 0, index + 1, index - 1) < count)
    other = jnp.where(odd == 0, index - 1, index + 1)
    second = dict(place=jnp.where(odd == 0, 0, own + tall), high=odd == 1, valid=(other >= 0) & (other < count))
    return index, odd, (first, second)


def x_frame(count, tall):
    index = lax.axis_index("gx")
    odd = index % 2
    if count == 1:
        return index, 0, ()
    own = HALO * odd if count == 2 else HALO
    _, _, (first, second) = pair_places("gx", count, own, tall)
    if count == 2:
        first["source"] = jnp.where(odd == 0, 0, tall - HALO)
        return index, own, (first,)
    first["source"] = second["source"] = 0
    return index, own, (first, second)


def frame_extent(count, tall):
    return tall + (0 if count == 1 else HALO if count == 2 else 2 * HALO)


def keep(valid, values):
    return jnp.where(valid, values, jnp.zeros_like(values))


def y_pack_kernel(mesh_shape, *refs):
    n_gx, n_gy, n_gz = mesh_shape
    n_in = 3 * (1 + min(n_gx - 1, 2))
    own_refs, part_refs, outs = refs[:3], refs[3:n_in], refs[n_in:]
    tall, wide = own_refs[0].shape[0], own_refs[0].shape[1]
    extent = frame_extent(n_gx, tall)
    tiles = own_refs[2].shape[1] // 128
    _, own, parts = x_frame(n_gx, tall)
    odd = lax.axis_index("gy") % 2
    low = jnp.where(odd == 0, wide - HALO, 0)
    for out, start in zip(outs, (low, wide - HALO - low)):
        rows = pl.ds(pl.multiple_of(start, 8), HALO)
        for a in range(2):
            out[pl.ds(a * extent + own, tall)] = own_refs[a][:, rows, :]
            for part, ref in zip(parts, (part_refs[a : a + 1], part_refs[3 + a : 4 + a])):
                out[pl.ds(a * extent + part["place"], HALO)] = keep(part["valid"], ref[0][pl.ds(part["source"], HALO), rows, :])
        base = 2 * extent
        for side in (0, 2):
            for t in range(tiles):
                out[base + side * tiles + t] = jnp.zeros((HALO, 128), F32)
        for t in range(tiles):
            out[base + tiles + t] = own_refs[2][:, t * 128 : (t + 1) * 128]
            for part, ref in zip(parts, (part_refs[2:3], part_refs[5:6])):
                side = jnp.where(part["high"], 2, 0)
                out[base + side * tiles + t] = keep(part["valid"], ref[0][:, t * 128 : (t + 1) * 128])


def z_pack_kernel(mesh_shape, *refs):
    n_gx, n_gy, n_gz = mesh_shape
    n_in = 3 * (1 + min(n_gx - 1, 2))
    own_refs, part_refs = refs[:3], refs[3:n_in]
    y_refs = refs[n_in : n_in + 2]
    frames = refs[n_in + 2 : n_in + 4]
    rows_ref, z_outs = refs[n_in + 4], refs[n_in + 5 :]
    tall, wide = own_refs[0].shape[0], own_refs[0].shape[1]
    extent = frame_extent(n_gx, tall)
    tiles = own_refs[2].shape[1] // 128
    _, own, parts = x_frame(n_gx, tall)
    _, _, y_parts = pair_places("gy", n_gy, HALO, wide)
    for a in range(2):
        frames[a][pl.ds(own, tall), HALO : HALO + wide, :] = own_refs[a][...]
        for part, ref in zip(parts, (part_refs[a : a + 1], part_refs[3 + a : 4 + a])):
            frames[a][pl.ds(part["place"], HALO), HALO : HALO + wide, :] = keep(part["valid"], ref[0][pl.ds(part["source"], HALO)])
        for part, ref in zip(y_parts, y_refs):
            rows = pl.ds(pl.multiple_of(part["place"], 8), HALO)
            frames[a][:, rows, :] = keep(part["valid"], ref[a * extent : (a + 1) * extent])
    for t in range(tiles):
        for side in (0, 2):
            rows_ref[(side * 3 + 1) * tiles + t] = jnp.zeros((HALO, 128), F32)
        rows_ref[4 * tiles + t] = own_refs[2][:, t * 128 : (t + 1) * 128]
        for part, ref in zip(parts, (part_refs[2:3], part_refs[5:6])):
            side = jnp.where(part["high"], 2, 0)
            rows_ref[(side * 3 + 1) * tiles + t] = keep(part["valid"], ref[0][:, t * 128 : (t + 1) * 128])
        for x_side in range(3):
            for part, ref in zip(y_parts, y_refs):
                side = jnp.where(part["high"], 2, 0)
                rows_ref[(x_side * 3 + side) * tiles + t] = keep(part["valid"], ref[2 * extent + x_side * tiles + t])
    odd = lax.axis_index("gz") % 2
    groups = extent // HALO
    slot = iota((4 * HALO, 128), 1) // HALO
    for out, tail in zip(z_outs, (odd == 0, odd == 1)):
        bump = jnp.where(tail, HALO, 0)
        for group in range(groups):
            packed = jnp.zeros((4 * HALO, 128), F32)
            for i in range(HALO):
                for a in range(2):
                    piece = roll(frames[a][group * HALO + i], bump + (16 * i + 8 * a))
                    packed = jnp.where(slot == 2 * i + a, piece, packed)
            out[group] = packed
        row = jnp.where(tail, HALO - 1, 0)
        for s in range((tiles + 1) // 2):
            out[groups + s] = jnp.zeros((4 * HALO, 128), F32)
        for t in range(tiles):
            for m in range(9):
                out[groups + t // 2, 16 * (t % 2) + m : 16 * (t % 2) + m + 1, :] = rows_ref[m * tiles + t, pl.ds(row, 1), :]


def down_kernel(mesh_shape, *refs):
    n_gx, n_gy, n_gz = mesh_shape
    fb, fw, za, zb = refs[:4]
    send, v0w, w0w, v0h, w0h, g0, v1m, v1s, w1m, w1s, g1m, g1s = refs[4:16]
    gm, gs, vm, vs, ws, tm, ts, um, us, small = refs[16:]
    extent, rows = fb.shape[0], fb.shape[1]
    tall = g0.shape[0]
    wide = g0.shape[1]
    half, half_rows = extent // 2, rows // 2
    _, own, _ = x_frame(n_gx, tall)
    _, odd, z_parts = pair_places("gz", n_gz, 0, 120)
    groups = extent // HALO
    zero = jnp.zeros((8, 128), F32)

    def clear(ref, count, depth):
        for x in (0, count + 1):
            for r in range(0, depth + 16, 8):
                ref[x, r : r + 8, :] = zero
        for x in range(1, count + 1):
            ref[x, 0:8, :] = zero
            ref[x, depth + 8 : depth + 16, :] = zero

    for ref in (gm, gs, vm, vs):
        clear(ref, extent, rows)
    for ref in (v1m, v1s, g1m, g1s, w1m, w1s):
        clear(ref, half, half_rows)

    lane = iota((rows, 128), 1)
    low_lane, high_lane = lane >= 120, lane < 8
    part_mask, part_base = [], []
    for part in z_parts:
        part_mask.append(jnp.where(part["high"], high_lane.astype(F32), low_lane.astype(F32)) * part["valid"].astype(F32))
        part_base.append(jnp.where(part["high"], 0, 120))

    def load(group):
        for i in range(HALO):
            x = group * HALO + i
            sides = []
            for a in range(2):
                total = None
                for ref, mask, base in zip((za, zb), part_mask, part_base):
                    piece = roll(ref[group], lax.rem(base + (256 - 16 * i - 8 * a), 128)) * mask
                    total = piece if total is None else total + piece
                sides.append(total)
            ws[x] = sides[1]
            gm[x + 1, 8 : 8 + rows, :] = K * fb[x] * inverse(fw[x])
            gs[x + 1, 8 : 8 + rows, :] = K * sides[0] * inverse(sides[1])

    each(groups, load)

    def second(x):
        main, side, main_n, side_n = neighbours(gm, gs, x + 1, 8, rows, 1)
        vm[x + 1, 8 : 8 + rows, :] = 1.2 * main + jnp.where(fw[x] > 0.0, K * main_n, 0.0)
        vs[x + 1, 8 : 8 + rows, :] = 1.2 * side + jnp.where(ws[x] > 0.0, K * side_n, 0.0)

    each(extent, second, 2)

    def residual(x2):
        for j in range(2):
            x = 2 * x2 + j
            main, side, main_n, side_n = neighbours(vm, vs, x + 1, 8, rows, 1)
            w_main, w_side = fw[x], ws[x]
            r_main = w_main * ((1.0 / K) * gm[x + 1, 8 : 8 + rows, :] - 6.0 * main + main_n)
            r_side = w_side * ((1.0 / K) * gs[x + 1, 8 : 8 + rows, :] - 6.0 * side + side_n)
            if j == 0:
                tm[...], ts[...], um[...], us[...] = r_main, r_side, w_main, w_side
            else:
                tm[...] += r_main
                ts[...] += r_side
                um[...] += w_main
                us[...] += w_side

        def pairs(ref):
            return lane_pairs(ref[pl.ds(0, half_rows, stride=2), :] + ref[pl.ds(1, half_rows, stride=2), :], 1)

        for t_ref, u_ref, w_out, g_out in ((tm, um, w1m, g1m), (ts, us, w1s, g1s)):
            weights = 0.0625 * pairs(u_ref)
            w_out[x2 + 1, 8 : 8 + half_rows, :] = weights
            g_out[x2 + 1, 8 : 8 + half_rows, :] = (0.125 * K) * pairs(t_ref) * inverse(weights)

    each(half, residual)

    def second_1(x):
        main, side, main_n, side_n = neighbours(g1m, g1s, x + 1, 8, half_rows, 2)
        v1m[x + 1, 8 : 8 + half_rows, :] = 1.2 * main + jnp.where(w1m[x + 1, 8 : 8 + half_rows, :] > 0.0, K * main_n, 0.0)
        v1s[x + 1, 8 : 8 + half_rows, :] = 1.2 * side + jnp.where(w1s[x + 1, 8 : 8 + half_rows, :] > 0.0, K * side_n, 0.0)

    each(half, second_1, 2)

    base = own // 2
    first_row = 8 + HALO // 2
    quarter, quarter_rows = tall // 4, wide // 4
    for x2 in range(quarter):
        total_r = total_w = None
        for j in range(2):
            x = base + 2 * x2 + j + 1
            main, _, main_n, _ = neighbours(v1m, v1s, x, first_row, wide // 2, 2)
            weights = w1m[x, pl.ds(first_row, wide // 2), :]
            res = weights * ((1.0 / K) * g1m[x, pl.ds(first_row, wide // 2), :] - 6.0 * main + main_n)
            total_r = res if j == 0 else total_r + res
            total_w = weights if j == 0 else total_w + weights
        small[0, x2] = total_r
        small[1, x2] = total_w
    q = []
    for a, factor in ((0, 0.125), (1, 0.0625)):
        for x2 in range(quarter):
            ref = small.at[a, x2]
            both = ref[pl.ds(0, quarter_rows, stride=2), :] + ref[pl.ds(1, quarter_rows, stride=2), :]
            q.append(factor * lane_pairs(both, 2))
    stacked = jnp.concatenate([jnp.concatenate(q[:quarter], axis=0), jnp.concatenate(q[quarter:], axis=0)], axis=0)
    src, dst = iota((128, 128), 0), iota((128, 128), 1)
    pick = (src == 4 * (dst % 32)).astype(F32)
    compact = jnp.dot(stacked, pick, precision=lax.Precision.HIGHEST, preferred_element_type=F32)
    block = iota((quarter_rows, 128), 1) // 32
    gz = lax.axis_index("gz")
    out = []
    for a in range(2):
        packed = jnp.zeros((quarter_rows, 128), F32)
        for x2 in range(quarter):
            r = (a * quarter + x2) * quarter_rows
            packed = jnp.where(block == lax.rem(gz + x2, 4), compact[r : r + quarter_rows], packed)
        out.append(packed)
    message = jnp.concatenate(out, axis=0)

    def copy(d):
        send[d] = message

    each(send.shape[0], copy, 8)

    for i in range(tall + 2):
        v0w[i] = vm[own + i, 8 : 8 + rows, :]
        x = own + (i - 1)
        inside = (x >= 0) & (x < extent)
        w0w[i] = keep(inside, fw[jnp.clip(x, 0, extent - 1)])
    for i in range(tall):
        v0h[i] = vs[own + i + 1, 8 + HALO : 8 + HALO + wide, :]
        w0h[i] = ws[own + i, HALO : HALO + wide, :]
        g0[i] = gm[own + i + 1, 8 + HALO : 8 + HALO + wide, :]


def up_kernel(mesh_shape, *refs):
    n_gx, n_gy, n_gz = mesh_shape
    recv, rows_ref, za, zb, v0w, w0w, v0h, w0h, g0, v1m, v1s, w1m, w1s, g1m, g1s, out = refs[:16]
    g2, w2, v2, y2, e2, p2, t3, u3, g3, w3, v3, y3, p3, b4, col, y1m, y1s, e1m, e1s, f1m, f1s, y0m, y0s = refs[16:]
    tall, wide = out.shape[0], out.shape[1]
    size_x, size_z = w2.shape[0], w2.shape[2]
    size_y = w2.shape[1]
    ix, own, _ = x_frame(n_gx, tall)
    iy, iz = lax.axis_index("gy"), lax.axis_index("gz")
    quarter, quarter_rows = tall // 4, wide // 4
    extent = frame_extent(n_gx, tall)
    half, half_rows = v1m.shape[0] - 2, v1m.shape[1] - 16

    def clear(ref):
        count, depth, size = ref.shape
        zero = jnp.zeros((8, size), F32)
        for x in range(count):
            for r in range(0, depth, 8):
                if x in (0, count - 1) or r in (0, depth - 8):
                    ref[x, r : r + 8, :] = zero

    for ref in (g2, v2, y2, g3, v3, y3):
        clear(ref)
    e2[...] = jnp.zeros(e2.shape, F32)
    p3[...] = jnp.zeros(p3.shape, F32)

    lane = iota((quarter_rows, 128), 1)
    block = lane // 32
    for gx in range(n_gx):
        for gy in range(n_gy):
            for x in range(quarter):
                tiles_b, tiles_w = [], []
                for tile in range(size_z // 128):
                    picked = [jnp.zeros((quarter_rows, 128), F32)] * 2
                    for j in range(4):
                        gz = tile * 4 + j
                        d = (gx * n_gy + gy) * n_gz + gz
                        mask = block == (gz + x) % 4
                        for a in range(2):
                            piece = recv[d, a * quarter_rows : (a + 1) * quarter_rows, :]
                            picked[a] = jnp.where(mask, piece, picked[a])
                    tiles_b.append(roll(picked[0], -32 * x))
                    tiles_w.append(roll(picked[1], -32 * x))
                weights = joined(tiles_w)
                w2[gx * quarter + x, gy * quarter_rows : (gy + 1) * quarter_rows, :] = weights
                g2[gx * quarter + x + 1, 8 + gy * quarter_rows : 8 + (gy + 1) * quarter_rows, :] = K * joined(tiles_b) / weights

    def smooth(g, v, x, rows, step):
        main, near = global_neighbours(g, x + 1, 8, rows, step)
        v[x + 1, 8 : 8 + rows, :] = 1.2 * main + K * near

    def resid(g, v, w, x, rows, step):
        main, near = global_neighbours(v, x + 1, 8, rows, step)
        return w[x] * ((1.0 / K) * g[x + 1, 8 : 8 + rows, :] - 6.0 * main + near)

    each(size_x, lambda x: smooth(g2, v2, x, size_y, 1), 8)
    rows3, x3 = size_y // 2, size_x // 2

    def restrict_2(x):
        for t, part in enumerate(tiled(resid(g2, v2, w2, 2 * x, size_y, 1) + resid(g2, v2, w2, 2 * x + 1, size_y, 1))):
            t3[t] = part
        for t, part in enumerate(tiled(w2[2 * x] + w2[2 * x + 1])):
            u3[t] = part
        pairs = lambda ref: lane_pairs(row_pairs(ref, size_y), 1)
        weights = 0.0625 * pairs(u3)
        w3[x] = weights
        g3[x + 1, 8 : 8 + rows3, :] = (0.125 * K) * pairs(t3) / weights

    each(x3, restrict_2, 4)
    each(x3, lambda x: smooth(g3, v3, x, rows3, 2), 8)
    rows4, x4 = rows3 // 2, x3 // 2

    def restrict_3(x):
        for t, part in enumerate(tiled(resid(g3, v3, w3, 2 * x, rows3, 2) + resid(g3, v3, w3, 2 * x + 1, rows3, 2))):
            t3[t, 0:rows3, :] = part
        b4[x] = 0.125 * lane_pairs(row_pairs(t3, rows3), 2)

    each(x4, restrict_3, 4)

    tiles = rows_ref.shape[0] // 9
    coarse_z = size_z // 4
    per = 128 // coarse_z
    src, dst = iota((size_z, 128), 0), iota((size_z, 128), 1)
    pick = (src == 4 * (dst % coarse_z)).astype(F32)
    values = b4[0] if x4 == 1 else jnp.concatenate([b4[x] for x in range(x4)], axis=0)
    compact = jnp.dot(values, pick, precision=lax.Precision.HIGHEST, preferred_element_type=F32)
    place = iota((x4 * rows4, 128), 0) % per == iota((x4 * rows4, 128), 1) // coarse_z
    compact = jnp.where(place, compact, 0.0)
    vectors = [jnp.sum(compact[t * per : (t + 1) * per], axis=0, keepdims=True) for t in range(tiles)]
    _, _, z_parts = pair_places("gz", n_gz, 0, 120)
    groups = extent // HALO
    fine = iota((HALO, size_z), 1) // 4
    fine_row = fine == iz * HALO + iota((HALO, size_z), 0)
    edge_row = iota((16, 128), 0)
    first_total = [None, None]
    for k, ref in enumerate((za, zb)):
        total = None
        for t in range(tiles):
            piece = ref[groups + t // 2, 16 * (t % 2) : 16 * (t % 2) + 16, :] * vectors[t]
            total = piece if total is None else total + piece
        first_total[k] = jnp.sum(total, axis=1, keepdims=True) * z_parts[k]["valid"].astype(F32)
    z_lane = iota((16, size_z), 1) // 4
    spread = None
    for k in range(2):
        where = jnp.where(z_parts[k]["high"], iz * HALO + HALO, iz * HALO - 1)
        piece = jnp.where(z_lane == where, first_total[k], 0.0)
        spread = piece if spread is None else spread + piece
    for m in range(9):
        total = None
        for t in range(tiles):
            piece = rows_ref[m * tiles + t] * vectors[t]
            total = piece if total is None else total + piece
        values = jnp.sum(total, axis=1, keepdims=True)
        line = jnp.sum(jnp.where(fine_row, values, 0.0), axis=0, keepdims=True) + spread[m : m + 1, :]
        row = 8 + 2 * (iy + (m % 3 - 1))
        for t, part in enumerate(tiled(line)):
            p3[ix + m // 3, t, pl.ds(row, 1), :] = part
            p3[ix + m // 3, t, pl.ds(row + 1, 1), :] = part

    def lift(y, v, w, p, x, px, rows, row):
        coarse = joined([p[px, t, row : row + rows, :] for t in range(p.shape[1])])
        y[x + 1, 8 : 8 + rows, :] = v[x + 1, 8 : 8 + rows, :] + w[x] * coarse

    def relax(y, g, w, x, rows, step):
        main, near = global_neighbours(y, x + 1, 8, rows, step)
        return (0.2 * main + g[x + 1, 8 : 8 + rows, :] + K * near) / w[x]

    each(x3, lambda x: lift(y3, v3, w3, p3, x, x // 2 + 1, rows3, 8), 8)

    def up_3(x):
        for t, e3 in enumerate(tiled(relax(y3, g3, w3, x, rows3, 2))):
            p2[x, t, pl.ds(0, rows3, stride=2), :] = e3
            p2[x, t, pl.ds(1, rows3, stride=2), :] = e3

    each(x3, up_3, 4)
    each(size_x, lambda x: lift(y2, v2, w2, p2, x, x // 2, size_y, 0), 8)

    def up_2(x):
        for t, part in enumerate(tiled(relax(y2, g2, w2, x, size_y, 1))):
            e2[x + 2, t, 8 : 8 + size_y, :] = part

    each(size_x, up_2, 8)

    src, dst = iota((size_z, 256), 0), iota((size_z, 256), 1)
    start = iz * 32
    cell = jnp.where(dst < 128, dst // 4, jnp.where(dst < 192, 32 + (dst - 128) // 4, -1 - (255 - dst) // 4))
    widen = (src == start + cell).astype(F32)
    n2 = extent // 4
    x_start = ix * quarter - own // 4
    y_start = 8 + iy * quarter_rows - HALO // 4
    spread = None
    for t in range(size_z // 128):
        stacked = jnp.concatenate([e2[x_start + 2 + i, t, pl.ds(y_start, 8), :] for i in range(n2)], axis=0)
        part = jnp.dot(stacked, widen[t * 128 : (t + 1) * 128], precision=lax.Precision.HIGHEST, preferred_element_type=F32)
        spread = part if spread is None else spread + part
    for i in range(n2):
        for ref, part in ((e1m, spread[i * 8 : i * 8 + 8, :128]), (e1s, spread[i * 8 : i * 8 + 8, 128:])):
            ref[i, pl.ds(0, 8, stride=2), :] = part
            ref[i, pl.ds(1, 8, stride=2), :] = part

    clear(y1m)
    clear(y1s)
    inner = slice(8, 8 + half_rows)
    for x in range(half):
        y1m[x + 1, inner, :] = v1m[x + 1, inner, :] + w1m[x + 1, inner, :] * e1m[x // 2]
        y1s[x + 1, inner, :] = v1s[x + 1, inner, :] + w1s[x + 1, inner, :] * e1s[x // 2]

    def up_1(x):
        main, side, main_n, side_n = neighbours(y1m, y1s, x + 1, 8, half_rows, 2)
        for f, y, near, g, w in ((f1m, main, main_n, g1m, w1m), (f1s, side, side_n, g1s, w1s)):
            e1 = (0.2 * y + g[x + 1, inner, :] + K * near) * inverse(w[x + 1, inner, :])
            f[x, pl.ds(0, half_rows, stride=2), :] = e1
            f[x, pl.ds(1, half_rows, stride=2), :] = e1

    each(half, up_1, 2)
    base = own // 2
    for i in range(tall + 2):
        parent = jnp.clip(base + (i + 1) // 2 - 1, 0, half - 1)
        y0m[i] = v0w[i] + w0w[i] * f1m[parent]
        if 0 < i <= tall:
            y0s[i - 1] = v0h[i - 1] + w0h[i - 1] * f1s[parent, HALO : HALO + wide, :]

    def up_0(i):
        main = y0m[i + 1, pl.ds(HALO, wide), :]
        main_z, _ = z_sum(main, y0s[i], 1)
        near = xy_sum(y0m, i + 1, HALO, wide) + main_z
        out[i] = (0.2 * main + g0[i] + K * near) / w0w[i + 1, HALO : HALO + wide, :]

    each(tall, up_0, 4)


def call(kernel, outs, scratch=()):
    shapes = [jax.ShapeDtypeStruct(s, F32) for s in outs]
    return pl.pallas_call(
        kernel,
        out_shape=shapes,
        scratch_shapes=[pltpu.VMEM(s, F32) for s in scratch],
        compiler_params=pltpu.CompilerParams(vmem_limit_bytes=56 * 1024 * 1024),
    )


def per_device(mesh_shape, sources, stiffness, coarse_inverse):
    n_gx, n_gy, n_gz = mesh_shape
    count = n_gx * n_gy * n_gz
    tall, wide, deep = stiffness.shape
    cells = coarse_inverse.shape[1]
    assert sources.shape[0] == 1 and deep == 128 and tall == 16 and wide == 16 and n_gz % 4 == 0 and cells % 128 == 0
    tiles = cells // 128
    extent = frame_extent(n_gx, tall)
    source = sources[0]
    own = (source, stiffness, coarse_inverse)
    parts = ()
    if n_gx == 2:
        parts = tuple(swap(a, "gx", 0) for a in own)
    elif n_gx > 2:
        odd = lax.axis_index("gx") % 2
        for first in range(2):
            start = jnp.where(odd == first, tall - HALO, 0)
            faces = [lax.dynamic_slice_in_dim(a, start, HALO, 0) for a in own[:2]] + [coarse_inverse]
            parts += tuple(swap(a, "gx", first) for a in faces)
    slab = (2 * extent + 3 * tiles, HALO, 128)
    y_slabs = call(functools.partial(y_pack_kernel, mesh_shape), [slab, slab])(*own, *parts)
    y_parts = [swap(s, "gy", first) for first, s in enumerate(y_slabs)]
    rows = wide + 2 * HALO
    z_slab = (extent // HALO + (tiles + 1) // 2, rows, 128)
    frame = (extent, rows, 128)
    fb, fw, matrix, z_a, z_b = call(
        functools.partial(z_pack_kernel, mesh_shape), [frame, frame, (9 * tiles, HALO, 128), z_slab, z_slab]
    )(*own, *parts, *y_parts)
    z_a, z_b = swap(z_a, "gz", 0), swap(z_b, "gz", 1)
    padded = (extent + 2, rows + 16, 128)
    half, half_rows = extent // 2, rows // 2
    level1 = (half + 2, half_rows + 16, 128)
    window, face = (tall + 2, rows, 128), (tall, wide, 128)
    message = (count, wide // 2, 128)
    outs = [message, window, window, face, face, face] + [level1] * 6
    scratch = [padded] * 4 + [frame] + [(rows, 128)] * 4 + [(2, tall // 4, wide // 2, 128)]
    send, *state = call(functools.partial(down_kernel, mesh_shape), outs, scratch)(fb, fw, z_a, z_b)
    recv = lax.all_to_all(send, AXES, 0, 0, tiled=True)
    size_x, size_y, size_z = n_gx * tall // 4, n_gy * wide // 4, n_gz * deep // 4
    pad2 = (size_x + 2, size_y + 16, size_z)
    x3, rows3 = size_x // 2, size_y // 2
    pad3 = (x3 + 2, rows3 + 16, size_z)
    n2, lane_tiles = extent // 4, size_z // 128
    scratch = [
        pad2, (size_x, size_y, size_z), pad2, pad2, (size_x + 4, lane_tiles, size_y + 16, 128), (x3, lane_tiles, size_y, 128),
        (lane_tiles, size_y, 128), (lane_tiles, size_y, 128), pad3, (x3, rows3, size_z), pad3, pad3,
        (x3 // 2 + 2, lane_tiles, rows3 + 16, 128),
        (x3 // 2, rows3 // 2, size_z), (8, 128), level1, level1, (n2, 16, 128), (n2, 16, 128),
        (half, rows, 128), (half, rows, 128), window, face,
    ]
    (pressure,) = call(functools.partial(up_kernel, mesh_shape), [face], scratch)(recv, matrix, z_a, z_b, *state)
    return pressure[None]


def solution(mesh):
    mesh_shape = tuple(mesh.shape[a] for a in AXES)
    in_specs = (P(None, "gx", "gy", "gz"), P("gx", "gy", "gz"), P(AXES, None))
    return jax.shard_map(
        functools.partial(per_device, mesh_shape),
        mesh=mesh,
        in_specs=in_specs,
        out_specs=P(None, "gx", "gy", "gz"),
        check_vma=False,
    )
```

```python
import functools
import math

import jax
import jax.numpy as jnp
from jax import lax
from jax.experimental import pallas as pl
from jax.experimental.pallas import tpu as pltpu
from jax.sharding import PartitionSpec as P

damping = 0.8
K = damping / 6.0
AXES = ("gx", "gy", "gz")
HALO = 8
F32 = jnp.float32


def swap(values, axis, first):
    count = lax.axis_size(axis)
    partner = list(range(count))
    for i in range(first, count - 1, 2):
        partner[i], partner[i + 1] = i + 1, i
    return lax.ppermute(values, axis, list(enumerate(partner)))


def iota(shape, dim):
    return lax.broadcasted_iota(jnp.int32, shape, dim)


def roll(values, amount):
    size = values.shape[-1]
    if isinstance(amount, int):
        amount = amount % size
        if amount == 0:
            return values
    return pltpu.roll(values, amount, values.ndim - 1)


def z_sum(main, side, step):
    lane = iota(main.shape, main.ndim - 1)
    size = main.shape[-1]
    main_up, side_up = roll(main, -step), roll(side, -step)
    main_dn, side_dn = roll(main, step), roll(side, step)
    last = lane >= size - step
    first = lane < step
    main_sum = jnp.where(last, side_up, main_up) + jnp.where(first, side_dn, main_dn)
    side_sum = jnp.where(last, main_up, side_up) + jnp.where(first, main_dn, side_dn)
    return main_sum, side_sum


def xy_sum(ref, x, row, rows):
    total = ref[x - 1, pl.ds(row, rows), :] + ref[x + 1, pl.ds(row, rows), :]
    return total + ref[x, pl.ds(row - 1, rows), :] + ref[x, pl.ds(row + 1, rows), :]


def neighbours(main_ref, side_ref, x, row, rows, step):
    main = main_ref[x, pl.ds(row, rows), :]
    side = side_ref[x, pl.ds(row, rows), :]
    main_z, side_z = z_sum(main, side, step)
    return main, side, xy_sum(main_ref, x, row, rows) + main_z, xy_sum(side_ref, x, row, rows) + side_z


def global_neighbours(ref, x, row, rows, step):
    main = ref[x, pl.ds(row, rows), :]
    lane = iota(main.shape, 1)
    size = main.shape[-1]
    up = jnp.where(lane >= size - step, 0.0, roll(main, -step))
    dn = jnp.where(lane < step, 0.0, roll(main, step))
    return main, xy_sum(ref, x, row, rows) + up + dn


def lane_pairs(values, step):
    lane = iota(values.shape, values.ndim - 1)
    return values + jnp.where((lane // step) % 2 == 0, roll(values, -step), roll(values, step))


def inverse(weights):
    return jnp.where(weights > 0.0, 1.0 / jnp.where(weights > 0.0, weights, 1.0), 0.0)


def tiled(value):
    return [value[:, t * 128 : (t + 1) * 128] for t in range(value.shape[1] // 128)]


def joined(parts):
    return parts[0] if len(parts) == 1 else jnp.concatenate(parts, axis=1)


def row_pairs(ref, rows):
    return joined([ref[t, pl.ds(0, rows // 2, stride=2), :] + ref[t, pl.ds(1, rows // 2, stride=2), :] for t in range(ref.shape[0])])


def each(count, body, width=1):
    while count % width:
        width -= 1
    if count == width:
        for i in range(count):
            body(i)
        return

    def step(i, carry):
        for j in range(width):
            body(i * width + j)
        return carry

    lax.fori_loop(0, count // width, step, 0)


def pair_places(axis, count, own, tall):
    index = lax.axis_index(axis)
    odd = index % 2
    first = dict(place=jnp.where(odd == 0, own + tall, 0), high=odd == 0, valid=jnp.where(odd == 0, index + 1, index - 1) < count)
    other = jnp.where(odd == 0, index - 1, index + 1)
    second = dict(place=jnp.where(odd == 0, 0, own + tall), high=odd == 1, valid=(other >= 0) & (other < count))
    return index, odd, (first, second)


def x_frame(count, tall):
    index = lax.axis_index("gx")
    odd = index % 2
    if count == 1:
        return index, 0, ()
    own = HALO * odd if count == 2 else HALO
    _, _, (first, second) = pair_places("gx", count, own, tall)
    if count == 2:
        first["source"] = jnp.where(odd == 0, 0, tall - HALO)
        return index, own, (first,)
    first["source"] = second["source"] = 0
    return index, own, (first, second)


def frame_extent(count, tall):
    return tall + (0 if count == 1 else HALO if count == 2 else 2 * HALO)


def keep(valid, values):
    return jnp.where(valid, values, jnp.zeros_like(values))


def y_pack_kernel(mesh_shape, *refs):
    n_gx, n_gy, n_gz = mesh_shape
    n_in = 3 * (1 + min(n_gx - 1, 2))
    own_refs, part_refs, outs = refs[:3], refs[3:n_in], refs[n_in:]
    tall, wide = own_refs[0].shape[0], own_refs[0].shape[1]
    extent = frame_extent(n_gx, tall)
    tiles = own_refs[2].shape[1] // 128
    _, own, parts = x_frame(n_gx, tall)
    odd = lax.axis_index("gy") % 2
    low = jnp.where(odd == 0, wide - HALO, 0)
    for out, start in zip(outs, (low, wide - HALO - low)):
        rows = pl.ds(pl.multiple_of(start, 8), HALO)
        for a in range(2):
            out[pl.ds(a * extent + own, tall)] = own_refs[a][:, rows, :]
            for part, ref in zip(parts, (part_refs[a : a + 1], part_refs[3 + a : 4 + a])):
                out[pl.ds(a * extent + part["place"], HALO)] = keep(part["valid"], ref[0][pl.ds(part["source"], HALO), rows, :])
        base = 2 * extent
        for side in (0, 2):
            for t in range(tiles):
                out[base + side * tiles + t] = jnp.zeros((HALO, 128), F32)
        for t in range(tiles):
            out[base + tiles + t] = own_refs[2][:, t * 128 : (t + 1) * 128]
            for part, ref in zip(parts, (part_refs[2:3], part_refs[5:6])):
                side = jnp.where(part["high"], 2, 0)
                out[base + side * tiles + t] = keep(part["valid"], ref[0][:, t * 128 : (t + 1) * 128])


def z_pack_kernel(mesh_shape, *refs):
    n_gx, n_gy, n_gz = mesh_shape
    n_in = 3 * (1 + min(n_gx - 1, 2))
    own_refs, part_refs = refs[:3], refs[3:n_in]
    y_refs = refs[n_in : n_in + 2]
    frames = refs[n_in + 2 : n_in + 4]
    rows_ref, z_outs = refs[n_in + 4], refs[n_in + 5 :]
    tall, wide = own_refs[0].shape[0], own_refs[0].shape[1]
    extent = frame_extent(n_gx, tall)
    tiles = own_refs[2].shape[1] // 128
    _, own, parts = x_frame(n_gx, tall)
    _, _, y_parts = pair_places("gy", n_gy, HALO, wide)
    for a in range(2):
        frames[a][pl.ds(own, tall), HALO : HALO + wide, :] = own_refs[a][...]
        for part, ref in zip(parts, (part_refs[a : a + 1], part_refs[3 + a : 4 + a])):
            frames[a][pl.ds(part["place"], HALO), HALO : HALO + wide, :] = keep(part["valid"], ref[0][pl.ds(part["source"], HALO)])
        for part, ref in zip(y_parts, y_refs):
            rows = pl.ds(pl.multiple_of(part["place"], 8), HALO)
            frames[a][:, rows, :] = keep(part["valid"], ref[a * extent : (a + 1) * extent])
    for t in range(tiles):
        for side in (0, 2):
            rows_ref[(side * 3 + 1) * tiles + t] = jnp.zeros((HALO, 128), F32)
        rows_ref[4 * tiles + t] = own_refs[2][:, t * 128 : (t + 1) * 128]
        for part, ref in zip(parts, (part_refs[2:3], part_refs[5:6])):
            side = jnp.where(part["high"], 2, 0)
            rows_ref[(side * 3 + 1) * tiles + t] = keep(part["valid"], ref[0][:, t * 128 : (t + 1) * 128])
        for x_side in range(3):
            for part, ref in zip(y_parts, y_refs):
                side = jnp.where(part["high"], 2, 0)
                rows_ref[(x_side * 3 + side) * tiles + t] = keep(part["valid"], ref[2 * extent + x_side * tiles + t])
    odd = lax.axis_index("gz") % 2
    groups = extent // HALO
    slot = iota((4 * HALO, 128), 1) // HALO
    for out, tail in zip(z_outs, (odd == 0, odd == 1)):
        bump = jnp.where(tail, HALO, 0)
        for group in range(groups):
            packed = jnp.zeros((4 * HALO, 128), F32)
            for i in range(HALO):
                for a in range(2):
                    piece = roll(frames[a][group * HALO + i], bump + (16 * i + 8 * a))
                    packed = jnp.where(slot == 2 * i + a, piece, packed)
            out[group] = packed
        row = jnp.where(tail, HALO - 1, 0)
        for s in range((tiles + 1) // 2):
            out[groups + s] = jnp.zeros((4 * HALO, 128), F32)
        for t in range(tiles):
            for m in range(9):
                out[groups + t // 2, 16 * (t % 2) + m : 16 * (t % 2) + m + 1, :] = rows_ref[m * tiles + t, pl.ds(row, 1), :]


def side_places(axis, count, own, side):
    index = lax.axis_index(axis)
    high = index % 2 == side
    other = jnp.where(high, index + 1, index - 1)
    return high, (other >= 0) & (other < count)


def faces_kernel(*refs):
    b, w, matrix, mine, theirs = refs
    tall, wide = b.shape[0], b.shape[1]
    tiles = matrix.shape[1] // 128
    strips = (tiles + 7) // 8
    groups = tall // HALO
    ix = lax.axis_index("gx")
    y_odd, z_odd = lax.axis_index("gy") % 2, lax.axis_index("gz") % 2
    slot = iota((wide, 128), 1) // HALO
    z_tail = (z_odd == 0, z_odd == 1)
    packed = []
    for tail in z_tail:
        bump = jnp.where(tail, HALO, 0)
        for group in range(groups):
            total = jnp.zeros((wide, 128), F32)
            for i in range(HALO):
                for a, ref in enumerate((b, w)):
                    piece = roll(ref[group * HALO + i], bump + (16 * i + 8 * a))
                    total = jnp.where(slot == 2 * i + a, piece, total)
            packed.append(total)
    for out, side in ((mine, ix), (theirs, 1 - ix)):
        y_high = y_odd == side
        rows = pl.ds(pl.multiple_of(jnp.where(y_high, wide - HALO, 0), 8), HALO)
        for a, ref in enumerate((b, w)):
            out[a * tall : (a + 1) * tall] = ref[:, rows, :]
        at = 2 * tall
        for t in range(tiles):
            out[at + t] = matrix[:, t * 128 : (t + 1) * 128]
        at += tiles

        def put_rows(at, tail):
            line = jnp.where(tail, matrix[HALO - 1 : HALO, :], matrix[0:1, :])
            for strip in range(strips):
                out[at + strip] = jnp.zeros((8, 128), F32)
            for t in range(tiles):
                out[at + t // 8, t % 8 : t % 8 + 1, :] = line[:, t * 128 : (t + 1) * 128]

        for group in range(groups):
            chosen = jnp.where(side == 0, packed[group], packed[groups + group])
            for r in range(wide // 8):
                out[at + r] = chosen[8 * r : 8 * r + 8]
            at += wide // 8
        put_rows(at, z_odd == side)
        at += strips
        for k in range(2):
            for group in range(groups):
                whole = packed[k * groups + group]
                out[at] = jnp.where(y_high, whole[wide - HALO :], whole[:HALO])
                at += 1
            put_rows(at, z_tail[k])
            at += strips


def face_counts(tall, wide, tiles):
    strips, groups = (tiles + 7) // 8, tall // HALO
    corner = (groups, strips)
    return (2 * tall, tiles), (groups * wide // 8, strips), corner, corner


def join_kernel(counts, *refs):
    mine, theirs, outs = refs[0], refs[1], refs[2:]
    ix = lax.axis_index("gx")
    at = 0
    for i, (out, parts) in enumerate(zip(outs, counts)):
        base = 0
        split = (parts[0] // 2, parts[0] // 2, parts[1]) if i == 0 else parts
        for size in split:
            out[pl.ds(base + ix * size, size)] = mine[at : at + size]
            out[pl.ds(base + (1 - ix) * size, size)] = theirs[at : at + size]
            base += 2 * size
            at += size


def frame_kernel(mesh_shape, *refs):
    n_gx, n_gy, n_gz = mesh_shape
    own_refs, part_refs = refs[:3], refs[3:6]
    mine, theirs = refs[6:10], refs[10:14]
    frames, rows_ref, z_outs = refs[14:16], refs[16], refs[17:]
    tall, wide = own_refs[0].shape[0], own_refs[0].shape[1]
    extent = frame_extent(n_gx, tall)
    tiles = own_refs[2].shape[1] // 128
    strips, groups = (tiles + 7) // 8, extent // HALO
    ix, own, parts = x_frame(n_gx, tall)
    part = parts[0]
    first = ix == 0
    _, _, y_parts = pair_places("gy", n_gy, HALO, wide)
    skip = HALO * ix

    def sides(i, place):
        a, b = mine[i][place], theirs[i][place]
        return jnp.where(first, a, b), jnp.where(first, b, a)

    for a in range(2):
        frames[a][pl.ds(own, tall), HALO : HALO + wide, :] = own_refs[a][...]
        frames[a][pl.ds(part["place"], HALO), HALO : HALO + wide, :] = part_refs[a][pl.ds(part["source"], HALO)]
        for y_part, values in zip(y_parts, sides(0, pl.ds(a * 2 * tall + skip, extent))):
            frames[a][:, pl.ds(pl.multiple_of(y_part["place"], 8), HALO), :] = keep(y_part["valid"], values)
    for x_side in range(3):
        gx = ix + x_side - 1
        inside = (gx >= 0) & (gx < n_gx)
        gx = jnp.clip(gx, 0, n_gx - 1)
        for t in range(tiles):
            for y_part, values in zip(y_parts, sides(0, 4 * tall + gx * tiles + t)):
                side = jnp.where(y_part["high"], 2, 0)
                rows_ref[(x_side * 3 + side) * tiles + t] = keep(y_part["valid"] & inside, values)
            line = own_refs[2] if x_side == 1 else part_refs[2]
            rows_ref[(x_side * 3 + 1) * tiles + t] = keep(inside, line[:, t * 128 : (t + 1) * 128])
    n_groups = 2 * tall // HALO
    for k, out in enumerate(z_outs):
        for s in range((tiles + 1) // 2):
            out[groups + s] = jnp.zeros((4 * HALO, 128), F32)
        for group in range(groups):
            g = group + ix
            for r in range(wide // 8):
                out[group, HALO + 8 * r : HALO + 8 * r + 8, :] = sides(1, g * (wide // 8) + r)[k]
            for y_part, values in zip(y_parts, sides(2 + k, g)):
                out[group, pl.ds(pl.multiple_of(y_part["place"], 8), HALO), :] = keep(y_part["valid"], values)
        for x_side in range(3):
            gx = ix + x_side - 1
            inside = (gx >= 0) & (gx < n_gx)
            gx = jnp.clip(gx, 0, n_gx - 1)
            for strip in range(strips):
                middle = keep(inside, sides(1, n_groups * wide // 8 + gx * strips + strip)[k])
                edges = [keep(p["valid"] & inside, v) for p, v in zip(y_parts, sides(2 + k, n_groups + gx * strips + strip))]
                low = jnp.where(y_parts[0]["high"], edges[1], edges[0])
                high = jnp.where(y_parts[0]["high"], edges[0], edges[1])
                for j in range(min(8, tiles - 8 * strip)):
                    t = 8 * strip + j
                    for y_side, values in enumerate((low, middle, high)):
                        m = 16 * (t % 2) + x_side * 3 + y_side
                        out[groups + t // 2, m : m + 1, :] = values[j : j + 1]


def down_kernel(mesh_shape, *refs):
    n_gx, n_gy, n_gz = mesh_shape
    fb, fw, za, zb = refs[:4]
    send, v0w, w0w, v0h, w0h, g0, v1m, v1s, w1m, w1s, g1m, g1s = refs[4:16]
    gm, gs, vm, vs, ws, tm, ts, um, us, small = refs[16:]
    extent, rows = fb.shape[0], fb.shape[1]
    tall = g0.shape[0]
    wide = g0.shape[1]
    half, half_rows = extent // 2, rows // 2
    _, own, _ = x_frame(n_gx, tall)
    _, odd, z_parts = pair_places("gz", n_gz, 0, 120)
    groups = extent // HALO
    zero = jnp.zeros((8, 128), F32)

    def clear(ref, count, depth):
        for x in (0, count + 1):
            for r in range(0, depth + 16, 8):
                ref[x, r : r + 8, :] = zero
        for x in range(1, count + 1):
            ref[x, 0:8, :] = zero
            ref[x, depth + 8 : depth + 16, :] = zero

    for ref in (gm, gs, vm, vs):
        clear(ref, extent, rows)
    for ref in (v1m, v1s, g1m, g1s, w1m, w1s):
        clear(ref, half, half_rows)

    lane = iota((rows, 128), 1)
    low_lane, high_lane = lane >= 120, lane < 8
    part_mask, part_base = [], []
    for part in z_parts:
        part_mask.append(jnp.where(part["high"], high_lane.astype(F32), low_lane.astype(F32)) * part["valid"].astype(F32))
        part_base.append(jnp.where(part["high"], 0, 120))

    def load(group):
        for i in range(HALO):
            x = group * HALO + i
            sides = []
            for a in range(2):
                total = None
                for ref, mask, base in zip((za, zb), part_mask, part_base):
                    piece = roll(ref[group], lax.rem(base + (256 - 16 * i - 8 * a), 128)) * mask
                    total = piece if total is None else total + piece
                sides.append(total)
            ws[x] = sides[1]
            gm[x + 1, 8 : 8 + rows, :] = K * fb[x] * inverse(fw[x])
            gs[x + 1, 8 : 8 + rows, :] = K * sides[0] * inverse(sides[1])

    each(groups, load)

    def second(x):
        main, side, main_n, side_n = neighbours(gm, gs, x + 1, 8, rows, 1)
        vm[x + 1, 8 : 8 + rows, :] = 1.2 * main + jnp.where(fw[x] > 0.0, K * main_n, 0.0)
        vs[x + 1, 8 : 8 + rows, :] = 1.2 * side + jnp.where(ws[x] > 0.0, K * side_n, 0.0)

    each(extent, second, 2)

    def residual(x2):
        for j in range(2):
            x = 2 * x2 + j
            main, side, main_n, side_n = neighbours(vm, vs, x + 1, 8, rows, 1)
            w_main, w_side = fw[x], ws[x]
            r_main = w_main * ((1.0 / K) * gm[x + 1, 8 : 8 + rows, :] - 6.0 * main + main_n)
            r_side = w_side * ((1.0 / K) * gs[x + 1, 8 : 8 + rows, :] - 6.0 * side + side_n)
            if j == 0:
                tm[...], ts[...], um[...], us[...] = r_main, r_side, w_main, w_side
            else:
                tm[...] += r_main
                ts[...] += r_side
                um[...] += w_main
                us[...] += w_side

        def pairs(ref):
            return lane_pairs(ref[pl.ds(0, half_rows, stride=2), :] + ref[pl.ds(1, half_rows, stride=2), :], 1)

        for t_ref, u_ref, w_out, g_out in ((tm, um, w1m, g1m), (ts, us, w1s, g1s)):
            weights = 0.0625 * pairs(u_ref)
            w_out[x2 + 1, 8 : 8 + half_rows, :] = weights
            g_out[x2 + 1, 8 : 8 + half_rows, :] = (0.125 * K) * pairs(t_ref) * inverse(weights)

    each(half, residual)

    def second_1(x):
        main, side, main_n, side_n = neighbours(g1m, g1s, x + 1, 8, half_rows, 2)
        v1m[x + 1, 8 : 8 + half_rows, :] = 1.2 * main + jnp.where(w1m[x + 1, 8 : 8 + half_rows, :] > 0.0, K * main_n, 0.0)
        v1s[x + 1, 8 : 8 + half_rows, :] = 1.2 * side + jnp.where(w1s[x + 1, 8 : 8 + half_rows, :] > 0.0, K * side_n, 0.0)

    each(half, second_1, 2)

    base = own // 2
    first_row = 8 + HALO // 2
    quarter, quarter_rows = tall // 4, wide // 4
    for x2 in range(quarter):
        total_r = total_w = None
        for j in range(2):
            x = base + 2 * x2 + j + 1
            main, _, main_n, _ = neighbours(v1m, v1s, x, first_row, wide // 2, 2)
            weights = w1m[x, pl.ds(first_row, wide // 2), :]
            res = weights * ((1.0 / K) * g1m[x, pl.ds(first_row, wide // 2), :] - 6.0 * main + main_n)
            total_r = res if j == 0 else total_r + res
            total_w = weights if j == 0 else total_w + weights
        small[0, x2] = total_r
        small[1, x2] = total_w
    q = []
    for a, factor in ((0, 0.125), (1, 0.0625)):
        for x2 in range(quarter):
            ref = small.at[a, x2]
            both = ref[pl.ds(0, quarter_rows, stride=2), :] + ref[pl.ds(1, quarter_rows, stride=2), :]
            q.append(factor * lane_pairs(both, 2))
    stacked = jnp.concatenate([jnp.concatenate(q[:quarter], axis=0), jnp.concatenate(q[quarter:], axis=0)], axis=0)
    src, dst = iota((128, 128), 0), iota((128, 128), 1)
    pick = (src == 4 * (dst % 32)).astype(F32)
    compact = jnp.dot(stacked, pick, precision=lax.Precision.HIGHEST, preferred_element_type=F32)
    block = iota((quarter_rows, 128), 1) // 32
    gz = lax.axis_index("gz")
    out = []
    for a in range(2):
        packed = jnp.zeros((quarter_rows, 128), F32)
        for x2 in range(quarter):
            r = (a * quarter + x2) * quarter_rows
            packed = jnp.where(block == lax.rem(gz + x2, 4), compact[r : r + quarter_rows], packed)
        out.append(packed)
    message = jnp.concatenate(out, axis=0)

    def copy(d):
        send[d] = message

    each(send.shape[0], copy, 8)

    for i in range(tall + 2):
        v0w[i] = vm[own + i, 8 : 8 + rows, :]
        x = own + (i - 1)
        inside = (x >= 0) & (x < extent)
        w0w[i] = keep(inside, fw[jnp.clip(x, 0, extent - 1)])
    for i in range(tall):
        v0h[i] = vs[own + i + 1, 8 + HALO : 8 + HALO + wide, :]
        w0h[i] = ws[own + i, HALO : HALO + wide, :]
        g0[i] = gm[own + i + 1, 8 + HALO : 8 + HALO + wide, :]


def up_kernel(mesh_shape, *refs):
    n_gx, n_gy, n_gz = mesh_shape
    recv, rows_ref, za, zb, v0w, w0w, v0h, w0h, g0, v1m, v1s, w1m, w1s, g1m, g1s, out = refs[:16]
    g2, w2, v2, y2, e2, p2, t3, u3, g3, w3, v3, y3, p3, b4, col, y1m, y1s, e1m, e1s, f1m, f1s, y0m, y0s = refs[16:]
    tall, wide = out.shape[0], out.shape[1]
    size_x, size_z = w2.shape[0], w2.shape[2]
    size_y = w2.shape[1]
    ix, own, _ = x_frame(n_gx, tall)
    iy, iz = lax.axis_index("gy"), lax.axis_index("gz")
    quarter, quarter_rows = tall // 4, wide // 4
    extent = frame_extent(n_gx, tall)
    half, half_rows = v1m.shape[0] - 2, v1m.shape[1] - 16

    def clear(ref):
        count, depth, size = ref.shape
        zero = jnp.zeros((8, size), F32)
        for x in range(count):
            ref[x, 0:8, :] = zero
            ref[x, depth - 8 : depth, :] = zero
        for x in (0, count - 1):
            ref[x] = jnp.zeros((depth, size), F32)

    for ref in (g2, v2, y2, g3, v3, y3):
        clear(ref)
    e2[...] = jnp.zeros(e2.shape, F32)
    p3[...] = jnp.zeros(p3.shape, F32)

    lane = iota((quarter_rows, 128), 1)
    block = lane // 32
    for gx in range(n_gx):
        for gy in range(n_gy):
            for x in range(quarter):
                tiles_b, tiles_w = [], []
                for tile in range(size_z // 128):
                    picked = [jnp.zeros((quarter_rows, 128), F32)] * 2
                    for j in range(4):
                        gz = tile * 4 + j
                        d = (gx * n_gy + gy) * n_gz + gz
                        mask = block == (gz + x) % 4
                        for a in range(2):
                            piece = recv[d, a * quarter_rows : (a + 1) * quarter_rows, :]
                            picked[a] = jnp.where(mask, piece, picked[a])
                    tiles_b.append(roll(picked[0], -32 * x))
                    tiles_w.append(roll(picked[1], -32 * x))
                weights = joined(tiles_w)
                w2[gx * quarter + x, gy * quarter_rows : (gy + 1) * quarter_rows, :] = weights
                g2[gx * quarter + x + 1, 8 + gy * quarter_rows : 8 + (gy + 1) * quarter_rows, :] = K * joined(tiles_b) / weights

    def smooth(g, v, x, rows, step):
        main, near = global_neighbours(g, x + 1, 8, rows, step)
        v[x + 1, 8 : 8 + rows, :] = 1.2 * main + K * near

    def resid(g, v, w, x, rows, step):
        main, near = global_neighbours(v, x + 1, 8, rows, step)
        return w[x] * ((1.0 / K) * g[x + 1, 8 : 8 + rows, :] - 6.0 * main + near)

    each(size_x, lambda x: smooth(g2, v2, x, size_y, 1), 8)
    rows3, x3 = size_y // 2, size_x // 2

    def restrict_2(x):
        for t, part in enumerate(tiled(resid(g2, v2, w2, 2 * x, size_y, 1) + resid(g2, v2, w2, 2 * x + 1, size_y, 1))):
            t3[t] = part
        for t, part in enumerate(tiled(w2[2 * x] + w2[2 * x + 1])):
            u3[t] = part
        pairs = lambda ref: lane_pairs(row_pairs(ref, size_y), 1)
        weights = 0.0625 * pairs(u3)
        w3[x] = weights
        g3[x + 1, 8 : 8 + rows3, :] = (0.125 * K) * pairs(t3) / weights

    each(x3, restrict_2, 4)
    each(x3, lambda x: smooth(g3, v3, x, rows3, 2), 8)
    rows4, x4 = rows3 // 2, x3 // 2

    def restrict_3(x):
        for t, part in enumerate(tiled(resid(g3, v3, w3, 2 * x, rows3, 2) + resid(g3, v3, w3, 2 * x + 1, rows3, 2))):
            t3[t, 0:rows3, :] = part
        b4[x] = 0.125 * lane_pairs(row_pairs(t3, rows3), 2)

    each(x4, restrict_3, 4)

    tiles = rows_ref.shape[0] // 9
    coarse_z = size_z // 4
    per = 128 // coarse_z
    src, dst = iota((size_z, 128), 0), iota((size_z, 128), 1)
    pick = (src == 4 * (dst % coarse_z)).astype(F32)
    values = b4[0] if x4 == 1 else jnp.concatenate([b4[x] for x in range(x4)], axis=0)
    compact = jnp.dot(values, pick, precision=lax.Precision.HIGHEST, preferred_element_type=F32)
    place = iota((x4 * rows4, 128), 0) % per == iota((x4 * rows4, 128), 1) // coarse_z
    compact = jnp.where(place, compact, 0.0)
    vectors = [jnp.sum(compact[t * per : (t + 1) * per], axis=0, keepdims=True) for t in range(tiles)]
    _, _, z_parts = pair_places("gz", n_gz, 0, 120)
    groups = extent // HALO
    fine = iota((HALO, size_z), 1) // 4
    fine_row = fine == iz * HALO + iota((HALO, size_z), 0)
    edge_row = iota((16, 128), 0)
    first_total = [None, None]
    for k, ref in enumerate((za, zb)):
        total = None
        for t in range(tiles):
            piece = ref[groups + t // 2, 16 * (t % 2) : 16 * (t % 2) + 16, :] * vectors[t]
            total = piece if total is None else total + piece
        first_total[k] = jnp.sum(total, axis=1, keepdims=True) * z_parts[k]["valid"].astype(F32)
    z_lane = iota((16, size_z), 1) // 4
    spread = None
    for k in range(2):
        where = jnp.where(z_parts[k]["high"], iz * HALO + HALO, iz * HALO - 1)
        piece = jnp.where(z_lane == where, first_total[k], 0.0)
        spread = piece if spread is None else spread + piece
    for m in range(9):
        total = None
        for t in range(tiles):
            piece = rows_ref[m * tiles + t] * vectors[t]
            total = piece if total is None else total + piece
        values = jnp.sum(total, axis=1, keepdims=True)
        line = jnp.sum(jnp.where(fine_row, values, 0.0), axis=0, keepdims=True) + spread[m : m + 1, :]
        row = 8 + 2 * (iy + (m % 3 - 1))
        for t, part in enumerate(tiled(line)):
            p3[ix + m // 3, t, pl.ds(row, 1), :] = part
            p3[ix + m // 3, t, pl.ds(row + 1, 1), :] = part

    def lift(y, v, w, p, x, px, rows, row):
        coarse = joined([p[px, t, row : row + rows, :] for t in range(p.shape[1])])
        y[x + 1, 8 : 8 + rows, :] = v[x + 1, 8 : 8 + rows, :] + w[x] * coarse

    def relax(y, g, w, x, rows, step):
        main, near = global_neighbours(y, x + 1, 8, rows, step)
        return (0.2 * main + g[x + 1, 8 : 8 + rows, :] + K * near) / w[x]

    each(x3, lambda x: lift(y3, v3, w3, p3, x, x // 2 + 1, rows3, 8), 8)

    def up_3(x):
        for t, e3 in enumerate(tiled(relax(y3, g3, w3, x, rows3, 2))):
            p2[x, t, pl.ds(0, rows3, stride=2), :] = e3
            p2[x, t, pl.ds(1, rows3, stride=2), :] = e3

    each(x3, up_3, 4)
    each(size_x, lambda x: lift(y2, v2, w2, p2, x, x // 2, size_y, 0), 8)

    def up_2(x):
        for t, part in enumerate(tiled(relax(y2, g2, w2, x, size_y, 1))):
            e2[x + 2, t, 8 : 8 + size_y, :] = part

    each(size_x, up_2, 8)

    src, dst = iota((size_z, 256), 0), iota((size_z, 256), 1)
    start = iz * 32
    cell = jnp.where(dst < 128, dst // 4, jnp.where(dst < 192, 32 + (dst - 128) // 4, -1 - (255 - dst) // 4))
    widen = (src == start + cell).astype(F32)
    n2 = extent // 4
    x_start = ix * quarter - own // 4
    y_start = 8 + iy * quarter_rows - HALO // 4
    spread = None
    for t in range(size_z // 128):
        stacked = jnp.concatenate([e2[x_start + 2 + i, t, pl.ds(y_start, 8), :] for i in range(n2)], axis=0)
        part = jnp.dot(stacked, widen[t * 128 : (t + 1) * 128], precision=lax.Precision.HIGHEST, preferred_element_type=F32)
        spread = part if spread is None else spread + part
    for i in range(n2):
        for ref, part in ((e1m, spread[i * 8 : i * 8 + 8, :128]), (e1s, spread[i * 8 : i * 8 + 8, 128:])):
            ref[i, pl.ds(0, 8, stride=2), :] = part
            ref[i, pl.ds(1, 8, stride=2), :] = part

    clear(y1m)
    clear(y1s)
    inner = slice(8, 8 + half_rows)
    for x in range(half):
        y1m[x + 1, inner, :] = v1m[x + 1, inner, :] + w1m[x + 1, inner, :] * e1m[x // 2]
        y1s[x + 1, inner, :] = v1s[x + 1, inner, :] + w1s[x + 1, inner, :] * e1s[x // 2]

    def up_1(x):
        main, side, main_n, side_n = neighbours(y1m, y1s, x + 1, 8, half_rows, 2)
        for f, y, near, g, w in ((f1m, main, main_n, g1m, w1m), (f1s, side, side_n, g1s, w1s)):
            e1 = (0.2 * y + g[x + 1, inner, :] + K * near) * inverse(w[x + 1, inner, :])
            f[x, pl.ds(0, half_rows, stride=2), :] = e1
            f[x, pl.ds(1, half_rows, stride=2), :] = e1

    each(half, up_1, 2)
    base = own // 2
    for i in range(tall + 2):
        parent = jnp.clip(base + (i + 1) // 2 - 1, 0, half - 1)
        y0m[i] = v0w[i] + w0w[i] * f1m[parent]
        if 0 < i <= tall:
            y0s[i - 1] = v0h[i - 1] + w0h[i - 1] * f1s[parent, HALO : HALO + wide, :]

    def up_0(i):
        main = y0m[i + 1, pl.ds(HALO, wide), :]
        main_z, _ = z_sum(main, y0s[i], 1)
        near = xy_sum(y0m, i + 1, HALO, wide) + main_z
        out[i] = (0.2 * main + g0[i] + K * near) / w0w[i + 1, HALO : HALO + wide, :]

    each(tall, up_0, 4)


def size_of(shape):
    return 4 * math.prod(shape)


def call(kernel, outs, scratch=(), resident=True):
    limit = 8 * 2**20 + sum(map(size_of, scratch)) + sum(size_of(s) for s in outs if size_of(s) > 2**20)
    run = pl.pallas_call(
        kernel,
        out_shape=[(pltpu.VMEM if resident and size_of(s) <= 2**20 else jax.ShapeDtypeStruct)(s, F32) for s in outs],
        scratch_shapes=[pltpu.VMEM(s, F32) for s in scratch],
        compiler_params=pltpu.CompilerParams(vmem_limit_bytes=min(limit, 56 * 2**20)),
    )

    def place(value):
        return pltpu.with_memory_space_constraint(value, pltpu.VMEM) if size_of(value.shape) <= 2**20 else value

    return lambda *values: run(*map(place, values))


def plain_halo(mesh_shape, own, frames):
    n_gx = mesh_shape[0]
    tall = own[0].shape[0]
    extent, tiles = frames[0][0], own[2].shape[1] // 128
    parts = ()
    if n_gx > 1:
        odd = lax.axis_index("gx") % 2
        for first in range(2):
            start = jnp.where(odd == first, tall - HALO, 0)
            faces = [lax.dynamic_slice_in_dim(a, start, HALO, 0) for a in own[:2]] + [own[2]]
            parts += tuple(swap(a, "gx", first) for a in faces)
    slab = (2 * extent + 3 * tiles, HALO, 128)
    y_slabs = call(functools.partial(y_pack_kernel, mesh_shape), [slab, slab])(*own, *parts)
    y_parts = [swap(s, "gy", first) for first, s in enumerate(y_slabs)]
    fb, fw, matrix, z_a, z_b = call(functools.partial(z_pack_kernel, mesh_shape), frames)(*own, *parts, *y_parts)
    return fb, fw, matrix, swap(z_a, "gz", 0), swap(z_b, "gz", 1)


def pair(index, count, first):
    other = index + 1 if index % 2 == first else index - 1
    return other if 0 <= other < count else index


def shared_halo(mesh_shape, own, frames):
    n_gx, n_gy, n_gz = mesh_shape
    tall, wide = own[0].shape[:2]
    tiles = own[2].shape[1] // 128
    counts = face_counts(tall, wide, tiles)
    total = (sum(map(sum, counts)), HALO, 128)
    mine, theirs = call(faces_kernel, [total, total])(*own)
    theirs = swap(theirs, "gx", 0)
    messages = call(functools.partial(join_kernel, counts), [(2 * sum(c), HALO, 128) for c in counts])(mine, theirs)

    def send(message, y_side, z_side):
        links = []
        for x in range(n_gx):
            for y in range(n_gy):
                for z in range(n_gz):
                    y_to = y if y_side is None else pair(y, n_gy, x)
                    z_to = z if z_side is None else pair(z, n_gz, x if z_side < 0 else z_side)
                    links.append(((x * n_gy + y) * n_gz + z, (x * n_gy + y_to) * n_gz + z_to))
        return lax.ppermute(message, AXES, links)

    got = [send(m, *way) for m, way in zip(messages, ((0, None), (None, -1), (0, 0), (0, 1)))]
    parts = [swap(a, "gx", 0) for a in own]
    got = lax.optimization_barrier(got)
    others = [swap(m, "gx", 0) for m in got]
    return call(functools.partial(frame_kernel, mesh_shape), frames)(*own, *parts, *got, *others)


def per_device(mesh_shape, sources, stiffness, coarse_inverse):
    n_gx, n_gy, n_gz = mesh_shape
    count = n_gx * n_gy * n_gz
    tall, wide, deep = stiffness.shape
    cells = coarse_inverse.shape[1]
    assert sources.shape[0] == 1 and deep == 128 and tall == 16 and wide == 16 and n_gz % 4 == 0 and cells % 128 == 0
    tiles = cells // 128
    extent = frame_extent(n_gx, tall)
    source = sources[0]
    own = (source, stiffness, coarse_inverse)
    rows = wide + 2 * HALO
    frame = (extent, rows, 128)
    z_slab = (extent // HALO + (tiles + 1) // 2, rows, 128)
    frames = [frame, frame, (9 * tiles, HALO, 128), z_slab, z_slab]
    exchange = shared_halo if n_gx == 2 else plain_halo
    fb, fw, matrix, z_a, z_b = exchange(mesh_shape, own, frames)
    padded = (extent + 2, rows + 16, 128)
    half, half_rows = extent // 2, rows // 2
    level1 = (half + 2, half_rows + 16, 128)
    window, face = (tall + 2, rows, 128), (tall, wide, 128)
    message = (count, wide // 2, 128)
    outs = [message, window, window, face, face, face] + [level1] * 6
    scratch = [padded] * 4 + [frame] + [(rows, 128)] * 4 + [(2, tall // 4, wide // 2, 128)]
    send, *state = call(functools.partial(down_kernel, mesh_shape), outs, scratch)(fb, fw, z_a, z_b)
    recv = lax.all_to_all(send, AXES, 0, 0, tiled=True)
    size_x, size_y, size_z = n_gx * tall // 4, n_gy * wide // 4, n_gz * deep // 4
    pad2 = (size_x + 2, size_y + 16, size_z)
    x3, rows3 = size_x // 2, size_y // 2
    pad3 = (x3 + 2, rows3 + 16, size_z)
    n2, lane_tiles = extent // 4, size_z // 128
    scratch = [
        pad2, (size_x, size_y, size_z), pad2, pad2, (size_x + 4, lane_tiles, size_y + 16, 128), (x3, lane_tiles, size_y, 128),
        (lane_tiles, size_y, 128), (lane_tiles, size_y, 128), pad3, (x3, rows3, size_z), pad3, pad3,
        (x3 // 2 + 2, lane_tiles, rows3 + 16, 128),
        (x3 // 2, rows3 // 2, size_z), (8, 128), level1, level1, (n2, 16, 128), (n2, 16, 128),
        (half, rows, 128), (half, rows, 128), window, face,
    ]
    (pressure,) = call(functools.partial(up_kernel, mesh_shape), [face], scratch, False)(recv, matrix, z_a, z_b, *state)
    return pressure[None]


def solution(mesh):
    mesh_shape = tuple(mesh.shape[a] for a in AXES)
    in_specs = (P(None, "gx", "gy", "gz"), P("gx", "gy", "gz"), P(AXES, None))
    return jax.shard_map(
        functools.partial(per_device, mesh_shape),
        mesh=mesh,
        in_specs=in_specs,
        out_specs=P(None, "gx", "gy", "gz"),
        check_vma=False,
    )
```

```python
import functools
import math

import jax
import jax.numpy as jnp
from jax import lax
from jax.experimental import pallas as pl
from jax.experimental.pallas import tpu as pltpu
from jax.sharding import PartitionSpec as P

damping = 0.8
K = damping / 6.0
AXES = ("gx", "gy", "gz")
HALO = 8
F32 = jnp.float32


def swap(values, axis, first):
    count = lax.axis_size(axis)
    partner = list(range(count))
    for i in range(first, count - 1, 2):
        partner[i], partner[i + 1] = i + 1, i
    return lax.ppermute(values, axis, list(enumerate(partner)))


def iota(shape, dim):
    return lax.broadcasted_iota(jnp.int32, shape, dim)


def roll(values, amount):
    size = values.shape[-1]
    if isinstance(amount, int):
        amount = amount % size
        if amount == 0:
            return values
    return pltpu.roll(values, amount, values.ndim - 1)


def z_sum(main, side, step):
    lane = iota(main.shape, main.ndim - 1)
    size = main.shape[-1]
    main_up, side_up = roll(main, -step), roll(side, -step)
    main_dn, side_dn = roll(main, step), roll(side, step)
    last = lane >= size - step
    first = lane < step
    main_sum = jnp.where(last, side_up, main_up) + jnp.where(first, side_dn, main_dn)
    side_sum = jnp.where(last, main_up, side_up) + jnp.where(first, main_dn, side_dn)
    return main_sum, side_sum


def xy_sum(ref, x, row, rows):
    total = ref[x - 1, pl.ds(row, rows), :] + ref[x + 1, pl.ds(row, rows), :]
    return total + ref[x, pl.ds(row - 1, rows), :] + ref[x, pl.ds(row + 1, rows), :]


def neighbours(main_ref, side_ref, x, row, rows, step):
    main = main_ref[x, pl.ds(row, rows), :]
    side = side_ref[x, pl.ds(row, rows), :]
    main_z, side_z = z_sum(main, side, step)
    return main, side, xy_sum(main_ref, x, row, rows) + main_z, xy_sum(side_ref, x, row, rows) + side_z


def global_neighbours(ref, x, row, rows, step):
    main = ref[x, pl.ds(row, rows), :]
    lane = iota(main.shape, 1)
    size = main.shape[-1]
    up = jnp.where(lane >= size - step, 0.0, roll(main, -step))
    dn = jnp.where(lane < step, 0.0, roll(main, step))
    return main, xy_sum(ref, x, row, rows) + up + dn


def lane_pairs(values, step):
    lane = iota(values.shape, values.ndim - 1)
    return values + jnp.where((lane // step) % 2 == 0, roll(values, -step), roll(values, step))


def inverse(weights):
    return jnp.where(weights > 0.0, 1.0 / jnp.where(weights > 0.0, weights, 1.0), 0.0)


def tiled(value):
    return [value[:, t * 128 : (t + 1) * 128] for t in range(value.shape[1] // 128)]


def joined(parts):
    return parts[0] if len(parts) == 1 else jnp.concatenate(parts, axis=1)


def row_pairs(ref, rows):
    return joined([ref[t, pl.ds(0, rows // 2, stride=2), :] + ref[t, pl.ds(1, rows // 2, stride=2), :] for t in range(ref.shape[0])])


def each(count, body, width=1):
    while count % width:
        width -= 1
    if count == width:
        for i in range(count):
            body(i)
        return

    def step(i, carry):
        for j in range(width):
            body(i * width + j)
        return carry

    lax.fori_loop(0, count // width, step, 0)


def pair_places(axis, count, own, tall):
    index = lax.axis_index(axis)
    odd = index % 2
    first = dict(place=jnp.where(odd == 0, own + tall, 0), high=odd == 0, valid=jnp.where(odd == 0, index + 1, index - 1) < count)
    other = jnp.where(odd == 0, index - 1, index + 1)
    second = dict(place=jnp.where(odd == 0, 0, own + tall), high=odd == 1, valid=(other >= 0) & (other < count))
    return index, odd, (first, second)


def x_frame(count, tall):
    index = lax.axis_index("gx")
    odd = index % 2
    if count == 1:
        return index, 0, ()
    own = HALO * odd if count == 2 else HALO
    _, _, (first, second) = pair_places("gx", count, own, tall)
    if count == 2:
        first["source"] = jnp.where(odd == 0, 0, tall - HALO)
        return index, own, (first,)
    first["source"] = second["source"] = 0
    return index, own, (first, second)


def frame_extent(count, tall):
    return tall + (0 if count == 1 else HALO if count == 2 else 2 * HALO)


def keep(valid, values):
    return jnp.where(valid, values, jnp.zeros_like(values))


def y_pack_kernel(mesh_shape, *refs):
    n_gx, n_gy, n_gz = mesh_shape
    n_in = 3 * (1 + min(n_gx - 1, 2))
    own_refs, part_refs, outs = refs[:3], refs[3:n_in], refs[n_in:]
    tall, wide = own_refs[0].shape[0], own_refs[0].shape[1]
    extent = frame_extent(n_gx, tall)
    tiles = own_refs[2].shape[1] // 128
    _, own, parts = x_frame(n_gx, tall)
    odd = lax.axis_index("gy") % 2
    low = jnp.where(odd == 0, wide - HALO, 0)
    for out, start in zip(outs, (low, wide - HALO - low)):
        rows = pl.ds(pl.multiple_of(start, 8), HALO)
        for a in range(2):
            out[pl.ds(a * extent + own, tall)] = own_refs[a][:, rows, :]
            for part, ref in zip(parts, (part_refs[a : a + 1], part_refs[3 + a : 4 + a])):
                out[pl.ds(a * extent + part["place"], HALO)] = keep(part["valid"], ref[0][pl.ds(part["source"], HALO), rows, :])
        base = 2 * extent
        for side in (0, 2):
            for t in range(tiles):
                out[base + side * tiles + t] = jnp.zeros((HALO, 128), F32)
        for t in range(tiles):
            out[base + tiles + t] = own_refs[2][:, t * 128 : (t + 1) * 128]
            for part, ref in zip(parts, (part_refs[2:3], part_refs[5:6])):
                side = jnp.where(part["high"], 2, 0)
                out[base + side * tiles + t] = keep(part["valid"], ref[0][:, t * 128 : (t + 1) * 128])


def z_pack_kernel(mesh_shape, *refs):
    n_gx, n_gy, n_gz = mesh_shape
    n_in = 3 * (1 + min(n_gx - 1, 2))
    own_refs, part_refs = refs[:3], refs[3:n_in]
    y_refs = refs[n_in : n_in + 2]
    frames = refs[n_in + 2 : n_in + 4]
    rows_ref, z_outs = refs[n_in + 4], refs[n_in + 5 :]
    tall, wide = own_refs[0].shape[0], own_refs[0].shape[1]
    extent = frame_extent(n_gx, tall)
    tiles = own_refs[2].shape[1] // 128
    _, own, parts = x_frame(n_gx, tall)
    _, _, y_parts = pair_places("gy", n_gy, HALO, wide)
    for a in range(2):
        frames[a][pl.ds(own, tall), HALO : HALO + wide, :] = own_refs[a][...]
        for part, ref in zip(parts, (part_refs[a : a + 1], part_refs[3 + a : 4 + a])):
            frames[a][pl.ds(part["place"], HALO), HALO : HALO + wide, :] = keep(part["valid"], ref[0][pl.ds(part["source"], HALO)])
        for part, ref in zip(y_parts, y_refs):
            rows = pl.ds(pl.multiple_of(part["place"], 8), HALO)
            frames[a][:, rows, :] = keep(part["valid"], ref[a * extent : (a + 1) * extent])
    for t in range(tiles):
        for side in (0, 2):
            rows_ref[(side * 3 + 1) * tiles + t] = jnp.zeros((HALO, 128), F32)
        rows_ref[4 * tiles + t] = own_refs[2][:, t * 128 : (t + 1) * 128]
        for part, ref in zip(parts, (part_refs[2:3], part_refs[5:6])):
            side = jnp.where(part["high"], 2, 0)
            rows_ref[(side * 3 + 1) * tiles + t] = keep(part["valid"], ref[0][:, t * 128 : (t + 1) * 128])
        for x_side in range(3):
            for part, ref in zip(y_parts, y_refs):
                side = jnp.where(part["high"], 2, 0)
                rows_ref[(x_side * 3 + side) * tiles + t] = keep(part["valid"], ref[2 * extent + x_side * tiles + t])
    odd = lax.axis_index("gz") % 2
    groups = extent // HALO
    slot = iota((4 * HALO, 128), 1) // HALO
    for out, tail in zip(z_outs, (odd == 0, odd == 1)):
        bump = jnp.where(tail, HALO, 0)
        for group in range(groups):
            packed = jnp.zeros((4 * HALO, 128), F32)
            for i in range(HALO):
                for a in range(2):
                    piece = roll(frames[a][group * HALO + i], bump + (16 * i + 8 * a))
                    packed = jnp.where(slot == 2 * i + a, piece, packed)
            out[group] = packed
        row = jnp.where(tail, HALO - 1, 0)
        for s in range((tiles + 1) // 2):
            out[groups + s] = jnp.zeros((4 * HALO, 128), F32)
        for t in range(tiles):
            for m in range(9):
                out[groups + t // 2, 16 * (t % 2) + m : 16 * (t % 2) + m + 1, :] = rows_ref[m * tiles + t, pl.ds(row, 1), :]


def side_places(axis, count, own, side):
    index = lax.axis_index(axis)
    high = index % 2 == side
    other = jnp.where(high, index + 1, index - 1)
    return high, (other >= 0) & (other < count)


def faces_kernel(*refs):
    b, w, matrix, mine, theirs, *copies = refs
    for ref, copy in zip((b, w, matrix), copies):
        copy[...] = ref[...]
    tall, wide = b.shape[0], b.shape[1]
    tiles = matrix.shape[1] // 128
    strips = (tiles + 7) // 8
    groups = tall // HALO
    ix = lax.axis_index("gx")
    y_odd, z_odd = lax.axis_index("gy") % 2, lax.axis_index("gz") % 2
    slot = iota((wide, 128), 1) // HALO
    z_tail = (z_odd == 0, z_odd == 1)
    packed = []
    for tail in z_tail:
        bump = jnp.where(tail, HALO, 0)
        for group in range(groups):
            total = jnp.zeros((wide, 128), F32)
            for i in range(HALO):
                for a, ref in enumerate((b, w)):
                    piece = roll(ref[group * HALO + i], bump + (16 * i + 8 * a))
                    total = jnp.where(slot == 2 * i + a, piece, total)
            packed.append(total)
    for out, side in ((mine, ix), (theirs, 1 - ix)):
        y_high = y_odd == side
        rows = pl.ds(pl.multiple_of(jnp.where(y_high, wide - HALO, 0), 8), HALO)
        for a, ref in enumerate((b, w)):
            out[a * tall : (a + 1) * tall] = ref[:, rows, :]
        at = 2 * tall
        for t in range(tiles):
            out[at + t] = matrix[:, t * 128 : (t + 1) * 128]
        at += tiles

        def put_rows(at, tail):
            line = jnp.where(tail, matrix[HALO - 1 : HALO, :], matrix[0:1, :])
            for strip in range(strips):
                out[at + strip] = jnp.zeros((8, 128), F32)
            for t in range(tiles):
                out[at + t // 8, t % 8 : t % 8 + 1, :] = line[:, t * 128 : (t + 1) * 128]

        for group in range(groups):
            chosen = jnp.where(side == 0, packed[group], packed[groups + group])
            for r in range(wide // 8):
                out[at + r] = chosen[8 * r : 8 * r + 8]
            at += wide // 8
        put_rows(at, z_odd == side)
        at += strips
        for k in range(2):
            for group in range(groups):
                whole = packed[k * groups + group]
                out[at] = jnp.where(y_high, whole[wide - HALO :], whole[:HALO])
                at += 1
            put_rows(at, z_tail[k])
            at += strips


def face_counts(tall, wide, tiles):
    strips, groups = (tiles + 7) // 8, tall // HALO
    corner = (groups, strips)
    return (2 * tall, tiles), (groups * wide // 8, strips), corner, corner


def join_kernel(counts, *refs):
    mine, theirs, outs = refs[0], refs[1], refs[2:]
    ix = lax.axis_index("gx")
    at = 0
    for i, (out, parts) in enumerate(zip(outs, counts)):
        base = 0
        split = (parts[0] // 2, parts[0] // 2, parts[1]) if i == 0 else parts
        for size in split:
            out[pl.ds(base + ix * size, size)] = mine[at : at + size]
            out[pl.ds(base + (1 - ix) * size, size)] = theirs[at : at + size]
            base += 2 * size
            at += size


def frame_kernel(mesh_shape, *refs):
    n_gx, n_gy, n_gz = mesh_shape
    own_refs, part_refs = refs[:3], refs[3:6]
    mine, theirs = refs[6:10], refs[10:14]
    frames, rows_ref, z_outs = refs[14:16], refs[16], refs[17:]
    tall, wide = own_refs[0].shape[0], own_refs[0].shape[1]
    extent = frame_extent(n_gx, tall)
    tiles = own_refs[2].shape[1] // 128
    strips, groups = (tiles + 7) // 8, extent // HALO
    ix, own, parts = x_frame(n_gx, tall)
    part = parts[0]
    first = ix == 0
    _, _, y_parts = pair_places("gy", n_gy, HALO, wide)
    skip = HALO * ix

    def sides(i, place):
        a, b = mine[i][place], theirs[i][place]
        return jnp.where(first, a, b), jnp.where(first, b, a)

    for a in range(2):
        frames[a][pl.ds(own, tall), HALO : HALO + wide, :] = own_refs[a][...]
        frames[a][pl.ds(part["place"], HALO), HALO : HALO + wide, :] = part_refs[a][pl.ds(part["source"], HALO)]
        for y_part, values in zip(y_parts, sides(0, pl.ds(a * 2 * tall + skip, extent))):
            frames[a][:, pl.ds(pl.multiple_of(y_part["place"], 8), HALO), :] = keep(y_part["valid"], values)
    for x_side in range(3):
        gx = ix + x_side - 1
        inside = (gx >= 0) & (gx < n_gx)
        gx = jnp.clip(gx, 0, n_gx - 1)
        for t in range(tiles):
            for y_part, values in zip(y_parts, sides(0, 4 * tall + gx * tiles + t)):
                side = jnp.where(y_part["high"], 2, 0)
                rows_ref[(x_side * 3 + side) * tiles + t] = keep(y_part["valid"] & inside, values)
            line = own_refs[2] if x_side == 1 else part_refs[2]
            rows_ref[(x_side * 3 + 1) * tiles + t] = keep(inside, line[:, t * 128 : (t + 1) * 128])
    n_groups = 2 * tall // HALO
    for k, out in enumerate(z_outs):
        for s in range((tiles + 1) // 2):
            out[groups + s] = jnp.zeros((4 * HALO, 128), F32)
        for group in range(groups):
            g = group + ix
            for r in range(wide // 8):
                out[group, HALO + 8 * r : HALO + 8 * r + 8, :] = sides(1, g * (wide // 8) + r)[k]
            for y_part, values in zip(y_parts, sides(2 + k, g)):
                out[group, pl.ds(pl.multiple_of(y_part["place"], 8), HALO), :] = keep(y_part["valid"], values)
        for x_side in range(3):
            gx = ix + x_side - 1
            inside = (gx >= 0) & (gx < n_gx)
            gx = jnp.clip(gx, 0, n_gx - 1)
            for strip in range(strips):
                middle = keep(inside, sides(1, n_groups * wide // 8 + gx * strips + strip)[k])
                edges = [keep(p["valid"] & inside, v) for p, v in zip(y_parts, sides(2 + k, n_groups + gx * strips + strip))]
                low = jnp.where(y_parts[0]["high"], edges[1], edges[0])
                high = jnp.where(y_parts[0]["high"], edges[0], edges[1])
                for j in range(min(8, tiles - 8 * strip)):
                    t = 8 * strip + j
                    for y_side, values in enumerate((low, middle, high)):
                        m = 16 * (t % 2) + x_side * 3 + y_side
                        out[groups + t // 2, m : m + 1, :] = values[j : j + 1]


def down_kernel(mesh_shape, *refs):
    n_gx, n_gy, n_gz = mesh_shape
    fb, fw, za, zb = refs[:4]
    send, v0w, w0w, v0h, w0h, g0, v1m, v1s, w1m, w1s, g1m, g1s = refs[4:16]
    gm, gs, vm, vs, ws, tm, ts, um, us, small = refs[16:]
    extent, rows = fb.shape[0], fb.shape[1]
    tall = g0.shape[0]
    wide = g0.shape[1]
    half, half_rows = extent // 2, rows // 2
    _, own, _ = x_frame(n_gx, tall)
    _, odd, z_parts = pair_places("gz", n_gz, 0, 120)
    groups = extent // HALO
    zero = jnp.zeros((8, 128), F32)

    def clear(ref, count, depth):
        for x in (0, count + 1):
            for r in range(0, depth + 16, 8):
                ref[x, r : r + 8, :] = zero
        for x in range(1, count + 1):
            ref[x, 0:8, :] = zero
            ref[x, depth + 8 : depth + 16, :] = zero

    for ref in (gm, gs, vm, vs):
        clear(ref, extent, rows)
    for ref in (v1m, v1s, g1m, g1s, w1m, w1s):
        clear(ref, half, half_rows)

    lane = iota((rows, 128), 1)
    low_lane, high_lane = lane >= 120, lane < 8
    part_mask, part_base = [], []
    for part in z_parts:
        part_mask.append(jnp.where(part["high"], high_lane.astype(F32), low_lane.astype(F32)) * part["valid"].astype(F32))
        part_base.append(jnp.where(part["high"], 0, 120))

    def load(group):
        for i in range(HALO):
            x = group * HALO + i
            sides = []
            for a in range(2):
                total = None
                for ref, mask, base in zip((za, zb), part_mask, part_base):
                    piece = roll(ref[group], lax.rem(base + (256 - 16 * i - 8 * a), 128)) * mask
                    total = piece if total is None else total + piece
                sides.append(total)
            ws[x] = sides[1]
            gm[x + 1, 8 : 8 + rows, :] = K * fb[x] * inverse(fw[x])
            gs[x + 1, 8 : 8 + rows, :] = K * sides[0] * inverse(sides[1])

    each(groups, load, 4)

    def second(x):
        main, side, main_n, side_n = neighbours(gm, gs, x + 1, 8, rows, 1)
        vm[x + 1, 8 : 8 + rows, :] = 1.2 * main + jnp.where(fw[x] > 0.0, K * main_n, 0.0)
        vs[x + 1, 8 : 8 + rows, :] = 1.2 * side + jnp.where(ws[x] > 0.0, K * side_n, 0.0)

    each(extent, second, 8)

    def residual(x2):
        totals = None
        for j in range(2):
            x = 2 * x2 + j
            main, side, main_n, side_n = neighbours(vm, vs, x + 1, 8, rows, 1)
            w_main, w_side = fw[x], ws[x]
            r_main = w_main * ((1.0 / K) * gm[x + 1, 8 : 8 + rows, :] - 6.0 * main + main_n)
            r_side = w_side * ((1.0 / K) * gs[x + 1, 8 : 8 + rows, :] - 6.0 * side + side_n)
            values = (r_main, r_side, w_main, w_side)
            totals = values if j == 0 else tuple(a + b for a, b in zip(totals, values))
        for ref, value in zip((tm, ts, um, us), totals):
            ref[x2] = value

        def pairs(ref):
            return lane_pairs(ref[x2, pl.ds(0, half_rows, stride=2), :] + ref[x2, pl.ds(1, half_rows, stride=2), :], 1)

        for t_ref, u_ref, w_out, g_out in ((tm, um, w1m, g1m), (ts, us, w1s, g1s)):
            weights = 0.0625 * pairs(u_ref)
            w_out[x2 + 1, 8 : 8 + half_rows, :] = weights
            g_out[x2 + 1, 8 : 8 + half_rows, :] = (0.125 * K) * pairs(t_ref) * inverse(weights)

    each(half, residual, 4)

    def second_1(x):
        main, side, main_n, side_n = neighbours(g1m, g1s, x + 1, 8, half_rows, 2)
        v1m[x + 1, 8 : 8 + half_rows, :] = 1.2 * main + jnp.where(w1m[x + 1, 8 : 8 + half_rows, :] > 0.0, K * main_n, 0.0)
        v1s[x + 1, 8 : 8 + half_rows, :] = 1.2 * side + jnp.where(w1s[x + 1, 8 : 8 + half_rows, :] > 0.0, K * side_n, 0.0)

    each(half, second_1, 16)

    base = own // 2
    first_row = 8 + HALO // 2
    quarter, quarter_rows = tall // 4, wide // 4
    for x2 in range(quarter):
        total_r = total_w = None
        for j in range(2):
            x = base + 2 * x2 + j + 1
            main, _, main_n, _ = neighbours(v1m, v1s, x, first_row, wide // 2, 2)
            weights = w1m[x, pl.ds(first_row, wide // 2), :]
            res = weights * ((1.0 / K) * g1m[x, pl.ds(first_row, wide // 2), :] - 6.0 * main + main_n)
            total_r = res if j == 0 else total_r + res
            total_w = weights if j == 0 else total_w + weights
        small[0, x2] = total_r
        small[1, x2] = total_w
    q = []
    for a, factor in ((0, 0.125), (1, 0.0625)):
        for x2 in range(quarter):
            ref = small.at[a, x2]
            both = ref[pl.ds(0, quarter_rows, stride=2), :] + ref[pl.ds(1, quarter_rows, stride=2), :]
            q.append(factor * lane_pairs(both, 2))
    stacked = jnp.concatenate([jnp.concatenate(q[:quarter], axis=0), jnp.concatenate(q[quarter:], axis=0)], axis=0)
    src, dst = iota((128, 128), 0), iota((128, 128), 1)
    pick = (src == 4 * (dst % 32)).astype(F32)
    compact = jnp.dot(stacked, pick, precision=lax.Precision.HIGHEST, preferred_element_type=F32)
    block = iota((quarter_rows, 128), 1) // 32
    gz = lax.axis_index("gz")
    out = []
    for a in range(2):
        packed = jnp.zeros((quarter_rows, 128), F32)
        for x2 in range(quarter):
            r = (a * quarter + x2) * quarter_rows
            packed = jnp.where(block == lax.rem(gz + x2, 4), compact[r : r + quarter_rows], packed)
        out.append(packed)
    message = jnp.concatenate(out, axis=0)

    def copy(d):
        send[d] = message

    each(send.shape[0], copy, 8)

    for i in range(tall + 2):
        v0w[i] = vm[own + i, 8 : 8 + rows, :]
        x = own + (i - 1)
        inside = (x >= 0) & (x < extent)
        w0w[i] = keep(inside, fw[jnp.clip(x, 0, extent - 1)])
    for i in range(tall):
        v0h[i] = vs[own + i + 1, 8 + HALO : 8 + HALO + wide, :]
        w0h[i] = ws[own + i, HALO : HALO + wide, :]
        g0[i] = gm[own + i + 1, 8 + HALO : 8 + HALO + wide, :]


def up_kernel(mesh_shape, *refs):
    n_gx, n_gy, n_gz = mesh_shape
    recv, rows_ref, za, zb, v0w, w0w, v0h, w0h, g0, v1m, v1s, w1m, w1s, g1m, g1s, out = refs[:16]
    g2, w2, v2, y2, e2, p2, t3, u3, g3, w3, v3, y3, p3, b4, col, y1m, y1s, e1m, e1s, f1m, f1s, y0m, y0s = refs[16:]
    tall, wide = out.shape[0], out.shape[1]
    size_x, size_z = w2.shape[0], w2.shape[2]
    size_y = w2.shape[1]
    ix, own, _ = x_frame(n_gx, tall)
    iy, iz = lax.axis_index("gy"), lax.axis_index("gz")
    quarter, quarter_rows = tall // 4, wide // 4
    extent = frame_extent(n_gx, tall)
    half, half_rows = v1m.shape[0] - 2, v1m.shape[1] - 16

    def clear(ref):
        count, depth, size = ref.shape
        zero = jnp.zeros((8, size), F32)
        for x in range(count):
            ref[x, 0:8, :] = zero
            ref[x, depth - 8 : depth, :] = zero
        for x in (0, count - 1):
            ref[x] = jnp.zeros((depth, size), F32)

    for ref in (g2, v2, y2, g3, v3, y3):
        clear(ref)
    e2[...] = jnp.zeros(e2.shape, F32)
    p3[...] = jnp.zeros(p3.shape, F32)

    lane = iota((quarter_rows, 128), 1)
    block = lane // 32
    for gx in range(n_gx):
        for gy in range(n_gy):
            for x in range(quarter):
                tiles_b, tiles_w = [], []
                for tile in range(size_z // 128):
                    picked = [jnp.zeros((quarter_rows, 128), F32)] * 2
                    for j in range(4):
                        gz = tile * 4 + j
                        d = (gx * n_gy + gy) * n_gz + gz
                        mask = block == (gz + x) % 4
                        for a in range(2):
                            piece = recv[d, a * quarter_rows : (a + 1) * quarter_rows, :]
                            picked[a] = jnp.where(mask, piece, picked[a])
                    tiles_b.append(roll(picked[0], -32 * x))
                    tiles_w.append(roll(picked[1], -32 * x))
                weights = joined(tiles_w)
                w2[gx * quarter + x, gy * quarter_rows : (gy + 1) * quarter_rows, :] = weights
                g2[gx * quarter + x + 1, 8 + gy * quarter_rows : 8 + (gy + 1) * quarter_rows, :] = K * joined(tiles_b) / weights

    def smooth(g, v, x, rows, step):
        main, near = global_neighbours(g, x + 1, 8, rows, step)
        v[x + 1, 8 : 8 + rows, :] = 1.2 * main + K * near

    def resid(g, v, w, x, rows, step):
        main, near = global_neighbours(v, x + 1, 8, rows, step)
        return w[x] * ((1.0 / K) * g[x + 1, 8 : 8 + rows, :] - 6.0 * main + near)

    each(size_x, lambda x: smooth(g2, v2, x, size_y, 1), 8)
    rows3, x3 = size_y // 2, size_x // 2

    def restrict_2(x):
        for t, part in enumerate(tiled(resid(g2, v2, w2, 2 * x, size_y, 1) + resid(g2, v2, w2, 2 * x + 1, size_y, 1))):
            t3[t] = part
        for t, part in enumerate(tiled(w2[2 * x] + w2[2 * x + 1])):
            u3[t] = part
        pairs = lambda ref: lane_pairs(row_pairs(ref, size_y), 1)
        weights = 0.0625 * pairs(u3)
        w3[x] = weights
        g3[x + 1, 8 : 8 + rows3, :] = (0.125 * K) * pairs(t3) / weights

    each(x3, restrict_2, 4)
    each(x3, lambda x: smooth(g3, v3, x, rows3, 2), 8)
    rows4, x4 = rows3 // 2, x3 // 2

    def restrict_3(x):
        for t, part in enumerate(tiled(resid(g3, v3, w3, 2 * x, rows3, 2) + resid(g3, v3, w3, 2 * x + 1, rows3, 2))):
            t3[t, 0:rows3, :] = part
        b4[x] = 0.125 * lane_pairs(row_pairs(t3, rows3), 2)

    each(x4, restrict_3, 4)

    tiles = rows_ref.shape[0] // 9
    coarse_z = size_z // 4
    per = 128 // coarse_z
    src, dst = iota((size_z, 128), 0), iota((size_z, 128), 1)
    pick = (src == 4 * (dst % coarse_z)).astype(F32)
    values = b4[0] if x4 == 1 else jnp.concatenate([b4[x] for x in range(x4)], axis=0)
    compact = jnp.dot(values, pick, precision=lax.Precision.HIGHEST, preferred_element_type=F32)
    place = iota((x4 * rows4, 128), 0) % per == iota((x4 * rows4, 128), 1) // coarse_z
    compact = jnp.where(place, compact, 0.0)
    vectors = [jnp.sum(compact[t * per : (t + 1) * per], axis=0, keepdims=True) for t in range(tiles)]
    _, _, z_parts = pair_places("gz", n_gz, 0, 120)
    groups = extent // HALO
    fine = iota((HALO, size_z), 1) // 4
    fine_row = fine == iz * HALO + iota((HALO, size_z), 0)
    edge_row = iota((16, 128), 0)
    first_total = [None, None]
    for k, ref in enumerate((za, zb)):
        total = None
        for t in range(tiles):
            piece = ref[groups + t // 2, 16 * (t % 2) : 16 * (t % 2) + 16, :] * vectors[t]
            total = piece if total is None else total + piece
        first_total[k] = jnp.sum(total, axis=1, keepdims=True) * z_parts[k]["valid"].astype(F32)
    z_lane = iota((16, size_z), 1) // 4
    spread = None
    for k in range(2):
        where = jnp.where(z_parts[k]["high"], iz * HALO + HALO, iz * HALO - 1)
        piece = jnp.where(z_lane == where, first_total[k], 0.0)
        spread = piece if spread is None else spread + piece
    for m in range(9):
        total = None
        for t in range(tiles):
            piece = rows_ref[m * tiles + t] * vectors[t]
            total = piece if total is None else total + piece
        values = jnp.sum(total, axis=1, keepdims=True)
        line = jnp.sum(jnp.where(fine_row, values, 0.0), axis=0, keepdims=True) + spread[m : m + 1, :]
        row = 8 + 2 * (iy + (m % 3 - 1))
        for t, part in enumerate(tiled(line)):
            p3[ix + m // 3, t, pl.ds(row, 1), :] = part
            p3[ix + m // 3, t, pl.ds(row + 1, 1), :] = part

    def lift(y, v, w, p, x, px, rows, row):
        coarse = joined([p[px, t, row : row + rows, :] for t in range(p.shape[1])])
        y[x + 1, 8 : 8 + rows, :] = v[x + 1, 8 : 8 + rows, :] + w[x] * coarse

    def relax(y, g, w, x, rows, step):
        main, near = global_neighbours(y, x + 1, 8, rows, step)
        return (0.2 * main + g[x + 1, 8 : 8 + rows, :] + K * near) / w[x]

    each(x3, lambda x: lift(y3, v3, w3, p3, x, x // 2 + 1, rows3, 8), 8)

    def up_3(x):
        for t, e3 in enumerate(tiled(relax(y3, g3, w3, x, rows3, 2))):
            p2[x, t, pl.ds(0, rows3, stride=2), :] = e3
            p2[x, t, pl.ds(1, rows3, stride=2), :] = e3

    each(x3, up_3, 4)
    each(size_x, lambda x: lift(y2, v2, w2, p2, x, x // 2, size_y, 0), 8)

    def up_2(x):
        for t, part in enumerate(tiled(relax(y2, g2, w2, x, size_y, 1))):
            e2[x + 2, t, 8 : 8 + size_y, :] = part

    each(size_x, up_2, 8)

    src, dst = iota((size_z, 256), 0), iota((size_z, 256), 1)
    start = iz * 32
    cell = jnp.where(dst < 128, dst // 4, jnp.where(dst < 192, 32 + (dst - 128) // 4, -1 - (255 - dst) // 4))
    widen = (src == start + cell).astype(F32)
    n2 = extent // 4
    x_start = ix * quarter - own // 4
    y_start = 8 + iy * quarter_rows - HALO // 4
    spread = None
    for t in range(size_z // 128):
        stacked = jnp.concatenate([e2[x_start + 2 + i, t, pl.ds(y_start, 8), :] for i in range(n2)], axis=0)
        part = jnp.dot(stacked, widen[t * 128 : (t + 1) * 128], precision=lax.Precision.HIGHEST, preferred_element_type=F32)
        spread = part if spread is None else spread + part
    for i in range(n2):
        for ref, part in ((e1m, spread[i * 8 : i * 8 + 8, :128]), (e1s, spread[i * 8 : i * 8 + 8, 128:])):
            ref[i, pl.ds(0, 8, stride=2), :] = part
            ref[i, pl.ds(1, 8, stride=2), :] = part

    clear(y1m)
    clear(y1s)
    inner = slice(8, 8 + half_rows)
    for x in range(half):
        y1m[x + 1, inner, :] = v1m[x + 1, inner, :] + w1m[x + 1, inner, :] * e1m[x // 2]
        y1s[x + 1, inner, :] = v1s[x + 1, inner, :] + w1s[x + 1, inner, :] * e1s[x // 2]

    def up_1(x):
        main, side, main_n, side_n = neighbours(y1m, y1s, x + 1, 8, half_rows, 2)
        for f, y, near, g, w in ((f1m, main, main_n, g1m, w1m), (f1s, side, side_n, g1s, w1s)):
            e1 = (0.2 * y + g[x + 1, inner, :] + K * near) * inverse(w[x + 1, inner, :])
            f[x, pl.ds(0, half_rows, stride=2), :] = e1
            f[x, pl.ds(1, half_rows, stride=2), :] = e1

    each(half, up_1, 12)
    base = own // 2
    for i in range(tall + 2):
        parent = jnp.clip(base + (i + 1) // 2 - 1, 0, half - 1)
        y0m[i] = v0w[i] + w0w[i] * f1m[parent]
        if 0 < i <= tall:
            y0s[i - 1] = v0h[i - 1] + w0h[i - 1] * f1s[parent, HALO : HALO + wide, :]

    def up_0(i):
        main = y0m[i + 1, pl.ds(HALO, wide), :]
        main_z, _ = z_sum(main, y0s[i], 1)
        near = xy_sum(y0m, i + 1, HALO, wide) + main_z
        out[i] = (0.2 * main + g0[i] + K * near) / w0w[i + 1, HALO : HALO + wide, :]

    each(tall, up_0, 16)


def size_of(shape):
    return 4 * math.prod(shape)


def call(kernel, outs, scratch=(), resident=True, fetch=False):
    limit = 8 * 2**20 + sum(map(size_of, scratch)) + sum(size_of(s) for s in outs if size_of(s) > 2**20)
    run = pl.pallas_call(
        kernel,
        out_shape=[(pltpu.VMEM if resident and size_of(s) <= 2**20 else jax.ShapeDtypeStruct)(s, F32) for s in outs],
        scratch_shapes=[pltpu.VMEM(s, F32) for s in scratch],
        compiler_params=pltpu.CompilerParams(vmem_limit_bytes=min(limit, 56 * 2**20)),
    )

    def place(value):
        small = size_of(value.shape) <= 2**20 and not fetch
        return pltpu.with_memory_space_constraint(value, pltpu.VMEM if small else pltpu.HBM)

    return lambda *values: run(*map(place, values))


def plain_halo(mesh_shape, own, frames):
    n_gx = mesh_shape[0]
    tall = own[0].shape[0]
    extent, tiles = frames[0][0], own[2].shape[1] // 128
    parts = ()
    if n_gx > 1:
        odd = lax.axis_index("gx") % 2
        for first in range(2):
            start = jnp.where(odd == first, tall - HALO, 0)
            faces = [lax.dynamic_slice_in_dim(a, start, HALO, 0) for a in own[:2]] + [own[2]]
            parts += tuple(swap(a, "gx", first) for a in faces)
    slab = (2 * extent + 3 * tiles, HALO, 128)
    y_slabs = call(functools.partial(y_pack_kernel, mesh_shape), [slab, slab])(*own, *parts)
    y_parts = [swap(s, "gy", first) for first, s in enumerate(y_slabs)]
    fb, fw, matrix, z_a, z_b = call(functools.partial(z_pack_kernel, mesh_shape), frames)(*own, *parts, *y_parts)
    return fb, fw, matrix, swap(z_a, "gz", 0), swap(z_b, "gz", 1)


def pair(index, count, first):
    other = index + 1 if index % 2 == first else index - 1
    return other if 0 <= other < count else index


def shared_halo(mesh_shape, own, frames):
    n_gx, n_gy, n_gz = mesh_shape
    tall, wide = own[0].shape[:2]
    tiles = own[2].shape[1] // 128
    counts = face_counts(tall, wide, tiles)
    total = (sum(map(sum, counts)), HALO, 128)
    mine, theirs, *here = call(faces_kernel, [total, total] + [a.shape for a in own], fetch=True)(*own)
    theirs = swap(theirs, "gx", 0)
    messages = call(functools.partial(join_kernel, counts), [(2 * sum(c), HALO, 128) for c in counts])(mine, theirs)

    def send(message, y_side, z_side):
        links = []
        for x in range(n_gx):
            for y in range(n_gy):
                for z in range(n_gz):
                    y_to = y if y_side is None else pair(y, n_gy, x)
                    z_to = z if z_side is None else pair(z, n_gz, x if z_side < 0 else z_side)
                    links.append(((x * n_gy + y) * n_gz + z, (x * n_gy + y_to) * n_gz + z_to))
        return lax.ppermute(message, AXES, links)

    got = [send(m, *way) for m, way in zip(messages, ((0, None), (None, -1), (0, 0), (0, 1)))]
    parts = [swap(a, "gx", 0) for a in own]
    got = lax.optimization_barrier(got)
    others = [swap(m, "gx", 0) for m in got]
    return call(functools.partial(frame_kernel, mesh_shape), frames)(*here, *parts, *got, *others)


def per_device(mesh_shape, sources, stiffness, coarse_inverse):
    n_gx, n_gy, n_gz = mesh_shape
    count = n_gx * n_gy * n_gz
    tall, wide, deep = stiffness.shape
    cells = coarse_inverse.shape[1]
    assert sources.shape[0] == 1 and deep == 128 and tall == 16 and wide == 16 and n_gz % 4 == 0 and cells % 128 == 0
    tiles = cells // 128
    extent = frame_extent(n_gx, tall)
    source = sources[0]
    own = (source, stiffness, coarse_inverse)
    rows = wide + 2 * HALO
    frame = (extent, rows, 128)
    z_slab = (extent // HALO + (tiles + 1) // 2, rows, 128)
    frames = [frame, frame, (9 * tiles, HALO, 128), z_slab, z_slab]
    exchange = shared_halo if n_gx == 2 else plain_halo
    fb, fw, matrix, z_a, z_b = exchange(mesh_shape, own, frames)
    padded = (extent + 2, rows + 16, 128)
    half, half_rows = extent // 2, rows // 2
    level1 = (half + 2, half_rows + 16, 128)
    window, face = (tall + 2, rows, 128), (tall, wide, 128)
    message = (count, wide // 2, 128)
    outs = [message, window, window, face, face, face] + [level1] * 6
    scratch = [padded] * 4 + [frame] + [(half, rows, 128)] * 4 + [(2, tall // 4, wide // 2, 128)]
    send, *state = call(functools.partial(down_kernel, mesh_shape), outs, scratch)(fb, fw, z_a, z_b)
    recv = lax.all_to_all(send, AXES, 0, 0, tiled=True)
    size_x, size_y, size_z = n_gx * tall // 4, n_gy * wide // 4, n_gz * deep // 4
    pad2 = (size_x + 2, size_y + 16, size_z)
    x3, rows3 = size_x // 2, size_y // 2
    pad3 = (x3 + 2, rows3 + 16, size_z)
    n2, lane_tiles = extent // 4, size_z // 128
    scratch = [
        pad2, (size_x, size_y, size_z), pad2, pad2, (size_x + 4, lane_tiles, size_y + 16, 128), (x3, lane_tiles, size_y, 128),
        (lane_tiles, size_y, 128), (lane_tiles, size_y, 128), pad3, (x3, rows3, size_z), pad3, pad3,
        (x3 // 2 + 2, lane_tiles, rows3 + 16, 128),
        (x3 // 2, rows3 // 2, size_z), (8, 128), level1, level1, (n2, 16, 128), (n2, 16, 128),
        (half, rows, 128), (half, rows, 128), window, face,
    ]
    (pressure,) = call(functools.partial(up_kernel, mesh_shape), [face], scratch, False)(recv, matrix, z_a, z_b, *state)
    return pressure[None]


def solution(mesh):
    mesh_shape = tuple(mesh.shape[a] for a in AXES)
    in_specs = (P(None, "gx", "gy", "gz"), P("gx", "gy", "gz"), P(AXES, None))
    return jax.shard_map(
        functools.partial(per_device, mesh_shape),
        mesh=mesh,
        in_specs=in_specs,
        out_specs=P(None, "gx", "gy", "gz"),
        check_vma=False,
    )
```

```python
import functools
import math

import jax
import jax.numpy as jnp
from jax import lax
from jax.experimental import pallas as pl
from jax.experimental.pallas import tpu as pltpu
from jax.sharding import PartitionSpec as P

damping = 0.8
K = damping / 6.0
AXES = ("gx", "gy", "gz")
HALO = 8
F32 = jnp.float32


def swap(values, axis, first):
    count = lax.axis_size(axis)
    partner = list(range(count))
    for i in range(first, count - 1, 2):
        partner[i], partner[i + 1] = i + 1, i
    return lax.ppermute(values, axis, list(enumerate(partner)))


def ring(values, axis, step):
    count = lax.axis_size(axis)
    return lax.ppermute(values, axis, [(i, (i + step) % count) for i in range(count)])


def iota(shape, dim):
    return lax.broadcasted_iota(jnp.int32, shape, dim)


def roll(values, amount):
    size = values.shape[-1]
    if isinstance(amount, int):
        amount = amount % size
        if amount == 0:
            return values
    return pltpu.roll(values, amount, values.ndim - 1)


def z_sum(main, side, step):
    lane = iota(main.shape, main.ndim - 1)
    size = main.shape[-1]
    main_up, side_up = roll(main, -step), roll(side, -step)
    main_dn, side_dn = roll(main, step), roll(side, step)
    last = lane >= size - step
    first = lane < step
    main_sum = jnp.where(last, side_up, main_up) + jnp.where(first, side_dn, main_dn)
    side_sum = jnp.where(last, main_up, side_up) + jnp.where(first, main_dn, side_dn)
    return main_sum, side_sum


def xy_sum(ref, x, row, rows):
    total = ref[x - 1, pl.ds(row, rows), :] + ref[x + 1, pl.ds(row, rows), :]
    return total + ref[x, pl.ds(row - 1, rows), :] + ref[x, pl.ds(row + 1, rows), :]


def neighbours(main_ref, side_ref, x, row, rows, step):
    main = main_ref[x, pl.ds(row, rows), :]
    side = side_ref[x, pl.ds(row, rows), :]
    main_z, side_z = z_sum(main, side, step)
    return main, side, xy_sum(main_ref, x, row, rows) + main_z, xy_sum(side_ref, x, row, rows) + side_z


def global_neighbours(ref, x, row, rows, step):
    main = ref[x, pl.ds(row, rows), :]
    lane = iota(main.shape, 1)
    size = main.shape[-1]
    up = jnp.where(lane >= size - step, 0.0, roll(main, -step))
    dn = jnp.where(lane < step, 0.0, roll(main, step))
    return main, xy_sum(ref, x, row, rows) + up + dn


def lane_pairs(values, step):
    lane = iota(values.shape, values.ndim - 1)
    return values + jnp.where((lane // step) % 2 == 0, roll(values, -step), roll(values, step))


def inverse(weights):
    return jnp.where(weights > 0.0, 1.0 / jnp.where(weights > 0.0, weights, 1.0), 0.0)


def tiled(value):
    return [value[:, t * 128 : (t + 1) * 128] for t in range(value.shape[1] // 128)]


def joined(parts):
    return parts[0] if len(parts) == 1 else jnp.concatenate(parts, axis=1)


def row_pairs(ref, rows):
    return joined([ref[t, pl.ds(0, rows // 2, stride=2), :] + ref[t, pl.ds(1, rows // 2, stride=2), :] for t in range(ref.shape[0])])


def each(count, body, width=1):
    while count % width:
        width -= 1
    if count == width:
        for i in range(count):
            body(i)
        return

    def step(i, carry):
        for j in range(width):
            body(i * width + j)
        return carry

    lax.fori_loop(0, count // width, step, 0)


def pair_places(axis, count, own, tall):
    index = lax.axis_index(axis)
    odd = index % 2
    first = dict(place=jnp.where(odd == 0, own + tall, 0), high=odd == 0, valid=jnp.where(odd == 0, index + 1, index - 1) < count)
    other = jnp.where(odd == 0, index - 1, index + 1)
    second = dict(place=jnp.where(odd == 0, 0, own + tall), high=odd == 1, valid=(other >= 0) & (other < count))
    return index, odd, (first, second)


def x_frame(count, tall):
    index = lax.axis_index("gx")
    odd = index % 2
    if count == 1:
        return index, 0, ()
    own = HALO * odd if count == 2 else HALO
    _, _, (first, second) = pair_places("gx", count, own, tall)
    if count == 2:
        first["source"] = jnp.where(odd == 0, 0, tall - HALO)
        return index, own, (first,)
    first["source"] = second["source"] = 0
    return index, own, (first, second)


def frame_extent(count, tall):
    return tall + (0 if count == 1 else HALO if count == 2 else 2 * HALO)


def keep(valid, values):
    return jnp.where(valid, values, jnp.zeros_like(values))


def y_pack_kernel(mesh_shape, *refs):
    n_gx, n_gy, n_gz = mesh_shape
    n_in = 3 * (1 + min(n_gx - 1, 2))
    own_refs, part_refs, outs = refs[:3], refs[3:n_in], refs[n_in:]
    tall, wide = own_refs[0].shape[0], own_refs[0].shape[1]
    extent = frame_extent(n_gx, tall)
    tiles = own_refs[2].shape[1] // 128
    _, own, parts = x_frame(n_gx, tall)
    odd = lax.axis_index("gy") % 2
    low = jnp.where(odd == 0, wide - HALO, 0)
    for out, start in zip(outs, (low, wide - HALO - low)):
        rows = pl.ds(pl.multiple_of(start, 8), HALO)
        for a in range(2):
            out[pl.ds(a * extent + own, tall)] = own_refs[a][:, rows, :]
            for part, ref in zip(parts, (part_refs[a : a + 1], part_refs[3 + a : 4 + a])):
                out[pl.ds(a * extent + part["place"], HALO)] = keep(part["valid"], ref[0][pl.ds(part["source"], HALO), rows, :])
        base = 2 * extent
        for side in (0, 2):
            for t in range(tiles):
                out[base + side * tiles + t] = jnp.zeros((HALO, 128), F32)
        for t in range(tiles):
            out[base + tiles + t] = own_refs[2][:, t * 128 : (t + 1) * 128]
            for part, ref in zip(parts, (part_refs[2:3], part_refs[5:6])):
                side = jnp.where(part["high"], 2, 0)
                out[base + side * tiles + t] = keep(part["valid"], ref[0][:, t * 128 : (t + 1) * 128])


def z_pack_kernel(mesh_shape, *refs):
    n_gx, n_gy, n_gz = mesh_shape
    n_in = 3 * (1 + min(n_gx - 1, 2))
    own_refs, part_refs = refs[:3], refs[3:n_in]
    y_refs = refs[n_in : n_in + 2]
    frames = refs[n_in + 2 : n_in + 4]
    rows_ref, z_outs = refs[n_in + 4], refs[n_in + 5 :]
    tall, wide = own_refs[0].shape[0], own_refs[0].shape[1]
    extent = frame_extent(n_gx, tall)
    tiles = own_refs[2].shape[1] // 128
    _, own, parts = x_frame(n_gx, tall)
    _, _, y_parts = pair_places("gy", n_gy, HALO, wide)
    for a in range(2):
        frames[a][pl.ds(own, tall), HALO : HALO + wide, :] = own_refs[a][...]
        for part, ref in zip(parts, (part_refs[a : a + 1], part_refs[3 + a : 4 + a])):
            frames[a][pl.ds(part["place"], HALO), HALO : HALO + wide, :] = keep(part["valid"], ref[0][pl.ds(part["source"], HALO)])
        for part, ref in zip(y_parts, y_refs):
            rows = pl.ds(pl.multiple_of(part["place"], 8), HALO)
            frames[a][:, rows, :] = keep(part["valid"], ref[a * extent : (a + 1) * extent])
    for t in range(tiles):
        for side in (0, 2):
            rows_ref[(side * 3 + 1) * tiles + t] = jnp.zeros((HALO, 128), F32)
        rows_ref[4 * tiles + t] = own_refs[2][:, t * 128 : (t + 1) * 128]
        for part, ref in zip(parts, (part_refs[2:3], part_refs[5:6])):
            side = jnp.where(part["high"], 2, 0)
            rows_ref[(side * 3 + 1) * tiles + t] = keep(part["valid"], ref[0][:, t * 128 : (t + 1) * 128])
        for x_side in range(3):
            for part, ref in zip(y_parts, y_refs):
                side = jnp.where(part["high"], 2, 0)
                rows_ref[(x_side * 3 + side) * tiles + t] = keep(part["valid"], ref[2 * extent + x_side * tiles + t])
    groups = extent // HALO
    for out, tail in zip(z_outs, (1, 0)):

        def put(group, packed):
            out[group] = packed

        pack_z(frames, put, tail)
        row = (HALO - 1) * tail
        for s in range((tiles + 1) // 2):
            out[groups + s] = jnp.zeros((4 * HALO, 128), F32)
        for t in range(tiles):
            for m in range(9):
                out[groups + t // 2, 16 * (t % 2) + m : 16 * (t % 2) + m + 1, :] = rows_ref[m * tiles + t, row : row + 1, :]


def z_ends(count):
    index = lax.axis_index("gz")
    return (dict(valid=index > 0, lane=120, row=-1), dict(valid=index < count - 1, lane=0, row=HALO))


def pack_z(frames, out, tail):
    rows = frames[0].shape[1]
    slot = iota((rows, 128), 1) // HALO
    for group in range(frames[0].shape[0] // HALO):
        packed = jnp.zeros((rows, 128), F32)
        for i in range(HALO):
            for a in range(2):
                piece = roll(frames[a][group * HALO + i], 8 * (tail + 2 * i + a))
                packed = jnp.where(slot == 2 * i + a, piece, packed)
        out(group, packed)


def z_face_kernel(*refs):
    b, w, matrix, *outs = refs
    outs, copies = outs[:2], outs[2:]
    for ref, copy in zip((b, w, matrix), copies):
        copy[...] = ref[...]
    tall, wide = b.shape[0], b.shape[1]
    tiles = matrix.shape[1] // 128
    strips = (tiles + 7) // 8
    per = wide // 8
    for out, tail in zip(outs, (1, 0)):

        def put(group, packed):
            for r in range(per):
                out[group * per + r] = packed[8 * r : 8 * r + 8]

        pack_z((b, w), put, tail)
        at = tall // HALO * per
        line = matrix[HALO - 1 : HALO, :] if tail else matrix[0:1, :]
        for strip in range(strips):
            out[at + strip] = jnp.zeros((8, 128), F32)
        for t in range(tiles):
            out[at + t // 8, t % 8 : t % 8 + 1, :] = line[:, t * 128 : (t + 1) * 128]


def y_face_kernel(*refs):
    b, w, matrix, z_low, z_high, *outs = refs
    outs, both = outs[:2], outs[2]
    tall, wide = b.shape[0], b.shape[1]
    tiles = matrix.shape[1] // 128
    strips, groups, per = (tiles + 7) // 8, tall // HALO, wide // 8
    odd = lax.axis_index("gy") % 2
    low = jnp.where(odd == 0, wide - HALO, 0)
    for out, start in zip(outs, (low, wide - HALO - low)):
        rows = pl.ds(pl.multiple_of(start, 8), HALO)
        for a, ref in enumerate((b, w)):
            out[a * tall : (a + 1) * tall] = ref[:, rows, :]
        at = 2 * tall
        for t in range(tiles):
            out[at + t] = matrix[:, t * 128 : (t + 1) * 128]
        at += tiles
        for ref in (z_low, z_high):
            for group in range(groups):
                out[at + group] = ref[group * per + start // 8]
            out[at + groups : at + groups + strips] = ref[groups * per : groups * per + strips]
            at += groups + strips
    at = 0
    for ref in (b, w):
        for r in range(per):
            both[at : at + tall] = ref[:, 8 * r : 8 * r + 8, :]
            at += tall
    for t in range(tiles):
        both[at + t] = matrix[:, t * 128 : (t + 1) * 128]
    at += tiles
    for ref in (z_low, z_high):
        size = ref.shape[0]
        both[at : at + size] = ref[...]
        at += size


def frame_kernel(mesh_shape, *refs):
    n_gx, n_gy, n_gz = mesh_shape
    own_refs, other = refs[:3], refs[3]
    z_refs, y_refs, y_others = refs[4:6], refs[6:8], refs[8:10]
    frames, rows_ref, z_outs = refs[10:12], refs[12], refs[13:]
    tall, wide = own_refs[0].shape[0], own_refs[0].shape[1]
    extent = frame_extent(n_gx, tall)
    tiles = own_refs[2].shape[1] // 128
    strips, groups, per = (tiles + 7) // 8, tall // HALO, wide // 8
    ix, own, parts = x_frame(n_gx, tall)
    place, source = parts[0]["place"], parts[0]["source"]
    _, _, y_parts = pair_places("gy", n_gy, HALO, wide)
    far = jnp.where(parts[0]["high"], 2, 0)
    y_rows = [pl.ds(pl.multiple_of(p["place"], 8), HALO) for p in y_parts]
    y_side = [jnp.where(p["high"], 2, 0) for p in y_parts]
    for a in range(2):
        frames[a][pl.ds(own, tall), HALO : HALO + wide, :] = own_refs[a][...]
        for r in range(per):
            rows = slice(HALO + 8 * r, HALO + 8 * r + 8)
            frames[a][pl.ds(place, HALO), rows, :] = other[pl.ds((a * per + r) * tall + source, HALO)]
        for part, rows, ref, ref_other in zip(y_parts, y_rows, y_refs, y_others):
            frames[a][pl.ds(own, tall), rows, :] = keep(part["valid"], ref[a * tall : (a + 1) * tall])
            frames[a][pl.ds(place, HALO), rows, :] = keep(part["valid"], ref_other[pl.ds(a * tall + source, HALO)])
    zero = jnp.zeros((HALO, 128), F32)
    for t in range(tiles):
        for side in range(3):
            rows_ref[((2 - far) * 3 + side) * tiles + t] = zero
        rows_ref[4 * tiles + t] = own_refs[2][:, t * 128 : (t + 1) * 128]
        rows_ref[(far * 3 + 1) * tiles + t] = other[2 * per * tall + t]
        for part, side, ref, ref_other in zip(y_parts, y_side, y_refs, y_others):
            rows_ref[(3 + side) * tiles + t] = keep(part["valid"], ref[2 * tall + t])
            rows_ref[(far * 3 + side) * tiles + t] = keep(part["valid"], ref_other[2 * tall + t])
    for k, (out, ref) in enumerate(zip(z_outs, z_refs)):
        base = 2 * per * tall + tiles + k * (groups * per + strips)
        y_base = 2 * tall + tiles + k * (groups + strips)
        total = extent // HALO
        for s in range((tiles + 1) // 2):
            out[total + s] = jnp.zeros((4 * HALO, 128), F32)
        for g in range(groups):
            for r in range(per):
                out[own // HALO + g, HALO + 8 * r : HALO + 8 * r + 8, :] = ref[g * per + r]
            for part, rows, y_ref in zip(y_parts, y_rows, y_refs):
                out[own // HALO + g, rows, :] = keep(part["valid"], y_ref[y_base + g])
        for r in range(per):
            out[place // HALO, HALO + 8 * r : HALO + 8 * r + 8, :] = other[base + source // HALO * per + r]
        for part, rows, y_ref in zip(y_parts, y_rows, y_others):
            out[place // HALO, rows, :] = keep(part["valid"], y_ref[y_base + source // HALO])
        for strip in range(strips):
            for x_side in range(3):
                if x_side == 1:
                    middle = ref[groups * per + strip]
                    edges = [keep(p["valid"], r[y_base + groups + strip]) for p, r in zip(y_parts, y_refs)]
                else:
                    here = far == x_side
                    middle = keep(here, other[base + groups * per + strip])
                    edges = [keep(p["valid"] & here, r[y_base + groups + strip]) for p, r in zip(y_parts, y_others)]
                low = jnp.where(y_parts[0]["high"], edges[1], edges[0])
                high = jnp.where(y_parts[0]["high"], edges[0], edges[1])
                for j in range(min(8, tiles - 8 * strip)):
                    t = 8 * strip + j
                    for side, values in enumerate((low, middle, high)):
                        m = 16 * (t % 2) + x_side * 3 + side
                        out[total + t // 2, m : m + 1, :] = values[j : j + 1]


def down_kernel(mesh_shape, *refs):
    n_gx, n_gy, n_gz = mesh_shape
    fb, fw, za, zb = refs[:4]
    send, v0w, w0w, v0h, w0h, g0, v1m, v1s, w1m, w1s, g1m, g1s = refs[4:16]
    gm, gs, vm, vs, ws, tm, ts, um, us, small = refs[16:]
    extent, rows = fb.shape[0], fb.shape[1]
    tall = g0.shape[0]
    wide = g0.shape[1]
    half, half_rows = extent // 2, rows // 2
    _, own, _ = x_frame(n_gx, tall)
    groups = extent // HALO
    zero = jnp.zeros((8, 128), F32)

    def clear(ref, count, depth):
        for x in (0, count + 1):
            for r in range(0, depth + 16, 8):
                ref[x, r : r + 8, :] = zero
        for x in range(1, count + 1):
            ref[x, 0:8, :] = zero
            ref[x, depth + 8 : depth + 16, :] = zero

    for ref in (gm, gs, vm, vs):
        clear(ref, extent, rows)
    for ref in (v1m, v1s, g1m, g1s, w1m, w1s):
        clear(ref, half, half_rows)

    lane = iota((rows, 128), 1)
    ends = z_ends(n_gz)
    masks = [((lane >= e["lane"]) & (lane < e["lane"] + HALO)).astype(F32) * e["valid"].astype(F32) for e in ends]

    def load(group):
        for i in range(HALO):
            x = group * HALO + i
            sides = []
            for a in range(2):
                total = None
                for ref, mask, end in zip((za, zb), masks, ends):
                    piece = roll(ref[group], end["lane"] - 16 * i - 8 * a) * mask
                    total = piece if total is None else total + piece
                sides.append(total)
            ws[x] = sides[1]
            gm[x + 1, 8 : 8 + rows, :] = K * fb[x] * inverse(fw[x])
            gs[x + 1, 8 : 8 + rows, :] = K * sides[0] * inverse(sides[1])

    each(groups, load, 4)

    def second(x):
        main, side, main_n, side_n = neighbours(gm, gs, x + 1, 8, rows, 1)
        vm[x + 1, 8 : 8 + rows, :] = 1.2 * main + jnp.where(fw[x] > 0.0, K * main_n, 0.0)
        vs[x + 1, 8 : 8 + rows, :] = 1.2 * side + jnp.where(ws[x] > 0.0, K * side_n, 0.0)

    each(extent, second, 8)

    def residual(x2):
        totals = None
        for j in range(2):
            x = 2 * x2 + j
            main, side, main_n, side_n = neighbours(vm, vs, x + 1, 8, rows, 1)
            w_main, w_side = fw[x], ws[x]
            r_main = w_main * ((1.0 / K) * gm[x + 1, 8 : 8 + rows, :] - 6.0 * main + main_n)
            r_side = w_side * ((1.0 / K) * gs[x + 1, 8 : 8 + rows, :] - 6.0 * side + side_n)
            values = (r_main, r_side, w_main, w_side)
            totals = values if j == 0 else tuple(a + b for a, b in zip(totals, values))
        for ref, value in zip((tm, ts, um, us), totals):
            ref[x2] = value

        def pairs(ref):
            return lane_pairs(ref[x2, pl.ds(0, half_rows, stride=2), :] + ref[x2, pl.ds(1, half_rows, stride=2), :], 1)

        for t_ref, u_ref, w_out, g_out in ((tm, um, w1m, g1m), (ts, us, w1s, g1s)):
            weights = 0.0625 * pairs(u_ref)
            w_out[x2 + 1, 8 : 8 + half_rows, :] = weights
            g_out[x2 + 1, 8 : 8 + half_rows, :] = (0.125 * K) * pairs(t_ref) * inverse(weights)

    each(half, residual, 4)

    def second_1(x):
        main, side, main_n, side_n = neighbours(g1m, g1s, x + 1, 8, half_rows, 2)
        v1m[x + 1, 8 : 8 + half_rows, :] = 1.2 * main + jnp.where(w1m[x + 1, 8 : 8 + half_rows, :] > 0.0, K * main_n, 0.0)
        v1s[x + 1, 8 : 8 + half_rows, :] = 1.2 * side + jnp.where(w1s[x + 1, 8 : 8 + half_rows, :] > 0.0, K * side_n, 0.0)

    each(half, second_1, 16)

    base = own // 2
    first_row = 8 + HALO // 2
    quarter, quarter_rows = tall // 4, wide // 4
    for x2 in range(quarter):
        total_r = total_w = None
        for j in range(2):
            x = base + 2 * x2 + j + 1
            main, _, main_n, _ = neighbours(v1m, v1s, x, first_row, wide // 2, 2)
            weights = w1m[x, pl.ds(first_row, wide // 2), :]
            res = weights * ((1.0 / K) * g1m[x, pl.ds(first_row, wide // 2), :] - 6.0 * main + main_n)
            total_r = res if j == 0 else total_r + res
            total_w = weights if j == 0 else total_w + weights
        small[0, x2] = total_r
        small[1, x2] = total_w
    q = []
    for a, factor in ((0, 0.125), (1, 0.0625)):
        for x2 in range(quarter):
            ref = small.at[a, x2]
            both = ref[pl.ds(0, quarter_rows, stride=2), :] + ref[pl.ds(1, quarter_rows, stride=2), :]
            q.append(factor * lane_pairs(both, 2))
    stacked = jnp.concatenate([jnp.concatenate(q[:quarter], axis=0), jnp.concatenate(q[quarter:], axis=0)], axis=0)
    src, dst = iota((128, 128), 0), iota((128, 128), 1)
    pick = (src == 4 * (dst % 32)).astype(F32)
    compact = jnp.dot(stacked, pick, precision=lax.Precision.HIGHEST, preferred_element_type=F32)
    block = iota((quarter_rows, 128), 1) // 32
    gz = lax.axis_index("gz")
    out = []
    for a in range(2):
        packed = jnp.zeros((quarter_rows, 128), F32)
        for x2 in range(quarter):
            r = (a * quarter + x2) * quarter_rows
            packed = jnp.where(block == lax.rem(gz + x2, 4), compact[r : r + quarter_rows], packed)
        out.append(packed)
    message = jnp.concatenate(out, axis=0)

    def copy(d):
        send[d] = message

    each(send.shape[0], copy, 8)

    for i in range(tall + 2):
        v0w[i] = vm[own + i, 8 : 8 + rows, :]
        x = own + (i - 1)
        inside = (x >= 0) & (x < extent)
        w0w[i] = keep(inside, fw[jnp.clip(x, 0, extent - 1)])
    for i in range(tall):
        v0h[i] = vs[own + i + 1, 8 + HALO : 8 + HALO + wide, :]
        w0h[i] = ws[own + i, HALO : HALO + wide, :]
        g0[i] = gm[own + i + 1, 8 + HALO : 8 + HALO + wide, :]


def up_kernel(mesh_shape, *refs):
    n_gx, n_gy, n_gz = mesh_shape
    recv, rows_ref, za, zb, v0w, w0w, v0h, w0h, g0, v1m, v1s, w1m, w1s, g1m, g1s, out = refs[:16]
    g2, w2, v2, y2, e2, p2, t3, u3, g3, w3, v3, y3, p3, b4, col, y1m, y1s, e1m, e1s, f1m, f1s, y0m, y0s = refs[16:]
    tall, wide = out.shape[0], out.shape[1]
    size_x, size_z = w2.shape[0], w2.shape[2]
    size_y = w2.shape[1]
    ix, own, _ = x_frame(n_gx, tall)
    iy, iz = lax.axis_index("gy"), lax.axis_index("gz")
    quarter, quarter_rows = tall // 4, wide // 4
    extent = frame_extent(n_gx, tall)
    half, half_rows = v1m.shape[0] - 2, v1m.shape[1] - 16

    def clear(ref):
        count, depth, size = ref.shape
        zero = jnp.zeros((8, size), F32)
        for x in range(count):
            ref[x, 0:8, :] = zero
            ref[x, depth - 8 : depth, :] = zero
        for x in (0, count - 1):
            ref[x] = jnp.zeros((depth, size), F32)

    for ref in (g2, v2, y2, g3, v3, y3):
        clear(ref)
    e2[...] = jnp.zeros(e2.shape, F32)
    p3[...] = jnp.zeros(p3.shape, F32)

    lane = iota((quarter_rows, 128), 1)
    block = lane // 32
    for gx in range(n_gx):
        for gy in range(n_gy):
            for x in range(quarter):
                tiles_b, tiles_w = [], []
                for tile in range(size_z // 128):
                    picked = [jnp.zeros((quarter_rows, 128), F32)] * 2
                    for j in range(4):
                        gz = tile * 4 + j
                        d = (gx * n_gy + gy) * n_gz + gz
                        mask = block == (gz + x) % 4
                        for a in range(2):
                            piece = recv[d, a * quarter_rows : (a + 1) * quarter_rows, :]
                            picked[a] = jnp.where(mask, piece, picked[a])
                    tiles_b.append(roll(picked[0], -32 * x))
                    tiles_w.append(roll(picked[1], -32 * x))
                weights = joined(tiles_w)
                w2[gx * quarter + x, gy * quarter_rows : (gy + 1) * quarter_rows, :] = weights
                g2[gx * quarter + x + 1, 8 + gy * quarter_rows : 8 + (gy + 1) * quarter_rows, :] = K * joined(tiles_b) / weights

    def smooth(g, v, x, rows, step):
        main, near = global_neighbours(g, x + 1, 8, rows, step)
        v[x + 1, 8 : 8 + rows, :] = 1.2 * main + K * near

    def resid(g, v, w, x, rows, step):
        main, near = global_neighbours(v, x + 1, 8, rows, step)
        return w[x] * ((1.0 / K) * g[x + 1, 8 : 8 + rows, :] - 6.0 * main + near)

    each(size_x, lambda x: smooth(g2, v2, x, size_y, 1), 8)
    rows3, x3 = size_y // 2, size_x // 2

    def restrict_2(x):
        for t, part in enumerate(tiled(resid(g2, v2, w2, 2 * x, size_y, 1) + resid(g2, v2, w2, 2 * x + 1, size_y, 1))):
            t3[t] = part
        for t, part in enumerate(tiled(w2[2 * x] + w2[2 * x + 1])):
            u3[t] = part
        pairs = lambda ref: lane_pairs(row_pairs(ref, size_y), 1)
        weights = 0.0625 * pairs(u3)
        w3[x] = weights
        g3[x + 1, 8 : 8 + rows3, :] = (0.125 * K) * pairs(t3) / weights

    each(x3, restrict_2, 4)
    each(x3, lambda x: smooth(g3, v3, x, rows3, 2), 8)
    rows4, x4 = rows3 // 2, x3 // 2

    def restrict_3(x):
        for t, part in enumerate(tiled(resid(g3, v3, w3, 2 * x, rows3, 2) + resid(g3, v3, w3, 2 * x + 1, rows3, 2))):
            t3[t, 0:rows3, :] = part
        b4[x] = 0.125 * lane_pairs(row_pairs(t3, rows3), 2)

    each(x4, restrict_3, 4)

    tiles = rows_ref.shape[0] // 9
    coarse_z = size_z // 4
    per = 128 // coarse_z
    src, dst = iota((size_z, 128), 0), iota((size_z, 128), 1)
    pick = (src == 4 * (dst % coarse_z)).astype(F32)
    values = b4[0] if x4 == 1 else jnp.concatenate([b4[x] for x in range(x4)], axis=0)
    compact = jnp.dot(values, pick, precision=lax.Precision.HIGHEST, preferred_element_type=F32)
    place = iota((x4 * rows4, 128), 0) % per == iota((x4 * rows4, 128), 1) // coarse_z
    compact = jnp.where(place, compact, 0.0)
    vectors = [jnp.sum(compact[t * per : (t + 1) * per], axis=0, keepdims=True) for t in range(tiles)]
    ends = z_ends(n_gz)
    groups = extent // HALO
    fine = iota((HALO, size_z), 1) // 4
    fine_row = fine == iz * HALO + iota((HALO, size_z), 0)
    edge_row = iota((16, 128), 0)
    first_total = [None, None]
    for k, ref in enumerate((za, zb)):
        total = None
        for t in range(tiles):
            piece = ref[groups + t // 2, 16 * (t % 2) : 16 * (t % 2) + 16, :] * vectors[t]
            total = piece if total is None else total + piece
        first_total[k] = jnp.sum(total, axis=1, keepdims=True) * ends[k]["valid"].astype(F32)
    z_lane = iota((16, size_z), 1) // 4
    spread = None
    for k in range(2):
        piece = jnp.where(z_lane == iz * HALO + ends[k]["row"], first_total[k], 0.0)
        spread = piece if spread is None else spread + piece
    for m in range(9):
        total = None
        for t in range(tiles):
            piece = rows_ref[m * tiles + t] * vectors[t]
            total = piece if total is None else total + piece
        values = jnp.sum(total, axis=1, keepdims=True)
        line = jnp.sum(jnp.where(fine_row, values, 0.0), axis=0, keepdims=True) + spread[m : m + 1, :]
        row = 8 + 2 * (iy + (m % 3 - 1))
        for t, part in enumerate(tiled(line)):
            p3[ix + m // 3, t, pl.ds(row, 1), :] = part
            p3[ix + m // 3, t, pl.ds(row + 1, 1), :] = part

    def lift(y, v, w, p, x, px, rows, row):
        coarse = joined([p[px, t, row : row + rows, :] for t in range(p.shape[1])])
        y[x + 1, 8 : 8 + rows, :] = v[x + 1, 8 : 8 + rows, :] + w[x] * coarse

    def relax(y, g, w, x, rows, step):
        main, near = global_neighbours(y, x + 1, 8, rows, step)
        return (0.2 * main + g[x + 1, 8 : 8 + rows, :] + K * near) / w[x]

    each(x3, lambda x: lift(y3, v3, w3, p3, x, x // 2 + 1, rows3, 8), 8)

    def up_3(x):
        for t, e3 in enumerate(tiled(relax(y3, g3, w3, x, rows3, 2))):
            p2[x, t, pl.ds(0, rows3, stride=2), :] = e3
            p2[x, t, pl.ds(1, rows3, stride=2), :] = e3

    each(x3, up_3, 4)
    each(size_x, lambda x: lift(y2, v2, w2, p2, x, x // 2, size_y, 0), 8)

    def up_2(x):
        for t, part in enumerate(tiled(relax(y2, g2, w2, x, size_y, 1))):
            e2[x + 2, t, 8 : 8 + size_y, :] = part

    each(size_x, up_2, 8)

    src, dst = iota((size_z, 256), 0), iota((size_z, 256), 1)
    start = iz * 32
    cell = jnp.where(dst < 128, dst // 4, jnp.where(dst < 192, 32 + (dst - 128) // 4, -1 - (255 - dst) // 4))
    widen = (src == start + cell).astype(F32)
    n2 = extent // 4
    x_start = ix * quarter - own // 4
    y_start = 8 + iy * quarter_rows - HALO // 4
    spread = None
    for t in range(size_z // 128):
        stacked = jnp.concatenate([e2[x_start + 2 + i, t, pl.ds(y_start, 8), :] for i in range(n2)], axis=0)
        part = jnp.dot(stacked, widen[t * 128 : (t + 1) * 128], precision=lax.Precision.HIGHEST, preferred_element_type=F32)
        spread = part if spread is None else spread + part
    for i in range(n2):
        for ref, part in ((e1m, spread[i * 8 : i * 8 + 8, :128]), (e1s, spread[i * 8 : i * 8 + 8, 128:])):
            ref[i, pl.ds(0, 8, stride=2), :] = part
            ref[i, pl.ds(1, 8, stride=2), :] = part

    clear(y1m)
    clear(y1s)
    inner = slice(8, 8 + half_rows)
    for x in range(half):
        y1m[x + 1, inner, :] = v1m[x + 1, inner, :] + w1m[x + 1, inner, :] * e1m[x // 2]
        y1s[x + 1, inner, :] = v1s[x + 1, inner, :] + w1s[x + 1, inner, :] * e1s[x // 2]

    def up_1(x):
        main, side, main_n, side_n = neighbours(y1m, y1s, x + 1, 8, half_rows, 2)
        for f, y, near, g, w in ((f1m, main, main_n, g1m, w1m), (f1s, side, side_n, g1s, w1s)):
            e1 = (0.2 * y + g[x + 1, inner, :] + K * near) * inverse(w[x + 1, inner, :])
            f[x, pl.ds(0, half_rows, stride=2), :] = e1
            f[x, pl.ds(1, half_rows, stride=2), :] = e1

    each(half, up_1, 12)
    base = own // 2
    for i in range(tall + 2):
        parent = jnp.clip(base + (i + 1) // 2 - 1, 0, half - 1)
        y0m[i] = v0w[i] + w0w[i] * f1m[parent]
        if 0 < i <= tall:
            y0s[i - 1] = v0h[i - 1] + w0h[i - 1] * f1s[parent, HALO : HALO + wide, :]

    def up_0(i):
        main = y0m[i + 1, pl.ds(HALO, wide), :]
        main_z, _ = z_sum(main, y0s[i], 1)
        near = xy_sum(y0m, i + 1, HALO, wide) + main_z
        out[i] = (0.2 * main + g0[i] + K * near) / w0w[i + 1, HALO : HALO + wide, :]

    each(tall, up_0, 16)


def size_of(shape):
    return 4 * math.prod(shape)


def call(kernel, outs, scratch=(), resident=True, fetch=False):
    limit = 8 * 2**20 + sum(map(size_of, scratch)) + sum(size_of(s) for s in outs if size_of(s) > 2**20)
    run = pl.pallas_call(
        kernel,
        out_shape=[(pltpu.VMEM if resident and size_of(s) <= 2**20 else jax.ShapeDtypeStruct)(s, F32) for s in outs],
        scratch_shapes=[pltpu.VMEM(s, F32) for s in scratch],
        compiler_params=pltpu.CompilerParams(vmem_limit_bytes=min(limit, 56 * 2**20)),
    )

    def place(value):
        small = size_of(value.shape) <= 2**20 and not fetch
        return pltpu.with_memory_space_constraint(value, pltpu.VMEM if small else pltpu.HBM)

    return lambda *values: run(*map(place, values))


def plain_halo(mesh_shape, own, frames):
    n_gx = mesh_shape[0]
    tall = own[0].shape[0]
    extent, tiles = frames[0][0], own[2].shape[1] // 128
    parts = ()
    if n_gx > 1:
        odd = lax.axis_index("gx") % 2
        for first in range(2):
            start = jnp.where(odd == first, tall - HALO, 0)
            faces = [lax.dynamic_slice_in_dim(a, start, HALO, 0) for a in own[:2]] + [own[2]]
            parts += tuple(swap(a, "gx", first) for a in faces)
    slab = (2 * extent + 3 * tiles, HALO, 128)
    y_slabs = call(functools.partial(y_pack_kernel, mesh_shape), [slab, slab])(*own, *parts)
    y_parts = [swap(s, "gy", first) for first, s in enumerate(y_slabs)]
    fb, fw, matrix, z_a, z_b = call(functools.partial(z_pack_kernel, mesh_shape), frames)(*own, *parts, *y_parts)
    return fb, fw, matrix, ring(z_a, "gz", 1), ring(z_b, "gz", -1)


def shared_halo(mesh_shape, own, frames):
    tall, wide = own[0].shape[:2]
    tiles = own[2].shape[1] // 128
    strips, groups, per = (tiles + 7) // 8, tall // HALO, wide // 8
    z_shape = (groups * per + strips, HALO, 128)
    y_shape = (2 * tall + tiles + 2 * (groups + strips), HALO, 128)
    x_shape = (2 * per * tall + tiles + 2 * z_shape[0], HALO, 128)
    z_tail, z_head, *here = call(z_face_kernel, [z_shape, z_shape] + [a.shape for a in own], fetch=True)(*own)
    z_got = lax.optimization_barrier((ring(z_tail, "gz", 1), ring(z_head, "gz", -1)))
    y_first, y_second, x_own = call(y_face_kernel, [y_shape, y_shape, x_shape])(*here, *z_got)
    y_got = (swap(y_first, "gy", 0), swap(y_second, "gy", 1))
    other = swap(x_own, "gx", 0)
    y_got = lax.optimization_barrier(y_got)
    y_other = [swap(y, "gx", 0) for y in y_got]
    return call(functools.partial(frame_kernel, mesh_shape), frames)(*here, other, *z_got, *y_got, *y_other)


def per_device(mesh_shape, sources, stiffness, coarse_inverse):
    n_gx, n_gy, n_gz = mesh_shape
    count = n_gx * n_gy * n_gz
    tall, wide, deep = stiffness.shape
    cells = coarse_inverse.shape[1]
    assert sources.shape[0] == 1 and deep == 128 and tall == 16 and wide == 16 and n_gz % 4 == 0 and cells % 128 == 0
    tiles = cells // 128
    extent = frame_extent(n_gx, tall)
    source = sources[0]
    own = (source, stiffness, coarse_inverse)
    rows = wide + 2 * HALO
    frame = (extent, rows, 128)
    z_slab = (extent // HALO + (tiles + 1) // 2, rows, 128)
    frames = [frame, frame, (9 * tiles, HALO, 128), z_slab, z_slab]
    exchange = shared_halo if n_gx == 2 else plain_halo
    fb, fw, matrix, z_a, z_b = exchange(mesh_shape, own, frames)
    padded = (extent + 2, rows + 16, 128)
    half, half_rows = extent // 2, rows // 2
    level1 = (half + 2, half_rows + 16, 128)
    window, face = (tall + 2, rows, 128), (tall, wide, 128)
    message = (count, wide // 2, 128)
    outs = [message, window, window, face, face, face] + [level1] * 6
    scratch = [padded] * 4 + [frame] + [(half, rows, 128)] * 4 + [(2, tall // 4, wide // 2, 128)]
    send, *state = call(functools.partial(down_kernel, mesh_shape), outs, scratch)(fb, fw, z_a, z_b)
    recv = lax.all_to_all(send, AXES, 0, 0, tiled=True)
    size_x, size_y, size_z = n_gx * tall // 4, n_gy * wide // 4, n_gz * deep // 4
    pad2 = (size_x + 2, size_y + 16, size_z)
    x3, rows3 = size_x // 2, size_y // 2
    pad3 = (x3 + 2, rows3 + 16, size_z)
    n2, lane_tiles = extent // 4, size_z // 128
    scratch = [
        pad2, (size_x, size_y, size_z), pad2, pad2, (size_x + 4, lane_tiles, size_y + 16, 128), (x3, lane_tiles, size_y, 128),
        (lane_tiles, size_y, 128), (lane_tiles, size_y, 128), pad3, (x3, rows3, size_z), pad3, pad3,
        (x3 // 2 + 2, lane_tiles, rows3 + 16, 128),
        (x3 // 2, rows3 // 2, size_z), (8, 128), level1, level1, (n2, 16, 128), (n2, 16, 128),
        (half, rows, 128), (half, rows, 128), window, face,
    ]
    (pressure,) = call(functools.partial(up_kernel, mesh_shape), [face], scratch, False)(recv, matrix, z_a, z_b, *state)
    return pressure[None]


def solution(mesh):
    mesh_shape = tuple(mesh.shape[a] for a in AXES)
    in_specs = (P(None, "gx", "gy", "gz"), P("gx", "gy", "gz"), P(AXES, None))
    return jax.shard_map(
        functools.partial(per_device, mesh_shape),
        mesh=mesh,
        in_specs=in_specs,
        out_specs=P(None, "gx", "gy", "gz"),
        check_vma=False,
    )
```

```python
import functools
import math

import jax
import jax.numpy as jnp
from jax import lax
from jax.experimental import pallas as pl
from jax.experimental.pallas import tpu as pltpu
from jax.sharding import PartitionSpec as P


damping = 0.8
K = damping / 6.0
AXES = ("gx", "gy", "gz")
HALO = 8
F32 = jnp.float32


def swap(values, axis, first):
    count = lax.axis_size(axis)
    partner = list(range(count))
    for i in range(first, count - 1, 2):
        partner[i], partner[i + 1] = i + 1, i
    return lax.ppermute(values, axis, list(enumerate(partner)))


def ring(values, axis, step):
    count = lax.axis_size(axis)
    return lax.ppermute(values, axis, [(i, (i + step) % count) for i in range(count)])


def iota(shape, dim):
    return lax.broadcasted_iota(jnp.int32, shape, dim)


def roll(values, amount):
    size = values.shape[-1]
    if isinstance(amount, int):
        amount = amount % size
        if amount == 0:
            return values
    return pltpu.roll(values, amount, values.ndim - 1)


def z_sum(main, side, step):
    lane = iota(main.shape, main.ndim - 1)
    size = main.shape[-1]
    main_up, side_up = roll(main, -step), roll(side, -step)
    main_dn, side_dn = roll(main, step), roll(side, step)
    last = lane >= size - step
    first = lane < step
    main_sum = jnp.where(last, side_up, main_up) + jnp.where(first, side_dn, main_dn)
    side_sum = jnp.where(last, main_up, side_up) + jnp.where(first, main_dn, side_dn)
    return main_sum, side_sum


def xy_sum(ref, x, row, rows):
    total = ref[x - 1, pl.ds(row, rows), :] + ref[x + 1, pl.ds(row, rows), :]
    return total + ref[x, pl.ds(row - 1, rows), :] + ref[x, pl.ds(row + 1, rows), :]


def neighbours(main_ref, side_ref, x, row, rows, step):
    main = main_ref[x, pl.ds(row, rows), :]
    side = side_ref[x, pl.ds(row, rows), :]
    main_z, side_z = z_sum(main, side, step)
    return main, side, xy_sum(main_ref, x, row, rows) + main_z, xy_sum(side_ref, x, row, rows) + side_z


def global_neighbours(ref, x, row, rows, step):
    main = ref[x, pl.ds(row, rows), :]
    lane = iota(main.shape, 1)
    size = main.shape[-1]
    up = jnp.where(lane >= size - step, 0.0, roll(main, -step))
    dn = jnp.where(lane < step, 0.0, roll(main, step))
    return main, xy_sum(ref, x, row, rows) + up + dn


def lane_pairs(values, step):
    lane = iota(values.shape, values.ndim - 1)
    return values + jnp.where((lane // step) % 2 == 0, roll(values, -step), roll(values, step))


def inverse(weights):
    return jnp.where(weights > 0.0, 1.0 / jnp.where(weights > 0.0, weights, 1.0), 0.0)


def tiled(value):
    return [value[:, t * 128 : (t + 1) * 128] for t in range(value.shape[1] // 128)]


def joined(parts):
    return parts[0] if len(parts) == 1 else jnp.concatenate(parts, axis=1)


def row_pairs(ref, rows):
    return joined([ref[t, pl.ds(0, rows // 2, stride=2), :] + ref[t, pl.ds(1, rows // 2, stride=2), :] for t in range(ref.shape[0])])


def each(count, body, width=1):
    while count % width:
        width -= 1
    if count == width:
        for i in range(count):
            body(i)
        return

    def step(i, carry):
        for j in range(width):
            body(i * width + j)
        return carry

    lax.fori_loop(0, count // width, step, 0)


def pair_places(axis, count, own, tall):
    index = lax.axis_index(axis)
    odd = index % 2
    first = dict(place=jnp.where(odd == 0, own + tall, 0), high=odd == 0, valid=jnp.where(odd == 0, index + 1, index - 1) < count)
    other = jnp.where(odd == 0, index - 1, index + 1)
    second = dict(place=jnp.where(odd == 0, 0, own + tall), high=odd == 1, valid=(other >= 0) & (other < count))
    return index, odd, (first, second)


def x_frame(count, tall):
    index = lax.axis_index("gx")
    odd = index % 2
    if count == 1:
        return index, 0, ()
    own = HALO * odd if count == 2 else HALO
    _, _, (first, second) = pair_places("gx", count, own, tall)
    if count == 2:
        first["source"] = jnp.where(odd == 0, 0, tall - HALO)
        return index, own, (first,)
    first["source"] = second["source"] = 0
    return index, own, (first, second)


def y_ends(count, wide):
    index = lax.axis_index("gy")
    return (dict(valid=index > 0, place=0, high=0), dict(valid=index < count - 1, place=wide + HALO, high=1))


def frame_extent(count, tall):
    return tall + (0 if count == 1 else HALO if count == 2 else 2 * HALO)


def keep(valid, values):
    return jnp.where(valid, values, jnp.zeros_like(values))


def y_pack_kernel(mesh_shape, *refs):
    n_gx, _, _ = mesh_shape
    n_in = 3 * (1 + min(n_gx - 1, 2))
    own_refs, part_refs, outs = refs[:3], refs[3:n_in], refs[n_in:]
    tall, wide = own_refs[0].shape[0], own_refs[0].shape[1]
    extent = frame_extent(n_gx, tall)
    tiles = own_refs[2].shape[1] // 128
    _, own, parts = x_frame(n_gx, tall)
    for out, start in zip(outs, (wide - HALO, 0)):
        rows = pl.ds(start, HALO)
        for a in range(2):
            out[pl.ds(a * extent + own, tall)] = own_refs[a][:, rows, :]
            for part, ref in zip(parts, (part_refs[a : a + 1], part_refs[3 + a : 4 + a])):
                out[pl.ds(a * extent + part["place"], HALO)] = keep(part["valid"], ref[0][pl.ds(part["source"], HALO), rows, :])
        base = 2 * extent
        for side in (0, 2):
            for t in range(tiles):
                out[base + side * tiles + t] = jnp.zeros((HALO, 128), F32)
        for t in range(tiles):
            out[base + tiles + t] = own_refs[2][:, t * 128 : (t + 1) * 128]
            for part, ref in zip(parts, (part_refs[2:3], part_refs[5:6])):
                side = jnp.where(part["high"], 2, 0)
                out[base + side * tiles + t] = keep(part["valid"], ref[0][:, t * 128 : (t + 1) * 128])


def z_pack_kernel(mesh_shape, *refs):
    n_gx, n_gy, _ = mesh_shape
    n_in = 3 * (1 + min(n_gx - 1, 2))
    own_refs, part_refs = refs[:3], refs[3:n_in]
    y_refs = refs[n_in : n_in + 2]
    frames = refs[n_in + 2 : n_in + 4]
    rows_ref, z_outs = refs[n_in + 4], refs[n_in + 5 :]
    tall, wide = own_refs[0].shape[0], own_refs[0].shape[1]
    extent = frame_extent(n_gx, tall)
    tiles = own_refs[2].shape[1] // 128
    _, own, parts = x_frame(n_gx, tall)
    y_parts = y_ends(n_gy, wide)
    for a in range(2):
        frames[a][pl.ds(own, tall), HALO : HALO + wide, :] = own_refs[a][...]
        for part, ref in zip(parts, (part_refs[a : a + 1], part_refs[3 + a : 4 + a])):
            frames[a][pl.ds(part["place"], HALO), HALO : HALO + wide, :] = keep(part["valid"], ref[0][pl.ds(part["source"], HALO)])
        for part, ref in zip(y_parts, y_refs):
            rows = pl.ds(part["place"], HALO)
            frames[a][:, rows, :] = keep(part["valid"], ref[a * extent : (a + 1) * extent])
    for t in range(tiles):
        for side in (0, 2):
            rows_ref[(side * 3 + 1) * tiles + t] = jnp.zeros((HALO, 128), F32)
        rows_ref[4 * tiles + t] = own_refs[2][:, t * 128 : (t + 1) * 128]
        for part, ref in zip(parts, (part_refs[2:3], part_refs[5:6])):
            side = jnp.where(part["high"], 2, 0)
            rows_ref[(side * 3 + 1) * tiles + t] = keep(part["valid"], ref[0][:, t * 128 : (t + 1) * 128])
        for x_side in range(3):
            for part, ref in zip(y_parts, y_refs):
                side = 2 * part["high"]
                rows_ref[(x_side * 3 + side) * tiles + t] = keep(part["valid"], ref[2 * extent + x_side * tiles + t])
    groups = extent // HALO
    for out, tail in zip(z_outs, (1, 0)):

        def put(group, packed):
            out[group] = packed

        pack_z(frames, put, tail)
        row = (HALO - 1) * tail
        for s in range((tiles + 1) // 2):
            out[groups + s] = jnp.zeros((4 * HALO, 128), F32)
        for t in range(tiles):
            for m in range(9):
                out[groups + t // 2, 16 * (t % 2) + m : 16 * (t % 2) + m + 1, :] = rows_ref[m * tiles + t, row : row + 1, :]


def z_ends(count):
    index = lax.axis_index("gz")
    return (dict(valid=index > 0, lane=120, row=-1), dict(valid=index < count - 1, lane=0, row=HALO))


def pack_z(frames, out, tail):
    rows = frames[0].shape[1]
    slot = iota((rows, 128), 1) // HALO
    for group in range(frames[0].shape[0] // HALO):
        packed = jnp.zeros((rows, 128), F32)
        for i in range(HALO):
            for a in range(2):
                piece = roll(frames[a][group * HALO + i], 8 * (tail + 2 * i + a))
                packed = jnp.where(slot == 2 * i + a, piece, packed)
        out(group, packed)


def face_kernel(*refs):
    b, w, matrix, *outs = refs
    outs, y_outs, both, copies = outs[:2], outs[2:4], outs[4], outs[5:]
    tall, wide = b.shape[0], b.shape[1]
    tiles = matrix.shape[1] // 128
    strips = (tiles + 7) // 8
    per = wide // 8
    for out, tail in zip(outs, (1, 0)):

        def put(group, packed):
            for r in range(per):
                out[group * per + r] = packed[8 * r : 8 * r + 8]

        pack_z((b, w), put, tail)
        at = tall // HALO * per
        line = matrix[HALO - 1 : HALO, :] if tail else matrix[0:1, :]
        for strip in range(strips):
            out[at + strip] = jnp.zeros((8, 128), F32)
        for t in range(tiles):
            out[at + t // 8, t % 8 : t % 8 + 1, :] = line[:, t * 128 : (t + 1) * 128]
    for out, row in zip(y_outs, (wide - HALO, 0)):
        for a, ref in enumerate((b, w)):
            out[a * tall : (a + 1) * tall] = ref[:, row : row + HALO, :]
        for t in range(tiles):
            out[2 * tall + t] = matrix[:, t * 128 : (t + 1) * 128]
    at = 0
    for ref in (b, w):
        for r in range(per):
            both[at : at + tall] = ref[:, 8 * r : 8 * r + 8, :]
            at += tall
    for t in range(tiles):
        both[at + t] = matrix[:, t * 128 : (t + 1) * 128]
    for ref, copy in zip((b, w, matrix), copies):
        copy[...] = ref[...]


def y_edge_kernel(groups, per, *refs):
    z_refs, outs, both = refs[:2], refs[2:4], refs[4]
    size = z_refs[0].shape[0]
    strips = size - groups * per
    for out, r in zip(outs, (per - 1, 0)):
        for k, ref in enumerate(z_refs):
            at = k * (groups + strips)
            for group in range(groups):
                out[at + group] = ref[group * per + r]
            out[at + groups : at + groups + strips] = ref[groups * per : size]
    for k, ref in enumerate(z_refs):
        both[k * size : (k + 1) * size] = ref[...]


def frame_kernel(mesh_shape, *refs):
    n_gx, n_gy, _ = mesh_shape
    own_refs, other, z_refs, z_other = refs[:3], refs[3], refs[4:6], refs[6]
    y_refs, y_others, edge_refs, edge_others = refs[7:9], refs[9:11], refs[11:13], refs[13:15]
    frames, rows_ref, z_outs = refs[15:17], refs[17], refs[18:]
    tall, wide = own_refs[0].shape[0], own_refs[0].shape[1]
    extent = frame_extent(n_gx, tall)
    tiles = own_refs[2].shape[1] // 128
    strips, groups, per = (tiles + 7) // 8, tall // HALO, wide // 8
    _, own, parts = x_frame(n_gx, tall)
    place, source = parts[0]["place"], parts[0]["source"]
    y_parts = y_ends(n_gy, wide)
    far = jnp.where(parts[0]["high"], 2, 0)
    y_rows = [pl.ds(p["place"], HALO) for p in y_parts]
    y_side = [2 * p["high"] for p in y_parts]
    for a in range(2):
        frames[a][pl.ds(own, tall), HALO : HALO + wide, :] = own_refs[a][...]
        for r in range(per):
            rows = slice(HALO + 8 * r, HALO + 8 * r + 8)
            frames[a][pl.ds(place, HALO), rows, :] = other[pl.ds((a * per + r) * tall + source, HALO)]
        for part, rows, ref, ref_other in zip(y_parts, y_rows, y_refs, y_others):
            frames[a][pl.ds(own, tall), rows, :] = keep(part["valid"], ref[a * tall : (a + 1) * tall])
            frames[a][pl.ds(place, HALO), rows, :] = keep(part["valid"], ref_other[pl.ds(a * tall + source, HALO)])
    zero = jnp.zeros((HALO, 128), F32)
    for t in range(tiles):
        for side in range(3):
            rows_ref[((2 - far) * 3 + side) * tiles + t] = zero
        rows_ref[4 * tiles + t] = own_refs[2][:, t * 128 : (t + 1) * 128]
        rows_ref[(far * 3 + 1) * tiles + t] = other[2 * per * tall + t]
        for part, side, ref, ref_other in zip(y_parts, y_side, y_refs, y_others):
            rows_ref[(3 + side) * tiles + t] = keep(part["valid"], ref[2 * tall + t])
            rows_ref[(far * 3 + side) * tiles + t] = keep(part["valid"], ref_other[2 * tall + t])
    for k, (out, ref) in enumerate(zip(z_outs, z_refs)):
        base = k * (groups * per + strips)
        y_base = k * (groups + strips)
        total = extent // HALO
        for s in range((tiles + 1) // 2):
            out[total + s] = jnp.zeros((4 * HALO, 128), F32)
        for g in range(groups):
            for r in range(per):
                out[own // HALO + g, HALO + 8 * r : HALO + 8 * r + 8, :] = ref[g * per + r]
            for part, rows, y_ref in zip(y_parts, y_rows, edge_refs):
                out[own // HALO + g, rows, :] = keep(part["valid"], y_ref[y_base + g])
        for r in range(per):
            out[place // HALO, HALO + 8 * r : HALO + 8 * r + 8, :] = z_other[base + source // HALO * per + r]
        for part, rows, y_ref in zip(y_parts, y_rows, edge_others):
            out[place // HALO, rows, :] = keep(part["valid"], y_ref[y_base + source // HALO])
        for strip in range(strips):
            for x_side in range(3):
                if x_side == 1:
                    middle = ref[groups * per + strip]
                    edges = [keep(p["valid"], r[y_base + groups + strip]) for p, r in zip(y_parts, edge_refs)]
                else:
                    here = far == x_side
                    middle = keep(here, z_other[base + groups * per + strip])
                    edges = [keep(p["valid"] & here, r[y_base + groups + strip]) for p, r in zip(y_parts, edge_others)]
                low, high = edges
                for j in range(min(8, tiles - 8 * strip)):
                    t = 8 * strip + j
                    for side, values in enumerate((low, middle, high)):
                        m = 16 * (t % 2) + x_side * 3 + side
                        out[total + t // 2, m : m + 1, :] = values[j : j + 1]


def down_kernel(mesh_shape, *refs):
    n_gx, _, n_gz = mesh_shape
    fb, fw, za, zb = refs[:4]
    send, v0w, w0w, v0h, w0h, g0, v1m, v1s, w1m, w1s, g1m, g1s = refs[4:16]
    gm, gs, vm, vs, ws, tm, ts, um, us, small = refs[16:]
    extent, rows = fb.shape[0], fb.shape[1]
    tall = g0.shape[0]
    wide = g0.shape[1]
    half, half_rows = extent // 2, rows // 2
    _, own, _ = x_frame(n_gx, tall)
    groups = extent // HALO
    zero = jnp.zeros((8, 128), F32)

    def clear(ref, count, depth):
        for x in (0, count + 1):
            for r in range(0, depth + 16, 8):
                ref[x, r : r + 8, :] = zero
        for x in range(1, count + 1):
            ref[x, 0:8, :] = zero
            ref[x, depth + 8 : depth + 16, :] = zero

    for ref in (gm, gs, vm, vs):
        clear(ref, extent, rows)
    for ref in (v1m, v1s, g1m, g1s, w1m, w1s):
        clear(ref, half, half_rows)

    lane = iota((rows, 128), 1)
    ends = z_ends(n_gz)
    masks = [((lane >= e["lane"]) & (lane < e["lane"] + HALO)).astype(F32) * e["valid"].astype(F32) for e in ends]

    def load(group):
        for i in range(HALO):
            x = group * HALO + i
            sides = []
            for a in range(2):
                total = None
                for ref, mask, end in zip((za, zb), masks, ends):
                    piece = roll(ref[group], end["lane"] - 16 * i - 8 * a) * mask
                    total = piece if total is None else total + piece
                sides.append(total)
            ws[x] = sides[1]
            gm[x + 1, 8 : 8 + rows, :] = K * fb[x] * inverse(fw[x])
            gs[x + 1, 8 : 8 + rows, :] = K * sides[0] * inverse(sides[1])

    each(groups, load, 4)

    def second(x):
        main, side, main_n, side_n = neighbours(gm, gs, x + 1, 8, rows, 1)
        vm[x + 1, 8 : 8 + rows, :] = 1.2 * main + jnp.where(fw[x] > 0.0, K * main_n, 0.0)
        vs[x + 1, 8 : 8 + rows, :] = 1.2 * side + jnp.where(ws[x] > 0.0, K * side_n, 0.0)

    each(extent, second, 8)

    def residual(x2):
        totals = None
        for j in range(2):
            x = 2 * x2 + j
            main, side, main_n, side_n = neighbours(vm, vs, x + 1, 8, rows, 1)
            w_main, w_side = fw[x], ws[x]
            r_main = w_main * ((1.0 / K) * gm[x + 1, 8 : 8 + rows, :] - 6.0 * main + main_n)
            r_side = w_side * ((1.0 / K) * gs[x + 1, 8 : 8 + rows, :] - 6.0 * side + side_n)
            values = (r_main, r_side, w_main, w_side)
            totals = values if j == 0 else tuple(a + b for a, b in zip(totals, values))
        for ref, value in zip((tm, ts, um, us), totals):
            ref[x2] = value

        def pairs(ref):
            return lane_pairs(ref[x2, pl.ds(0, half_rows, stride=2), :] + ref[x2, pl.ds(1, half_rows, stride=2), :], 1)

        for t_ref, u_ref, w_out, g_out in ((tm, um, w1m, g1m), (ts, us, w1s, g1s)):
            weights = 0.0625 * pairs(u_ref)
            w_out[x2 + 1, 8 : 8 + half_rows, :] = weights
            g_out[x2 + 1, 8 : 8 + half_rows, :] = (0.125 * K) * pairs(t_ref) * inverse(weights)

    each(half, residual, 4)

    def second_1(x):
        main, side, main_n, side_n = neighbours(g1m, g1s, x + 1, 8, half_rows, 2)
        v1m[x + 1, 8 : 8 + half_rows, :] = 1.2 * main + jnp.where(w1m[x + 1, 8 : 8 + half_rows, :] > 0.0, K * main_n, 0.0)
        v1s[x + 1, 8 : 8 + half_rows, :] = 1.2 * side + jnp.where(w1s[x + 1, 8 : 8 + half_rows, :] > 0.0, K * side_n, 0.0)

    each(half, second_1, 16)

    base = own // 2
    first_row = 8 + HALO // 2
    quarter, quarter_rows = tall // 4, wide // 4
    for x2 in range(quarter):
        total_r = total_w = None
        for j in range(2):
            x = base + 2 * x2 + j + 1
            main, _, main_n, _ = neighbours(v1m, v1s, x, first_row, wide // 2, 2)
            weights = w1m[x, pl.ds(first_row, wide // 2), :]
            res = weights * ((1.0 / K) * g1m[x, pl.ds(first_row, wide // 2), :] - 6.0 * main + main_n)
            total_r = res if j == 0 else total_r + res
            total_w = weights if j == 0 else total_w + weights
        small[0, x2] = total_r
        small[1, x2] = total_w
    q = []
    for a, factor in ((0, 0.125), (1, 0.0625)):
        for x2 in range(quarter):
            ref = small.at[a, x2]
            both = ref[pl.ds(0, quarter_rows, stride=2), :] + ref[pl.ds(1, quarter_rows, stride=2), :]
            q.append(factor * lane_pairs(both, 2))
    stacked = jnp.concatenate([jnp.concatenate(q[:quarter], axis=0), jnp.concatenate(q[quarter:], axis=0)], axis=0)
    src, dst = iota((128, 128), 0), iota((128, 128), 1)
    pick = (src == 4 * (dst % 32)).astype(F32)
    compact = jnp.dot(stacked, pick, precision=lax.Precision.HIGHEST, preferred_element_type=F32)
    block = iota((quarter_rows, 128), 1) // 32
    gz = lax.axis_index("gz")
    out = []
    for a in range(2):
        packed = jnp.zeros((quarter_rows, 128), F32)
        for x2 in range(quarter):
            r = (a * quarter + x2) * quarter_rows
            packed = jnp.where(block == lax.rem(gz + x2, 4), compact[r : r + quarter_rows], packed)
        out.append(packed)
    message = jnp.concatenate(out, axis=0)

    def copy(d):
        send[d] = message

    each(send.shape[0], copy, 8)

    for i in range(tall + 2):
        v0w[i] = vm[own + i, 8 : 8 + rows, :]
        x = own + (i - 1)
        inside = (x >= 0) & (x < extent)
        w0w[i] = keep(inside, fw[jnp.clip(x, 0, extent - 1)])
    for i in range(tall):
        v0h[i] = vs[own + i + 1, 8 + HALO : 8 + HALO + wide, :]
        w0h[i] = ws[own + i, HALO : HALO + wide, :]
        g0[i] = gm[own + i + 1, 8 + HALO : 8 + HALO + wide, :]


def up_kernel(mesh_shape, *refs):
    n_gx, n_gy, n_gz = mesh_shape
    recv, rows_ref, za, zb, v0w, w0w, v0h, w0h, g0, v1m, v1s, w1m, w1s, g1m, g1s, out = refs[:16]
    g2, w2, v2, y2, e2, p2, t3, u3, g3, w3, v3, y3, p3, b4, _, y1m, y1s, e1m, e1s, f1m, f1s, y0m, y0s = refs[16:]
    tall, wide = out.shape[0], out.shape[1]
    size_x, size_z = w2.shape[0], w2.shape[2]
    size_y = w2.shape[1]
    ix, own, _ = x_frame(n_gx, tall)
    iy, iz = lax.axis_index("gy"), lax.axis_index("gz")
    quarter, quarter_rows = tall // 4, wide // 4
    extent = frame_extent(n_gx, tall)
    half, half_rows = v1m.shape[0] - 2, v1m.shape[1] - 16

    def clear(ref):
        count, depth, size = ref.shape
        zero = jnp.zeros((8, size), F32)
        for x in range(count):
            ref[x, 0:8, :] = zero
            ref[x, depth - 8 : depth, :] = zero
        for x in (0, count - 1):
            ref[x] = jnp.zeros((depth, size), F32)

    for ref in (g2, v2, y2, g3, v3, y3):
        clear(ref)
    e2[...] = jnp.zeros(e2.shape, F32)
    p3[...] = jnp.zeros(p3.shape, F32)

    lane = iota((quarter_rows, 128), 1)
    block = lane // 32
    for gx in range(n_gx):
        for gy in range(n_gy):
            for x in range(quarter):
                tiles_b, tiles_w = [], []
                for tile in range(size_z // 128):
                    picked = [jnp.zeros((quarter_rows, 128), F32)] * 2
                    for j in range(4):
                        gz = tile * 4 + j
                        d = (gx * n_gy + gy) * n_gz + gz
                        mask = block == (gz + x) % 4
                        for a in range(2):
                            piece = recv[d, a * quarter_rows : (a + 1) * quarter_rows, :]
                            picked[a] = jnp.where(mask, piece, picked[a])
                    tiles_b.append(roll(picked[0], -32 * x))
                    tiles_w.append(roll(picked[1], -32 * x))
                weights = joined(tiles_w)
                w2[gx * quarter + x, gy * quarter_rows : (gy + 1) * quarter_rows, :] = weights
                g2[gx * quarter + x + 1, 8 + gy * quarter_rows : 8 + (gy + 1) * quarter_rows, :] = K * joined(tiles_b) / weights

    def smooth(g, v, x, rows, step):
        main, near = global_neighbours(g, x + 1, 8, rows, step)
        v[x + 1, 8 : 8 + rows, :] = 1.2 * main + K * near

    def resid(g, v, w, x, rows, step):
        main, near = global_neighbours(v, x + 1, 8, rows, step)
        return w[x] * ((1.0 / K) * g[x + 1, 8 : 8 + rows, :] - 6.0 * main + near)

    each(size_x, lambda x: smooth(g2, v2, x, size_y, 1), 8)
    rows3, x3 = size_y // 2, size_x // 2

    def restrict_2(x):
        for t, part in enumerate(tiled(resid(g2, v2, w2, 2 * x, size_y, 1) + resid(g2, v2, w2, 2 * x + 1, size_y, 1))):
            t3[t] = part
        for t, part in enumerate(tiled(w2[2 * x] + w2[2 * x + 1])):
            u3[t] = part
        pairs = lambda ref: lane_pairs(row_pairs(ref, size_y), 1)
        weights = 0.0625 * pairs(u3)
        w3[x] = weights
        g3[x + 1, 8 : 8 + rows3, :] = (0.125 * K) * pairs(t3) / weights

    each(x3, restrict_2, 4)
    each(x3, lambda x: smooth(g3, v3, x, rows3, 2), 8)
    rows4, x4 = rows3 // 2, x3 // 2

    def restrict_3(x):
        for t, part in enumerate(tiled(resid(g3, v3, w3, 2 * x, rows3, 2) + resid(g3, v3, w3, 2 * x + 1, rows3, 2))):
            t3[t, 0:rows3, :] = part
        b4[x] = 0.125 * lane_pairs(row_pairs(t3, rows3), 2)

    each(x4, restrict_3, 4)

    tiles = rows_ref.shape[0] // 9
    coarse_z = size_z // 4
    per = 128 // coarse_z
    src, dst = iota((size_z, 128), 0), iota((size_z, 128), 1)
    pick = (src == 4 * (dst % coarse_z)).astype(F32)
    values = b4[0] if x4 == 1 else jnp.concatenate([b4[x] for x in range(x4)], axis=0)
    compact = jnp.dot(values, pick, precision=lax.Precision.HIGHEST, preferred_element_type=F32)
    place = iota((x4 * rows4, 128), 0) % per == iota((x4 * rows4, 128), 1) // coarse_z
    compact = jnp.where(place, compact, 0.0)
    vectors = [jnp.sum(compact[t * per : (t + 1) * per], axis=0, keepdims=True) for t in range(tiles)]
    ends = z_ends(n_gz)
    groups = extent // HALO
    fine = iota((HALO, size_z), 1) // 4
    fine_row = fine == iz * HALO + iota((HALO, size_z), 0)
    edge_row = iota((16, 128), 0)
    first_total = [None, None]
    for k, ref in enumerate((za, zb)):
        total = None
        for t in range(tiles):
            piece = ref[groups + t // 2, 16 * (t % 2) : 16 * (t % 2) + 16, :] * vectors[t]
            total = piece if total is None else total + piece
        first_total[k] = jnp.sum(total, axis=1, keepdims=True) * ends[k]["valid"].astype(F32)
    z_lane = iota((16, size_z), 1) // 4
    spread = None
    for k in range(2):
        piece = jnp.where(z_lane == iz * HALO + ends[k]["row"], first_total[k], 0.0)
        spread = piece if spread is None else spread + piece
    for m in range(9):
        total = None
        for t in range(tiles):
            piece = rows_ref[m * tiles + t] * vectors[t]
            total = piece if total is None else total + piece
        values = jnp.sum(total, axis=1, keepdims=True)
        line = jnp.sum(jnp.where(fine_row, values, 0.0), axis=0, keepdims=True) + spread[m : m + 1, :]
        row = 8 + 2 * (iy + (m % 3 - 1))
        for t, part in enumerate(tiled(line)):
            p3[ix + m // 3, t, pl.ds(row, 1), :] = part
            p3[ix + m // 3, t, pl.ds(row + 1, 1), :] = part

    def lift(y, v, w, p, x, px, rows, row):
        coarse = joined([p[px, t, row : row + rows, :] for t in range(p.shape[1])])
        y[x + 1, 8 : 8 + rows, :] = v[x + 1, 8 : 8 + rows, :] + w[x] * coarse

    def relax(y, g, w, x, rows, step):
        main, near = global_neighbours(y, x + 1, 8, rows, step)
        return (0.2 * main + g[x + 1, 8 : 8 + rows, :] + K * near) / w[x]

    each(x3, lambda x: lift(y3, v3, w3, p3, x, x // 2 + 1, rows3, 8), 8)

    def up_3(x):
        for t, e3 in enumerate(tiled(relax(y3, g3, w3, x, rows3, 2))):
            p2[x, t, pl.ds(0, rows3, stride=2), :] = e3
            p2[x, t, pl.ds(1, rows3, stride=2), :] = e3

    each(x3, up_3, 4)
    each(size_x, lambda x: lift(y2, v2, w2, p2, x, x // 2, size_y, 0), 8)

    def up_2(x):
        for t, part in enumerate(tiled(relax(y2, g2, w2, x, size_y, 1))):
            e2[x + 2, t, 8 : 8 + size_y, :] = part

    each(size_x, up_2, 8)

    src, dst = iota((size_z, 256), 0), iota((size_z, 256), 1)
    start = iz * 32
    cell = jnp.where(dst < 128, dst // 4, jnp.where(dst < 192, 32 + (dst - 128) // 4, -1 - (255 - dst) // 4))
    widen = (src == start + cell).astype(F32)
    n2 = extent // 4
    x_start = ix * quarter - own // 4
    y_start = 8 + iy * quarter_rows - HALO // 4
    spread = None
    for t in range(size_z // 128):
        stacked = jnp.concatenate([e2[x_start + 2 + i, t, pl.ds(y_start, 8), :] for i in range(n2)], axis=0)
        part = jnp.dot(stacked, widen[t * 128 : (t + 1) * 128], precision=lax.Precision.HIGHEST, preferred_element_type=F32)
        spread = part if spread is None else spread + part
    for i in range(n2):
        for ref, part in ((e1m, spread[i * 8 : i * 8 + 8, :128]), (e1s, spread[i * 8 : i * 8 + 8, 128:])):
            ref[i, pl.ds(0, 8, stride=2), :] = part
            ref[i, pl.ds(1, 8, stride=2), :] = part

    clear(y1m)
    clear(y1s)
    inner = slice(8, 8 + half_rows)
    for x in range(half):
        y1m[x + 1, inner, :] = v1m[x + 1, inner, :] + w1m[x + 1, inner, :] * e1m[x // 2]
        y1s[x + 1, inner, :] = v1s[x + 1, inner, :] + w1s[x + 1, inner, :] * e1s[x // 2]

    def up_1(x):
        main, side, main_n, side_n = neighbours(y1m, y1s, x + 1, 8, half_rows, 2)
        for f, y, near, g, w in ((f1m, main, main_n, g1m, w1m), (f1s, side, side_n, g1s, w1s)):
            e1 = (0.2 * y + g[x + 1, inner, :] + K * near) * inverse(w[x + 1, inner, :])
            f[x, pl.ds(0, half_rows, stride=2), :] = e1
            f[x, pl.ds(1, half_rows, stride=2), :] = e1

    each(half, up_1, 12)
    base = own // 2
    for i in range(tall + 2):
        parent = jnp.clip(base + (i + 1) // 2 - 1, 0, half - 1)
        y0m[i] = v0w[i] + w0w[i] * f1m[parent]
        if 0 < i <= tall:
            y0s[i - 1] = v0h[i - 1] + w0h[i - 1] * f1s[parent, HALO : HALO + wide, :]

    def up_0(i):
        main = y0m[i + 1, pl.ds(HALO, wide), :]
        main_z, _ = z_sum(main, y0s[i], 1)
        near = xy_sum(y0m, i + 1, HALO, wide) + main_z
        out[i] = (0.2 * main + g0[i] + K * near) / w0w[i + 1, HALO : HALO + wide, :]

    each(tall, up_0, 16)


def size_of(shape):
    return 4 * math.prod(shape)


def call(kernel, outs, scratch=(), resident=True, fetch=False):
    limit = 8 * 2**20 + sum(map(size_of, scratch)) + sum(size_of(s) for s in outs if size_of(s) > 2**20)
    run = pl.pallas_call(
        kernel,
        out_shape=[(pltpu.VMEM if resident and size_of(s) <= 2**20 else jax.ShapeDtypeStruct)(s, F32) for s in outs],
        scratch_shapes=[pltpu.VMEM(s, F32) for s in scratch],
        compiler_params=pltpu.CompilerParams(vmem_limit_bytes=min(limit, 56 * 2**20)),
    )

    def place(value):
        small = size_of(value.shape) <= 2**20 and not fetch
        return pltpu.with_memory_space_constraint(value, pltpu.VMEM if small else pltpu.HBM)

    return lambda *values: run(*map(place, values))


def plain_halo(mesh_shape, own, frames):
    n_gx = mesh_shape[0]
    tall = own[0].shape[0]
    extent, tiles = frames[0][0], own[2].shape[1] // 128
    parts = ()
    if n_gx > 1:
        odd = lax.axis_index("gx") % 2
        for first in range(2):
            start = jnp.where(odd == first, tall - HALO, 0)
            faces = [lax.dynamic_slice_in_dim(a, start, HALO, 0) for a in own[:2]] + [own[2]]
            parts += tuple(swap(a, "gx", first) for a in faces)
    slab = (2 * extent + 3 * tiles, HALO, 128)
    y_slabs = call(functools.partial(y_pack_kernel, mesh_shape), [slab, slab])(*own, *parts)
    y_parts = [ring(s, "gy", step) for s, step in zip(y_slabs, (1, -1))]
    fb, fw, matrix, z_a, z_b = call(functools.partial(z_pack_kernel, mesh_shape), frames)(*own, *parts, *y_parts)
    return fb, fw, matrix, ring(z_a, "gz", 1), ring(z_b, "gz", -1)


def shared_halo(mesh_shape, own, frames):
    tall, wide = own[0].shape[:2]
    tiles = own[2].shape[1] // 128
    strips, groups, per = (tiles + 7) // 8, tall // HALO, wide // 8
    z_shape = (groups * per + strips, HALO, 128)
    y_shape = (2 * tall + tiles, HALO, 128)
    x_shape = (2 * per * tall + tiles, HALO, 128)
    outs = [z_shape, z_shape, y_shape, y_shape, x_shape] + [a.shape for a in own]
    z_tail, z_head, y_tail, y_head, x_own, *here = call(face_kernel, outs, fetch=True)(*own)

    z_got = (ring(z_tail, "gz", 1), ring(z_head, "gz", -1))
    y_got = (ring(y_tail, "gy", 1), ring(y_head, "gy", -1))
    other = swap(x_own, "gx", 0)
    z_got = lax.optimization_barrier(z_got)
    edge = (2 * (groups + strips), HALO, 128)
    both = (2 * z_shape[0], HALO, 128)
    edge_tail, edge_head, z_both = call(functools.partial(y_edge_kernel, groups, per), [edge, edge, both])(*z_got)
    edge_got = (ring(edge_tail, "gy", 1), ring(edge_head, "gy", -1))
    z_other = swap(z_both, "gx", 0)
    y_other = [swap(y, "gx", 0) for y in y_got]
    edge_other = [swap(y, "gx", 0) for y in edge_got]
    return call(functools.partial(frame_kernel, mesh_shape), frames)(
        *here, other, *z_got, z_other, *y_got, *y_other, *edge_got, *edge_other
    )


def per_device(mesh_shape, sources, stiffness, coarse_inverse):
    n_gx, n_gy, n_gz = mesh_shape
    count = n_gx * n_gy * n_gz
    tall, wide, deep = stiffness.shape
    cells = coarse_inverse.shape[1]
    assert sources.shape[0] == 1 and deep == 128 and tall == 16 and wide == 16 and n_gz % 4 == 0 and cells % 128 == 0
    tiles = cells // 128
    extent = frame_extent(n_gx, tall)
    source = sources[0]
    own = (source, stiffness, coarse_inverse)
    rows = wide + 2 * HALO
    frame = (extent, rows, 128)
    z_slab = (extent // HALO + (tiles + 1) // 2, rows, 128)
    frames = [frame, frame, (9 * tiles, HALO, 128), z_slab, z_slab]
    exchange = shared_halo if n_gx == 2 else plain_halo
    fb, fw, matrix, z_a, z_b = exchange(mesh_shape, own, frames)
    padded = (extent + 2, rows + 16, 128)
    half, half_rows = extent // 2, rows // 2
    level1 = (half + 2, half_rows + 16, 128)
    window, face = (tall + 2, rows, 128), (tall, wide, 128)
    message = (count, wide // 2, 128)
    outs = [message, window, window, face, face, face] + [level1] * 6
    scratch = [padded] * 4 + [frame] + [(half, rows, 128)] * 4 + [(2, tall // 4, wide // 2, 128)]
    send, *state = call(functools.partial(down_kernel, mesh_shape), outs, scratch)(fb, fw, z_a, z_b)
    recv = lax.all_to_all(send, AXES, 0, 0, tiled=True)
    size_x, size_y, size_z = n_gx * tall // 4, n_gy * wide // 4, n_gz * deep // 4
    pad2 = (size_x + 2, size_y + 16, size_z)
    x3, rows3 = size_x // 2, size_y // 2
    pad3 = (x3 + 2, rows3 + 16, size_z)
    n2, lane_tiles = extent // 4, size_z // 128
    scratch = [
        pad2, (size_x, size_y, size_z), pad2, pad2, (size_x + 4, lane_tiles, size_y + 16, 128), (x3, lane_tiles, size_y, 128),
        (lane_tiles, size_y, 128), (lane_tiles, size_y, 128), pad3, (x3, rows3, size_z), pad3, pad3,
        (x3 // 2 + 2, lane_tiles, rows3 + 16, 128),
        (x3 // 2, rows3 // 2, size_z), (8, 128), level1, level1, (n2, 16, 128), (n2, 16, 128),
        (half, rows, 128), (half, rows, 128), window, face,
    ]
    (pressure,) = call(functools.partial(up_kernel, mesh_shape), [face], scratch, False)(recv, matrix, z_a, z_b, *state)
    return pressure[None]


def solution(mesh):
    mesh_shape = tuple(mesh.shape[a] for a in AXES)
    in_specs = (P(None, "gx", "gy", "gz"), P("gx", "gy", "gz"), P(AXES, None))
    return jax.shard_map(
        functools.partial(per_device, mesh_shape),
        mesh=mesh,
        in_specs=in_specs,
        out_specs=P(None, "gx", "gy", "gz"),
        check_vma=False,
    )
```

```python
import functools
import math

import jax
import jax.numpy as jnp
from jax import lax
from jax.experimental import pallas as pl
from jax.experimental.pallas import tpu as pltpu
from jax.sharding import PartitionSpec as P


damping = 0.8
K = damping / 6.0
AXES = ("gx", "gy", "gz")
HALO = 8
F32 = jnp.float32


def swap(values, axis, first):
    count = lax.axis_size(axis)
    partner = list(range(count))
    for i in range(first, count - 1, 2):
        partner[i], partner[i + 1] = i + 1, i
    return lax.ppermute(values, axis, list(enumerate(partner)))


def ring(values, axis, step):
    count = lax.axis_size(axis)
    return lax.ppermute(values, axis, [(i, (i + step) % count) for i in range(count)])


def iota(shape, dim):
    return lax.broadcasted_iota(jnp.int32, shape, dim)


def roll(values, amount):
    size = values.shape[-1]
    if isinstance(amount, int):
        amount = amount % size
        if amount == 0:
            return values
    return pltpu.roll(values, amount, values.ndim - 1)


def z_sum(main, side, step):
    lane = iota(main.shape, main.ndim - 1)
    size = main.shape[-1]
    main_up, side_up = roll(main, -step), roll(side, -step)
    main_dn, side_dn = roll(main, step), roll(side, step)
    last = lane >= size - step
    first = lane < step
    main_sum = jnp.where(last, side_up, main_up) + jnp.where(first, side_dn, main_dn)
    side_sum = jnp.where(last, main_up, side_up) + jnp.where(first, main_dn, side_dn)
    return main_sum, side_sum


def xy_sum(ref, x, row, rows):
    total = ref[x - 1, pl.ds(row, rows), :] + ref[x + 1, pl.ds(row, rows), :]
    return total + ref[x, pl.ds(row - 1, rows), :] + ref[x, pl.ds(row + 1, rows), :]


def neighbours(main_ref, side_ref, x, row, rows, step):
    main = main_ref[x, pl.ds(row, rows), :]
    side = side_ref[x, pl.ds(row, rows), :]
    main_z, side_z = z_sum(main, side, step)
    return main, side, xy_sum(main_ref, x, row, rows) + main_z, xy_sum(side_ref, x, row, rows) + side_z


def global_neighbours(ref, x, row, rows, step):
    main = ref[x, pl.ds(row, rows), :]
    lane = iota(main.shape, 1)
    size = main.shape[-1]
    up = jnp.where(lane >= size - step, 0.0, roll(main, -step))
    dn = jnp.where(lane < step, 0.0, roll(main, step))
    return main, xy_sum(ref, x, row, rows) + up + dn


def lane_pairs(values, step):
    lane = iota(values.shape, values.ndim - 1)
    return values + jnp.where((lane // step) % 2 == 0, roll(values, -step), roll(values, step))


def inverse(weights):
    return jnp.where(weights > 0.0, 1.0 / jnp.where(weights > 0.0, weights, 1.0), 0.0)


def select_lanes(values, chosen):
    first = values.astype(jnp.bfloat16)
    rest = values - first.astype(F32)
    second = rest.astype(jnp.bfloat16)
    third = (rest - second.astype(F32)).astype(jnp.bfloat16)
    matrix = chosen.astype(F32).astype(jnp.bfloat16)
    parts = [jnp.dot(p, matrix, preferred_element_type=F32) for p in (first, second, third)]
    return parts[0] + (parts[1] + parts[2])


def tiled(value):
    return [value[:, t * 128 : (t + 1) * 128] for t in range(value.shape[1] // 128)]


def joined(parts):
    return parts[0] if len(parts) == 1 else jnp.concatenate(parts, axis=1)


def row_pairs(ref, rows):
    return joined([ref[t, pl.ds(0, rows // 2, stride=2), :] + ref[t, pl.ds(1, rows // 2, stride=2), :] for t in range(ref.shape[0])])


def each(count, body, width=1):
    while count % width:
        width -= 1
    if count == width:
        for i in range(count):
            body(i)
        return

    def step(i, carry):
        for j in range(width):
            body(i * width + j)
        return carry

    lax.fori_loop(0, count // width, step, 0)


def pair_places(axis, count, own, tall):
    index = lax.axis_index(axis)
    odd = index % 2
    first = dict(place=jnp.where(odd == 0, own + tall, 0), high=odd == 0, valid=jnp.where(odd == 0, index + 1, index - 1) < count)
    other = jnp.where(odd == 0, index - 1, index + 1)
    second = dict(place=jnp.where(odd == 0, 0, own + tall), high=odd == 1, valid=(other >= 0) & (other < count))
    return index, odd, (first, second)


def x_frame(count, tall):
    index = lax.axis_index("gx")
    odd = index % 2
    if count == 1:
        return index, 0, ()
    own = HALO * odd if count == 2 else HALO
    _, _, (first, second) = pair_places("gx", count, own, tall)
    if count == 2:
        first["source"] = jnp.where(odd == 0, 0, tall - HALO)
        return index, own, (first,)
    first["source"] = second["source"] = 0
    return index, own, (first, second)


def y_ends(count, wide):
    index = lax.axis_index("gy")
    return (dict(valid=index > 0, place=0, high=0), dict(valid=index < count - 1, place=wide + HALO, high=1))


def inner_frames(padded, plain):
    extent, rows = plain.shape[0], plain.shape[1]
    for x in (0, extent + 1):
        padded[x] = jnp.zeros(padded.shape[1:], F32)
    return padded.at[pl.ds(1, extent), pl.ds(8, rows), :], plain


def frame_extent(count, tall):
    return tall + (0 if count == 1 else HALO if count == 2 else 2 * HALO)


def keep(valid, values):
    return jnp.where(valid, values, jnp.zeros_like(values))


def y_pack_kernel(mesh_shape, *refs):
    n_gx, _, _ = mesh_shape
    n_in = 3 * (1 + min(n_gx - 1, 2))
    own_refs, part_refs, outs = refs[:3], refs[3:n_in], refs[n_in:]
    tall, wide = own_refs[0].shape[0], own_refs[0].shape[1]
    extent = frame_extent(n_gx, tall)
    tiles = own_refs[2].shape[1] // 128
    _, own, parts = x_frame(n_gx, tall)
    for out, start in zip(outs, (wide - HALO, 0)):
        rows = pl.ds(start, HALO)
        for a in range(2):
            out[pl.ds(a * extent + own, tall)] = own_refs[a][:, rows, :]
            for part, ref in zip(parts, (part_refs[a : a + 1], part_refs[3 + a : 4 + a])):
                out[pl.ds(a * extent + part["place"], HALO)] = keep(part["valid"], ref[0][pl.ds(part["source"], HALO), rows, :])
        base = 2 * extent
        for side in (0, 2):
            for t in range(tiles):
                out[base + side * tiles + t] = jnp.zeros((HALO, 128), F32)
        for t in range(tiles):
            out[base + tiles + t] = own_refs[2][:, t * 128 : (t + 1) * 128]
            for part, ref in zip(parts, (part_refs[2:3], part_refs[5:6])):
                side = jnp.where(part["high"], 2, 0)
                out[base + side * tiles + t] = keep(part["valid"], ref[0][:, t * 128 : (t + 1) * 128])


def z_pack_kernel(mesh_shape, *refs):
    n_gx, n_gy, _ = mesh_shape
    n_in = 3 * (1 + min(n_gx - 1, 2))
    own_refs, part_refs = refs[:3], refs[3:n_in]
    y_refs = refs[n_in : n_in + 2]
    frames = inner_frames(*refs[n_in + 2 : n_in + 4])
    rows_ref, z_outs = refs[n_in + 4], refs[n_in + 5 :]
    tall, wide = own_refs[0].shape[0], own_refs[0].shape[1]
    extent = frame_extent(n_gx, tall)
    tiles = own_refs[2].shape[1] // 128
    _, own, parts = x_frame(n_gx, tall)
    y_parts = y_ends(n_gy, wide)
    for a in range(2):
        frames[a][pl.ds(own, tall), HALO : HALO + wide, :] = own_refs[a][...]
        for part, ref in zip(parts, (part_refs[a : a + 1], part_refs[3 + a : 4 + a])):
            frames[a][pl.ds(part["place"], HALO), HALO : HALO + wide, :] = keep(part["valid"], ref[0][pl.ds(part["source"], HALO)])
        for part, ref in zip(y_parts, y_refs):
            rows = pl.ds(part["place"], HALO)
            frames[a][:, rows, :] = keep(part["valid"], ref[a * extent : (a + 1) * extent])
    for t in range(tiles):
        for side in (0, 2):
            rows_ref[(side * 3 + 1) * tiles + t] = jnp.zeros((HALO, 128), F32)
        rows_ref[4 * tiles + t] = own_refs[2][:, t * 128 : (t + 1) * 128]
        for part, ref in zip(parts, (part_refs[2:3], part_refs[5:6])):
            side = jnp.where(part["high"], 2, 0)
            rows_ref[(side * 3 + 1) * tiles + t] = keep(part["valid"], ref[0][:, t * 128 : (t + 1) * 128])
        for x_side in range(3):
            for part, ref in zip(y_parts, y_refs):
                side = 2 * part["high"]
                rows_ref[(x_side * 3 + side) * tiles + t] = keep(part["valid"], ref[2 * extent + x_side * tiles + t])
    groups = extent // HALO
    for out, tail in zip(z_outs, (1, 0)):

        def put(group, packed):
            out[group] = packed

        pack_z(frames, put, tail)
        row = (HALO - 1) * tail
        for s in range((tiles + 1) // 2):
            out[groups + s] = jnp.zeros((4 * HALO, 128), F32)
        for t in range(tiles):
            for m in range(9):
                out[groups + t // 2, 16 * (t % 2) + m : 16 * (t % 2) + m + 1, :] = rows_ref[m * tiles + t, row : row + 1, :]


def z_ends(count):
    index = lax.axis_index("gz")
    return (dict(valid=index > 0, lane=120, row=-1), dict(valid=index < count - 1, lane=0, row=HALO))


def pack_z(frames, out, tail):
    rows = frames[0].shape[1]
    slot = iota((rows, 128), 1) // HALO
    for group in range(frames[0].shape[0] // HALO):
        packed = jnp.zeros((rows, 128), F32)
        for i in range(HALO):
            for a in range(2):
                at = (2 * i + a + 1 - tail) % 16
                piece = roll(frames[a][group * HALO + i], 8 * (tail + at))
                packed = jnp.where(slot == at, piece, packed)
        out(group, packed)


def face_kernel(*refs):
    source, weights, matrix, *outs = refs
    outs, y_outs, both, (b, w, own_matrix, own_inverse) = outs[:2], outs[2:4], outs[4], outs[5:]
    tall, wide = b.shape[0], b.shape[1]
    inverses = 1.0 / weights[...]
    own_inverse[...] = inverses
    b[...] = K * source[...] * inverses
    w[...] = weights[...]
    own_matrix[...] = matrix[...]
    tiles = matrix.shape[1] // 128
    strips = (tiles + 7) // 8
    per = wide // 8
    for out, tail in zip(outs, (1, 0)):

        def put(group, packed):
            for r in range(per):
                out[group * per + r] = packed[8 * r : 8 * r + 8]

        pack_z((b, w), put, tail)
        at = tall // HALO * per
        line = matrix[HALO - 1 : HALO, :] if tail else matrix[0:1, :]
        for strip in range(strips):
            out[at + strip] = jnp.zeros((8, 128), F32)
        for t in range(tiles):
            out[at + t // 8, t % 8 : t % 8 + 1, :] = line[:, t * 128 : (t + 1) * 128]
    for out, row in zip(y_outs, (wide - HALO, 0)):
        for a, ref in enumerate((b, w)):
            out[a * tall : (a + 1) * tall] = ref[:, row : row + HALO, :]
        for t in range(tiles):
            out[2 * tall + t] = matrix[:, t * 128 : (t + 1) * 128]
    at = 0
    for ref in (b, w):
        for r in range(per):
            both[at : at + tall] = ref[:, 8 * r : 8 * r + 8, :]
            at += tall
    for t in range(tiles):
        both[at + t] = matrix[:, t * 128 : (t + 1) * 128]


def y_edge_kernel(groups, per, *refs):
    z_refs, outs, both = refs[:2], refs[2:4], refs[4]
    size = z_refs[0].shape[0]
    strips = size - groups * per
    for out, r in zip(outs, (per - 1, 0)):
        for k, ref in enumerate(z_refs):
            at = k * (groups + strips)
            for group in range(groups):
                out[at + group] = ref[group * per + r]
            out[at + groups : at + groups + strips] = ref[groups * per : size]
    for k, ref in enumerate(z_refs):
        both[k * size : (k + 1) * size] = ref[...]


def frame_kernel(mesh_shape, *refs):
    n_gx, n_gy, _ = mesh_shape
    own_refs, other, z_refs, z_other = refs[:3], refs[3], refs[4:6], refs[6]
    y_refs, y_others, edge_refs, edge_others = refs[7:9], refs[9:11], refs[11:13], refs[13:15]
    frames, rows_ref, z_outs = inner_frames(*refs[15:17]), refs[17], refs[18:]
    tall, wide = own_refs[0].shape[0], own_refs[0].shape[1]
    extent = frame_extent(n_gx, tall)
    tiles = own_refs[2].shape[1] // 128
    strips, groups, per = (tiles + 7) // 8, tall // HALO, wide // 8
    _, own, parts = x_frame(n_gx, tall)
    place, source = parts[0]["place"], parts[0]["source"]
    y_parts = y_ends(n_gy, wide)
    far = jnp.where(parts[0]["high"], 2, 0)
    y_rows = [pl.ds(p["place"], HALO) for p in y_parts]
    y_side = [2 * p["high"] for p in y_parts]
    for a in range(2):
        frames[a][pl.ds(own, tall), HALO : HALO + wide, :] = own_refs[a][...]
        for r in range(per):
            rows = slice(HALO + 8 * r, HALO + 8 * r + 8)
            frames[a][pl.ds(place, HALO), rows, :] = other[pl.ds((a * per + r) * tall + source, HALO)]
        for part, rows, ref, ref_other in zip(y_parts, y_rows, y_refs, y_others):
            frames[a][pl.ds(own, tall), rows, :] = keep(part["valid"], ref[a * tall : (a + 1) * tall])
            frames[a][pl.ds(place, HALO), rows, :] = keep(part["valid"], ref_other[pl.ds(a * tall + source, HALO)])
    zero = jnp.zeros((HALO, 128), F32)
    for t in range(tiles):
        for side in range(3):
            rows_ref[((2 - far) * 3 + side) * tiles + t] = zero
        rows_ref[4 * tiles + t] = own_refs[2][:, t * 128 : (t + 1) * 128]
        rows_ref[(far * 3 + 1) * tiles + t] = other[2 * per * tall + t]
        for part, side, ref, ref_other in zip(y_parts, y_side, y_refs, y_others):
            rows_ref[(3 + side) * tiles + t] = keep(part["valid"], ref[2 * tall + t])
            rows_ref[(far * 3 + side) * tiles + t] = keep(part["valid"], ref_other[2 * tall + t])
    for k, (out, ref) in enumerate(zip(z_outs, z_refs)):
        base = k * (groups * per + strips)
        y_base = k * (groups + strips)
        total = extent // HALO
        for s in range((tiles + 1) // 2):
            out[total + s] = jnp.zeros((4 * HALO, 128), F32)
        for g in range(groups):
            for r in range(per):
                out[own // HALO + g, HALO + 8 * r : HALO + 8 * r + 8, :] = ref[g * per + r]
            for part, rows, y_ref in zip(y_parts, y_rows, edge_refs):
                out[own // HALO + g, rows, :] = keep(part["valid"], y_ref[y_base + g])
        for r in range(per):
            out[place // HALO, HALO + 8 * r : HALO + 8 * r + 8, :] = z_other[base + source // HALO * per + r]
        for part, rows, y_ref in zip(y_parts, y_rows, edge_others):
            out[place // HALO, rows, :] = keep(part["valid"], y_ref[y_base + source // HALO])
        for strip in range(strips):
            for x_side in range(3):
                if x_side == 1:
                    middle = ref[groups * per + strip]
                    edges = [keep(p["valid"], r[y_base + groups + strip]) for p, r in zip(y_parts, edge_refs)]
                else:
                    here = far == x_side
                    middle = keep(here, z_other[base + groups * per + strip])
                    edges = [keep(p["valid"] & here, r[y_base + groups + strip]) for p, r in zip(y_parts, edge_others)]
                low, high = edges
                for j in range(min(8, tiles - 8 * strip)):
                    t = 8 * strip + j
                    for side, values in enumerate((low, middle, high)):
                        m = 16 * (t % 2) + x_side * 3 + side
                        out[total + t // 2, m : m + 1, :] = values[j : j + 1]


def down_kernel(mesh_shape, *refs):
    n_gx, n_gy, n_gz = mesh_shape
    gm, fw, za, zb = refs[:4]
    send, vm, gs, vs, ws, v1m, v1s, w1m, w1s, g1m, g1s, i1m, i1s = refs[4:17]
    tm, ts, um, us, small = refs[17:]
    extent, rows = fw.shape[0], fw.shape[1]
    tall, wide = extent - frame_extent(n_gx, 0), rows - 2 * HALO
    half, half_rows = extent // 2, rows // 2
    ix, own, _ = x_frame(n_gx, tall)
    groups = extent // HALO
    for ref in (gs, vm, vs, g1m, g1s, v1m, v1s):
        for x in (0, ref.shape[0] - 1):
            ref[x] = jnp.zeros(ref.shape[1:], F32)

    ends, sides = z_ends(n_gz), y_ends(n_gy, wide)

    def inside(depth, step):
        row, lane = iota((depth, 128), 0), iota((depth, 128), 1)
        edge = HALO // step
        low, high = ((e["valid"].astype(F32)) for e in sides)
        main = jnp.where(row < edge, K * low, jnp.where(row >= depth - edge, K * high, K))
        low, high = (e["valid"].astype(F32) for e in ends)
        return main, main * jnp.where(lane >= 120, low, jnp.where(lane < HALO, high, 0.0))

    def present(x, step):
        if n_gx <= 2:
            return None
        edge = HALO // step
        out = ((x < edge) & (ix == 0)) | ((x >= extent // step - edge) & (ix == n_gx - 1))
        return 1.0 - out.astype(F32)

    lane = iota((rows, 128), 1)
    halo_lanes = jnp.where(lane >= 120, ends[0]["valid"].astype(F32), 0.0) + jnp.where(lane < HALO, ends[1]["valid"].astype(F32), 0.0)
    first_half = lane % 16 < HALO

    def load(group):
        low, high = za[group], zb[group]
        both = (jnp.where(first_half, low, high), jnp.where(first_half, high, low))
        for i in range(HALO):
            x = group * HALO + i
            gs[x + 1, 8 : 8 + rows, :] = roll(both[0], 120 - 16 * i) * halo_lanes
            ws[x] = roll(both[1], 112 - 16 * i) * halo_lanes

    each(groups, load, 4)

    def smooth(g_refs, v_refs, factors, x, depth, step):
        main, side, main_n, side_n = neighbours(*g_refs, x + 1, 8, depth, step)
        here = present(x, step)
        for ref, value, near, factor in zip(v_refs, (main, side), (main_n, side_n), factors):
            ref[x + 1, 8 : 8 + depth, :] = 1.2 * value + (factor if here is None else factor * here) * near

    factors = inside(rows, 1)
    each(extent, lambda x: smooth((gm, gs), (vm, vs), factors, x, rows, 1), 24)

    def residual(x2):
        for row in range(0, rows, 8):
            totals = None
            for j in range(2):
                x = 2 * x2 + j
                main, side, main_n, side_n = neighbours(vm, vs, x + 1, 8 + row, 8, 1)
                w_main, w_side = fw[x, row : row + 8, :], ws[x, row : row + 8, :]
                r_main = w_main * ((1.0 / K) * gm[x + 1, 8 + row : 16 + row, :] - 6.0 * main + main_n)
                r_side = w_side * ((1.0 / K) * gs[x + 1, 8 + row : 16 + row, :] - 6.0 * side + side_n)
                values = (r_main, r_side, w_main, w_side)
                totals = values if j == 0 else tuple(a + b for a, b in zip(totals, values))
            for ref, value in zip((tm, ts, um, us), totals):
                ref[x2, row : row + 8, :] = value

        def pairs(ref):
            return lane_pairs(ref[x2, pl.ds(0, half_rows, stride=2), :] + ref[x2, pl.ds(1, half_rows, stride=2), :], 1)

        for t_ref, u_ref, w_out, g_out, i_out in ((tm, um, w1m, g1m, i1m), (ts, us, w1s, g1s, i1s)):
            weights = 0.0625 * pairs(u_ref)
            inverses = inverse(weights)
            w_out[x2, :, :] = weights
            i_out[x2, :, :] = inverses
            g_out[x2 + 1, 8 : 8 + half_rows, :] = (0.125 * K) * pairs(t_ref) * inverses

    each(half, residual, 12)

    factors_1 = inside(half_rows, 2)
    each(half, lambda x: smooth((g1m, g1s), (v1m, v1s), factors_1, x, half_rows, 2), 16)

    base = own // 2
    first_row = 8 + HALO // 2
    quarter, quarter_rows = tall // 4, wide // 4
    for x2 in range(quarter):
        total_r = total_w = None
        for j in range(2):
            x = base + 2 * x2 + j + 1
            main, _, main_n, _ = neighbours(v1m, v1s, x, first_row, wide // 2, 2)
            weights = w1m[x - 1, pl.ds(first_row - 8, wide // 2), :]
            res = weights * ((1.0 / K) * g1m[x, pl.ds(first_row, wide // 2), :] - 6.0 * main + main_n)
            total_r = res if j == 0 else total_r + res
            total_w = weights if j == 0 else total_w + weights
        small[0, x2] = total_r
        small[1, x2] = total_w
    q = []
    for a, factor in ((0, 0.125), (1, 0.0625)):
        for x2 in range(quarter):
            ref = small.at[a, x2]
            both = ref[pl.ds(0, quarter_rows, stride=2), :] + ref[pl.ds(1, quarter_rows, stride=2), :]
            q.append(factor * both)
    stacked = jnp.concatenate([jnp.concatenate(q[:quarter], axis=0), jnp.concatenate(q[quarter:], axis=0)], axis=0)
    src, dst = iota((128, 128), 0), iota((128, 128), 1)
    cell = 4 * (dst % 32)
    compact = select_lanes(stacked, (src == cell) | (src == cell + 2))
    block = iota((quarter_rows, 128), 1) // 32
    gz = lax.axis_index("gz")
    out = []
    for a in range(2):
        packed = jnp.zeros((quarter_rows, 128), F32)
        for x2 in range(quarter):
            r = (a * quarter + x2) * quarter_rows
            packed = jnp.where(block == lax.rem(gz + x2, 4), compact[r : r + quarter_rows], packed)
        out.append(packed)
    message = jnp.concatenate(out, axis=0)

    def copy(d):
        send[d] = message

    each(send.shape[0], copy, 8)


def up_kernel(mesh_shape, *refs):
    n_gx, n_gy, n_gz = mesh_shape
    recv, rows_ref, za, zb, gm, fw, i0, vm, _, vs, ws, v1m, v1s, w1m, w1s, g1m, g1s, i1m, i1s, out = refs[:20]
    g2, w2, i2, v2, y2, e2, p2, t3, u3, g3, w3, i3, v3, y3, p3, b4, y1m, y1s, e1m, e1s, f1m, f1s, y0m, y0s = refs[20:]
    tall, wide = out.shape[0], out.shape[1]
    size_x, size_z = w2.shape[0], w2.shape[2]
    size_y = w2.shape[1]
    ix, own, _ = x_frame(n_gx, tall)
    iy, iz = lax.axis_index("gy"), lax.axis_index("gz")
    quarter, quarter_rows = tall // 4, wide // 4
    extent = frame_extent(n_gx, tall)
    half, half_rows = w1m.shape[0], w1m.shape[1]

    def clear(ref):
        count, depth, size = ref.shape
        zero = jnp.zeros((8, size), F32)
        for x in range(count):
            ref[x, 0:8, :] = zero
            ref[x, depth - 8 : depth, :] = zero
        for x in (0, count - 1):
            ref[x] = jnp.zeros((depth, size), F32)

    for ref in (g2, v2, y2, g3, v3, y3):
        clear(ref)
    e2[...] = jnp.zeros(e2.shape, F32)
    p3[...] = jnp.zeros(p3.shape, F32)

    lane = iota((quarter_rows, 128), 1)
    block = lane // 32
    for gx in range(n_gx):
        for gy in range(n_gy):
            for x in range(quarter):
                tiles_b, tiles_w = [], []
                for tile in range(size_z // 128):
                    picked = [jnp.zeros((quarter_rows, 128), F32)] * 2
                    for j in range(4):
                        gz = tile * 4 + j
                        d = (gx * n_gy + gy) * n_gz + gz
                        mask = block == (gz + x) % 4
                        for a in range(2):
                            piece = recv[d, a * quarter_rows : (a + 1) * quarter_rows, :]
                            picked[a] = jnp.where(mask, piece, picked[a])
                    tiles_b.append(roll(picked[0], -32 * x))
                    tiles_w.append(roll(picked[1], -32 * x))
                weights = joined(tiles_w)
                inverses = 1.0 / weights
                w2[gx * quarter + x, gy * quarter_rows : (gy + 1) * quarter_rows, :] = weights
                i2[gx * quarter + x, gy * quarter_rows : (gy + 1) * quarter_rows, :] = inverses
                g2[gx * quarter + x + 1, 8 + gy * quarter_rows : 8 + (gy + 1) * quarter_rows, :] = K * joined(tiles_b) * inverses

    def smooth(g, v, x, rows, step):
        main, near = global_neighbours(g, x + 1, 8, rows, step)
        v[x + 1, 8 : 8 + rows, :] = 1.2 * main + K * near

    def resid(g, v, w, x, rows, step):
        main, near = global_neighbours(v, x + 1, 8, rows, step)
        return w[x] * ((1.0 / K) * g[x + 1, 8 : 8 + rows, :] - 6.0 * main + near)

    each(size_x, lambda x: smooth(g2, v2, x, size_y, 1), 8)
    rows3, x3 = size_y // 2, size_x // 2

    def restrict_2(x):
        for t, part in enumerate(tiled(resid(g2, v2, w2, 2 * x, size_y, 1) + resid(g2, v2, w2, 2 * x + 1, size_y, 1))):
            t3[t] = part
        for t, part in enumerate(tiled(w2[2 * x] + w2[2 * x + 1])):
            u3[t] = part
        pairs = lambda ref: lane_pairs(row_pairs(ref, size_y), 1)
        weights = 0.0625 * pairs(u3)
        inverses = 1.0 / weights
        w3[x] = weights
        i3[x] = inverses
        g3[x + 1, 8 : 8 + rows3, :] = (0.125 * K) * pairs(t3) * inverses

    each(x3, restrict_2, 4)
    each(x3, lambda x: smooth(g3, v3, x, rows3, 2), 8)
    rows4, x4 = rows3 // 2, x3 // 2

    def restrict_3(x):
        for t, part in enumerate(tiled(resid(g3, v3, w3, 2 * x, rows3, 2) + resid(g3, v3, w3, 2 * x + 1, rows3, 2))):
            t3[t, 0:rows3, :] = part
        b4[x] = 0.125 * row_pairs(t3, rows3)

    each(x4, restrict_3, 4)

    tiles = rows_ref.shape[0] // 9
    coarse_z = size_z // 4
    per = 128 // coarse_z
    src, dst = iota((size_z, 128), 0), iota((size_z, 128), 1)
    values = b4[0] if x4 == 1 else jnp.concatenate([b4[x] for x in range(x4)], axis=0)
    cell = 4 * (dst % coarse_z)
    compact = select_lanes(values, (src == cell) | (src == cell + 2))
    place = iota((x4 * rows4, 128), 0) % per == iota((x4 * rows4, 128), 1) // coarse_z
    compact = jnp.where(place, compact, 0.0)
    vectors = [jnp.sum(compact[t * per : (t + 1) * per], axis=0, keepdims=True) for t in range(tiles)]
    ends = z_ends(n_gz)
    groups = extent // HALO
    fine = iota((HALO, size_z), 1) // 4
    fine_row = fine == iz * HALO + iota((HALO, size_z), 0)
    edge_row = iota((16, 128), 0)
    first_total = [None, None]
    for k, ref in enumerate((za, zb)):
        total = None
        for t in range(tiles):
            piece = ref[groups + t // 2, 16 * (t % 2) : 16 * (t % 2) + 16, :] * vectors[t]
            total = piece if total is None else total + piece
        first_total[k] = jnp.sum(total, axis=1, keepdims=True) * ends[k]["valid"].astype(F32)
    z_lane = iota((16, size_z), 1) // 4
    spread = None
    for k in range(2):
        piece = jnp.where(z_lane == iz * HALO + ends[k]["row"], first_total[k], 0.0)
        spread = piece if spread is None else spread + piece
    for m in range(9):
        total = None
        for t in range(tiles):
            piece = rows_ref[m * tiles + t] * vectors[t]
            total = piece if total is None else total + piece
        values = jnp.sum(total, axis=1, keepdims=True)
        line = jnp.sum(jnp.where(fine_row, values, 0.0), axis=0, keepdims=True) + spread[m : m + 1, :]
        row = 8 + 2 * (iy + (m % 3 - 1))
        for t, part in enumerate(tiled(line)):
            p3[ix + m // 3, t, pl.ds(row, 1), :] = part
            p3[ix + m // 3, t, pl.ds(row + 1, 1), :] = part

    def lift(y, v, w, p, x, px, rows, row):
        coarse = joined([p[px, t, row : row + rows, :] for t in range(p.shape[1])])
        y[x + 1, 8 : 8 + rows, :] = v[x + 1, 8 : 8 + rows, :] + w[x] * coarse

    def relax(y, g, inverses, x, rows, step):
        main, near = global_neighbours(y, x + 1, 8, rows, step)
        return (0.2 * main + g[x + 1, 8 : 8 + rows, :] + K * near) * inverses[x]

    each(x3, lambda x: lift(y3, v3, w3, p3, x, x // 2 + 1, rows3, 8), 8)

    def up_3(x):
        for t, e3 in enumerate(tiled(relax(y3, g3, i3, x, rows3, 2))):
            p2[x, t, pl.ds(0, rows3, stride=2), :] = e3
            p2[x, t, pl.ds(1, rows3, stride=2), :] = e3

    each(x3, up_3, 4)
    each(size_x, lambda x: lift(y2, v2, w2, p2, x, x // 2, size_y, 0), 8)

    def up_2(x):
        for t, part in enumerate(tiled(relax(y2, g2, i2, x, size_y, 1))):
            e2[x + 2, t, 8 : 8 + size_y, :] = part

    each(size_x, up_2, 8)

    src, dst = iota((size_z, 256), 0), iota((size_z, 256), 1)
    start = iz * 32
    cell = jnp.where(dst < 128, dst // 4, jnp.where(dst < 192, 32 + (dst - 128) // 4, -1 - (255 - dst) // 4))
    widen = src == start + cell
    n2 = extent // 4
    x_start = ix * quarter - own // 4
    y_start = 8 + iy * quarter_rows - HALO // 4
    spread = None
    for t in range(size_z // 128):
        stacked = jnp.concatenate([e2[x_start + 2 + i, t, pl.ds(y_start, 8), :] for i in range(n2)], axis=0)
        part = select_lanes(stacked, widen[t * 128 : (t + 1) * 128])
        spread = part if spread is None else spread + part
    for i in range(n2):
        for ref, part in ((e1m, spread[i * 8 : i * 8 + 8, :128]), (e1s, spread[i * 8 : i * 8 + 8, 128:])):
            ref[i, pl.ds(0, 8, stride=2), :] = part
            ref[i, pl.ds(1, 8, stride=2), :] = part

    for ref in (y1m, y1s):
        for x in (0, half + 1):
            ref[x] = jnp.zeros(ref.shape[1:], F32)
    inner = slice(8, 8 + half_rows)
    for x in range(half):
        y1m[x + 1, inner, :] = v1m[x + 1, inner, :] + w1m[x] * e1m[x // 2]
        y1s[x + 1, inner, :] = v1s[x + 1, inner, :] + w1s[x] * e1s[x // 2]

    def up_1(x):
        main, side, main_n, side_n = neighbours(y1m, y1s, x + 1, 8, half_rows, 2)
        for f, y, near, g, inverses in ((f1m, main, main_n, g1m, i1m), (f1s, side, side_n, g1s, i1s)):
            e1 = (0.2 * y + g[x + 1, inner, :] + K * near) * inverses[x]
            f[x, pl.ds(0, half_rows, stride=2), :] = e1
            f[x, pl.ds(1, half_rows, stride=2), :] = e1

    each(half, up_1, 12)
    base = own // 2
    extent_rows = fw.shape[1]
    for i in range(tall + 2):
        parent = jnp.clip(base + (i + 1) // 2 - 1, 0, half - 1)
        x = own + (i - 1)
        weights = fw[jnp.clip(x, 0, extent - 1)] if i in (0, tall + 1) else fw[x]
        value = vm[x + 1, 8 : 8 + extent_rows, :] + weights * f1m[parent]
        if i in (0, tall + 1):
            value = keep((x >= 0) & (x < extent), value)
        else:
            y0s[i - 1] = (
                vs[x + 1, 8 + HALO : 8 + HALO + wide, :] + ws[x, HALO : HALO + wide, :] * f1s[parent, HALO : HALO + wide, :]
            )
        y0m[i] = value

    def up_0(i):
        main = y0m[i + 1, pl.ds(HALO, wide), :]
        main_z, _ = z_sum(main, y0s[i], 1)
        near = xy_sum(y0m, i + 1, HALO, wide) + main_z
        out[i] = (0.2 * main + gm[own + i + 1, 8 + HALO : 8 + HALO + wide, :] + K * near) * i0[i]

    each(tall, up_0, 16)


def size_of(shape):
    return 4 * math.prod(shape)


def call(kernel, outs, scratch=(), resident=True, fetch=False):
    limit = 8 * 2**20 + sum(map(size_of, scratch)) + sum(size_of(s) for s in outs if size_of(s) > 2**20)
    run = pl.pallas_call(
        kernel,
        out_shape=[(pltpu.VMEM if resident and size_of(s) <= 2**20 else jax.ShapeDtypeStruct)(s, F32) for s in outs],
        scratch_shapes=[pltpu.VMEM(s, F32) for s in scratch],
        compiler_params=pltpu.CompilerParams(vmem_limit_bytes=min(limit, 56 * 2**20)),
    )

    def place(value):
        small = size_of(value.shape) <= 2**20 and not fetch
        return pltpu.with_memory_space_constraint(value, pltpu.VMEM if small else pltpu.HBM)

    return lambda *values: run(*map(place, values))


def plain_halo(mesh_shape, own, frames):
    n_gx = mesh_shape[0]
    tall = own[0].shape[0]
    extent, tiles = frames[1][0], own[2].shape[1] // 128
    inverses = 1.0 / own[1]
    own = (K * own[0] * inverses, *own[1:])
    parts = ()
    if n_gx > 1:
        odd = lax.axis_index("gx") % 2
        for first in range(2):
            start = jnp.where(odd == first, tall - HALO, 0)
            faces = [lax.dynamic_slice_in_dim(a, start, HALO, 0) for a in own[:2]] + [own[2]]
            parts += tuple(swap(a, "gx", first) for a in faces)
    slab = (2 * extent + 3 * tiles, HALO, 128)
    y_slabs = call(functools.partial(y_pack_kernel, mesh_shape), [slab, slab])(*own, *parts)
    y_parts = [ring(s, "gy", step) for s, step in zip(y_slabs, (1, -1))]
    fb, fw, matrix, z_a, z_b = call(functools.partial(z_pack_kernel, mesh_shape), frames)(*own, *parts, *y_parts)
    return fb, fw, matrix, ring(z_a, "gz", 1), ring(z_b, "gz", -1), inverses


def shared_halo(mesh_shape, own, frames):
    tall, wide = own[0].shape[:2]
    tiles = own[2].shape[1] // 128
    strips, groups, per = (tiles + 7) // 8, tall // HALO, wide // 8
    z_shape = (groups * per + strips, HALO, 128)
    y_shape = (2 * tall + tiles, HALO, 128)
    x_shape = (2 * per * tall + tiles, HALO, 128)
    outs = [z_shape, z_shape, y_shape, y_shape, x_shape] + [a.shape for a in own] + [own[0].shape]
    z_tail, z_head, y_tail, y_head, x_own, *here, inverses = call(face_kernel, outs, fetch=True)(*own)

    z_got = (ring(z_tail, "gz", 1), ring(z_head, "gz", -1))
    y_got = (ring(y_tail, "gy", 1), ring(y_head, "gy", -1))
    other = swap(x_own, "gx", 0)
    z_got = lax.optimization_barrier(z_got)
    edge = (2 * (groups + strips), HALO, 128)
    both = (2 * z_shape[0], HALO, 128)
    edge_tail, edge_head, z_both = call(functools.partial(y_edge_kernel, groups, per), [edge, edge, both])(*z_got)
    edge_got = (ring(edge_tail, "gy", 1), ring(edge_head, "gy", -1))
    z_other = swap(z_both, "gx", 0)
    y_other = [swap(y, "gx", 0) for y in y_got]
    edge_other = [swap(y, "gx", 0) for y in edge_got]
    made = call(functools.partial(frame_kernel, mesh_shape), frames)(
        *here, other, *z_got, z_other, *y_got, *y_other, *edge_got, *edge_other
    )
    return *made, inverses


def per_device(mesh_shape, sources, stiffness, coarse_inverse):
    n_gx, n_gy, n_gz = mesh_shape
    count = n_gx * n_gy * n_gz
    tall, wide, deep = stiffness.shape
    cells = coarse_inverse.shape[1]
    assert sources.shape[0] == 1 and deep == 128 and tall == 16 and wide == 16 and n_gz % 4 == 0 and cells % 128 == 0
    tiles = cells // 128
    extent = frame_extent(n_gx, tall)
    source = sources[0]
    own = (source, stiffness, coarse_inverse)
    rows = wide + 2 * HALO
    frame, padded = (extent, rows, 128), (extent + 2, rows + 16, 128)
    z_slab = (extent // HALO + (tiles + 1) // 2, rows, 128)
    frames = [padded, frame, (9 * tiles, HALO, 128), z_slab, z_slab]
    exchange = shared_halo if n_gx == 2 else plain_halo
    gm, fw, matrix, z_a, z_b, inverses = exchange(mesh_shape, own, frames)
    half, half_rows = extent // 2, rows // 2
    level1, plain1 = (half + 2, half_rows + 16, 128), (half, half_rows, 128)
    window, face = (tall + 2, rows, 128), (tall, wide, 128)
    message = (count, wide // 2, 128)
    outs = [message, padded, padded, padded, frame] + [level1] * 2 + [plain1] * 2 + [level1] * 2 + [plain1] * 2
    scratch = [(half, rows, 128)] * 4 + [(2, tall // 4, wide // 2, 128)]
    send, *state = call(functools.partial(down_kernel, mesh_shape), outs, scratch)(gm, fw, z_a, z_b)
    recv = lax.all_to_all(send, AXES, 0, 0, tiled=True)
    size_x, size_y, size_z = n_gx * tall // 4, n_gy * wide // 4, n_gz * deep // 4
    pad2 = (size_x + 2, size_y + 16, size_z)
    x3, rows3 = size_x // 2, size_y // 2
    pad3 = (x3 + 2, rows3 + 16, size_z)
    n2, lane_tiles = extent // 4, size_z // 128
    scratch = [
        pad2, *[(size_x, size_y, size_z)] * 2, pad2, pad2, (size_x + 4, lane_tiles, size_y + 16, 128), (x3, lane_tiles, size_y, 128),
        (lane_tiles, size_y, 128), (lane_tiles, size_y, 128), pad3, *[(x3, rows3, size_z)] * 2, pad3, pad3,
        (x3 // 2 + 2, lane_tiles, rows3 + 16, 128),
        (x3 // 2, rows3 // 2, size_z), level1, level1, (n2, 16, 128), (n2, 16, 128),
        (half, rows, 128), (half, rows, 128), window, face,
    ]
    (pressure,) = call(functools.partial(up_kernel, mesh_shape), [face], scratch, False)(
        recv, matrix, z_a, z_b, gm, fw, inverses, *state
    )
    return pressure[None]


def solution(mesh):
    mesh_shape = tuple(mesh.shape[a] for a in AXES)
    in_specs = (P(None, "gx", "gy", "gz"), P("gx", "gy", "gz"), P(AXES, None))
    return jax.shard_map(
        functools.partial(per_device, mesh_shape),
        mesh=mesh,
        in_specs=in_specs,
        out_specs=P(None, "gx", "gy", "gz"),
        check_vma=False,
    )
```

```python
import functools
import math

import jax
import jax.numpy as jnp
from jax import lax
from jax.experimental import pallas as pl
from jax.experimental.pallas import tpu as pltpu
from jax.sharding import PartitionSpec as P


damping = 0.8
K = damping / 6.0
AXES = ("gx", "gy", "gz")
HALO = 8
F32 = jnp.float32


def swap(values, axis, first):
    count = lax.axis_size(axis)
    partner = list(range(count))
    for i in range(first, count - 1, 2):
        partner[i], partner[i + 1] = i + 1, i
    return lax.ppermute(values, axis, list(enumerate(partner)))


def ring(values, axis, step):
    count = lax.axis_size(axis)
    return lax.ppermute(values, axis, [(i, (i + step) % count) for i in range(count)])


def iota(shape, dim):
    return lax.broadcasted_iota(jnp.int32, shape, dim)


def roll(values, amount):
    size = values.shape[-1]
    if isinstance(amount, int):
        amount = amount % size
        if amount == 0:
            return values
    return pltpu.roll(values, amount, values.ndim - 1)


def z_sum(main, side, step):
    lane = iota(main.shape, main.ndim - 1)
    size = main.shape[-1]
    main_up, side_up = roll(main, -step), roll(side, -step)
    main_dn, side_dn = roll(main, step), roll(side, step)
    last = lane >= size - step
    first = lane < step
    main_sum = jnp.where(last, side_up, main_up) + jnp.where(first, side_dn, main_dn)
    side_sum = jnp.where(last, main_up, side_up) + jnp.where(first, main_dn, side_dn)
    return main_sum, side_sum


def xy_sum(ref, x, row, rows):
    total = ref[x - 1, pl.ds(row, rows), :] + ref[x + 1, pl.ds(row, rows), :]
    return total + ref[x, pl.ds(row - 1, rows), :] + ref[x, pl.ds(row + 1, rows), :]


def neighbours(main_ref, side_ref, x, row, rows, step):
    main = main_ref[x, pl.ds(row, rows), :]
    side = side_ref[x, pl.ds(row, rows), :]
    main_z, side_z = z_sum(main, side, step)
    return main, side, xy_sum(main_ref, x, row, rows) + main_z, xy_sum(side_ref, x, row, rows) + side_z


def global_neighbours(ref, x, row, rows, step):
    main = ref[x, pl.ds(row, rows), :]
    lane = iota(main.shape, 1)
    size = main.shape[-1]
    up = jnp.where(lane >= size - step, 0.0, roll(main, -step))
    dn = jnp.where(lane < step, 0.0, roll(main, step))
    return main, xy_sum(ref, x, row, rows) + up + dn


def lane_pairs(values, step):
    lane = iota(values.shape, values.ndim - 1)
    return values + jnp.where((lane // step) % 2 == 0, roll(values, -step), roll(values, step))


def inverse(weights):
    return jnp.where(weights > 0.0, 1.0 / jnp.where(weights > 0.0, weights, 1.0), 0.0)


def select_lanes(values, chosen):
    first = values.astype(jnp.bfloat16)
    rest = values - first.astype(F32)
    second = rest.astype(jnp.bfloat16)
    third = (rest - second.astype(F32)).astype(jnp.bfloat16)
    matrix = chosen.astype(F32).astype(jnp.bfloat16)
    parts = [jnp.dot(p, matrix, preferred_element_type=F32) for p in (first, second, third)]
    return parts[0] + (parts[1] + parts[2])


def tiled(value):
    return [value[:, t * 128 : (t + 1) * 128] for t in range(value.shape[1] // 128)]


def joined(parts):
    return parts[0] if len(parts) == 1 else jnp.concatenate(parts, axis=1)


def row_pairs(ref, rows):
    return joined([ref[t, pl.ds(0, rows // 2, stride=2), :] + ref[t, pl.ds(1, rows // 2, stride=2), :] for t in range(ref.shape[0])])


def each(count, body, width=1):
    while count % width:
        width -= 1
    if count == width:
        for i in range(count):
            body(i)
        return

    def step(i, carry):
        for j in range(width):
            body(i * width + j)
        return carry

    lax.fori_loop(0, count // width, step, 0)


def pair_places(axis, count, own, tall):
    index = lax.axis_index(axis)
    odd = index % 2
    first = dict(place=jnp.where(odd == 0, own + tall, 0), high=odd == 0, valid=jnp.where(odd == 0, index + 1, index - 1) < count)
    other = jnp.where(odd == 0, index - 1, index + 1)
    second = dict(place=jnp.where(odd == 0, 0, own + tall), high=odd == 1, valid=(other >= 0) & (other < count))
    return index, odd, (first, second)


def x_frame(count, tall):
    index = lax.axis_index("gx")
    odd = index % 2
    if count == 1:
        return index, 0, ()
    own = HALO * odd if count == 2 else HALO
    _, _, (first, second) = pair_places("gx", count, own, tall)
    if count == 2:
        first["source"] = jnp.where(odd == 0, 0, tall - HALO)
        return index, own, (first,)
    first["source"] = second["source"] = 0
    return index, own, (first, second)


def y_ends(count, wide):
    index = lax.axis_index("gy")
    return (dict(valid=index > 0, place=0, high=0), dict(valid=index < count - 1, place=wide + HALO, high=1))


def inner_frames(padded, plain):
    extent, rows = plain.shape[0], plain.shape[1]
    for x in (0, extent + 1):
        padded[x] = jnp.zeros(padded.shape[1:], F32)
    return padded.at[pl.ds(1, extent), pl.ds(8, rows), :], plain


def frame_extent(count, tall):
    return tall + (0 if count == 1 else HALO if count == 2 else 2 * HALO)


def keep(valid, values):
    return jnp.where(valid, values, jnp.zeros_like(values))


def y_pack_kernel(mesh_shape, *refs):
    n_gx, _, _ = mesh_shape
    n_in = 3 * (1 + min(n_gx - 1, 2))
    own_refs, part_refs, outs = refs[:3], refs[3:n_in], refs[n_in:]
    tall, wide = own_refs[0].shape[0], own_refs[0].shape[1]
    extent = frame_extent(n_gx, tall)
    tiles = own_refs[2].shape[1] // 128
    _, own, parts = x_frame(n_gx, tall)
    for out, start in zip(outs, (wide - HALO, 0)):
        rows = pl.ds(start, HALO)
        for a in range(2):
            out[pl.ds(a * extent + own, tall)] = own_refs[a][:, rows, :]
            for part, ref in zip(parts, (part_refs[a : a + 1], part_refs[3 + a : 4 + a])):
                out[pl.ds(a * extent + part["place"], HALO)] = keep(part["valid"], ref[0][pl.ds(part["source"], HALO), rows, :])
        base = 2 * extent
        for side in (0, 2):
            for t in range(tiles):
                out[base + side * tiles + t] = jnp.zeros((HALO, 128), F32)
        for t in range(tiles):
            out[base + tiles + t] = own_refs[2][:, t * 128 : (t + 1) * 128]
            for part, ref in zip(parts, (part_refs[2:3], part_refs[5:6])):
                side = jnp.where(part["high"], 2, 0)
                out[base + side * tiles + t] = keep(part["valid"], ref[0][:, t * 128 : (t + 1) * 128])


def z_pack_kernel(mesh_shape, *refs):
    n_gx, n_gy, _ = mesh_shape
    n_in = 3 * (1 + min(n_gx - 1, 2))
    own_refs, part_refs = refs[:3], refs[3:n_in]
    y_refs = refs[n_in : n_in + 2]
    frames = inner_frames(*refs[n_in + 2 : n_in + 4])
    rows_ref, z_outs = refs[n_in + 4], refs[n_in + 5 :]
    tall, wide = own_refs[0].shape[0], own_refs[0].shape[1]
    extent = frame_extent(n_gx, tall)
    tiles = own_refs[2].shape[1] // 128
    _, own, parts = x_frame(n_gx, tall)
    y_parts = y_ends(n_gy, wide)
    for a in range(2):
        frames[a][pl.ds(own, tall), HALO : HALO + wide, :] = own_refs[a][...]
        for part, ref in zip(parts, (part_refs[a : a + 1], part_refs[3 + a : 4 + a])):
            frames[a][pl.ds(part["place"], HALO), HALO : HALO + wide, :] = keep(part["valid"], ref[0][pl.ds(part["source"], HALO)])
        for part, ref in zip(y_parts, y_refs):
            rows = pl.ds(part["place"], HALO)
            frames[a][:, rows, :] = keep(part["valid"], ref[a * extent : (a + 1) * extent])
    for t in range(tiles):
        for side in (0, 2):
            rows_ref[(side * 3 + 1) * tiles + t] = jnp.zeros((HALO, 128), F32)
        rows_ref[4 * tiles + t] = own_refs[2][:, t * 128 : (t + 1) * 128]
        for part, ref in zip(parts, (part_refs[2:3], part_refs[5:6])):
            side = jnp.where(part["high"], 2, 0)
            rows_ref[(side * 3 + 1) * tiles + t] = keep(part["valid"], ref[0][:, t * 128 : (t + 1) * 128])
        for x_side in range(3):
            for part, ref in zip(y_parts, y_refs):
                side = 2 * part["high"]
                rows_ref[(x_side * 3 + side) * tiles + t] = keep(part["valid"], ref[2 * extent + x_side * tiles + t])
    groups = extent // HALO
    for out, tail in zip(z_outs, (1, 0)):

        def put(group, packed):
            out[group] = packed

        pack_z(frames, put, tail)
        row = (HALO - 1) * tail
        for s in range((tiles + 1) // 2):
            out[groups + s] = jnp.zeros((4 * HALO, 128), F32)
        for t in range(tiles):
            for m in range(9):
                out[groups + t // 2, 16 * (t % 2) + m : 16 * (t % 2) + m + 1, :] = rows_ref[m * tiles + t, row : row + 1, :]


def z_ends(count):
    index = lax.axis_index("gz")
    return (dict(valid=index > 0, lane=120, row=-1), dict(valid=index < count - 1, lane=0, row=HALO))


def pack_z(frames, out, tail):
    rows = frames[0].shape[1]
    slot = iota((rows, 128), 1) // HALO
    for group in range(frames[0].shape[0] // HALO):
        packed = jnp.zeros((rows, 128), F32)
        for i in range(HALO):
            for a in range(2):
                at = (2 * i + a + 1 - tail) % 16
                piece = roll(frames[a][group * HALO + i], 8 * (tail + at))
                packed = jnp.where(slot == at, piece, packed)
        out(group, packed)


def face_kernel(*refs):
    source, weights, matrix, *outs = refs
    outs, y_outs, both, (b, w, own_matrix, own_inverse) = outs[:2], outs[2:4], outs[4], outs[5:]
    tall, wide = b.shape[0], b.shape[1]
    inverses = 1.0 / weights[...]
    own_inverse[...] = inverses
    b[...] = K * source[...] * inverses
    w[...] = weights[...]
    own_matrix[...] = matrix[...]
    tiles = matrix.shape[1] // 128
    strips = (tiles + 7) // 8
    per = wide // 8
    for out, tail in zip(outs, (1, 0)):

        def put(group, packed):
            for r in range(per):
                out[group * per + r] = packed[8 * r : 8 * r + 8]

        pack_z((b, w), put, tail)
        at = tall // HALO * per
        line = matrix[HALO - 1 : HALO, :] if tail else matrix[0:1, :]
        for strip in range(strips):
            out[at + strip] = jnp.zeros((8, 128), F32)
        for t in range(tiles):
            out[at + t // 8, t % 8 : t % 8 + 1, :] = line[:, t * 128 : (t + 1) * 128]
    for out, row in zip(y_outs, (wide - HALO, 0)):
        for a, ref in enumerate((b, w)):
            out[a * tall : (a + 1) * tall] = ref[:, row : row + HALO, :]
        for t in range(tiles):
            out[2 * tall + t] = matrix[:, t * 128 : (t + 1) * 128]
    at = 0
    for ref in (b, w):
        for r in range(per):
            both[at : at + tall] = ref[:, 8 * r : 8 * r + 8, :]
            at += tall
    for t in range(tiles):
        both[at + t] = matrix[:, t * 128 : (t + 1) * 128]


def y_edge_kernel(groups, per, *refs):
    z_refs, outs, both = refs[:2], refs[2:4], refs[4]
    size = z_refs[0].shape[0]
    strips = size - groups * per
    for out, r in zip(outs, (per - 1, 0)):
        for k, ref in enumerate(z_refs):
            at = k * (groups + strips)
            for group in range(groups):
                out[at + group] = ref[group * per + r]
            out[at + groups : at + groups + strips] = ref[groups * per : size]
    for k, ref in enumerate(z_refs):
        both[k * size : (k + 1) * size] = ref[...]


def frame_kernel(mesh_shape, *refs):
    n_gx, n_gy, _ = mesh_shape
    own_refs, other, z_refs, z_other = refs[:3], refs[3], refs[4:6], refs[6]
    y_refs, y_others, edge_refs, edge_others = refs[7:9], refs[9:11], refs[11:13], refs[13:15]
    frames, rows_ref, z_outs = inner_frames(*refs[15:17]), refs[17], refs[18:]
    tall, wide = own_refs[0].shape[0], own_refs[0].shape[1]
    extent = frame_extent(n_gx, tall)
    tiles = own_refs[2].shape[1] // 128
    strips, groups, per = (tiles + 7) // 8, tall // HALO, wide // 8
    _, own, parts = x_frame(n_gx, tall)
    place, source = parts[0]["place"], parts[0]["source"]
    y_parts = y_ends(n_gy, wide)
    far = jnp.where(parts[0]["high"], 2, 0)
    y_rows = [pl.ds(p["place"], HALO) for p in y_parts]
    y_side = [2 * p["high"] for p in y_parts]
    for a in range(2):
        frames[a][pl.ds(own, tall), HALO : HALO + wide, :] = own_refs[a][...]
        for r in range(per):
            rows = slice(HALO + 8 * r, HALO + 8 * r + 8)
            frames[a][pl.ds(place, HALO), rows, :] = other[pl.ds((a * per + r) * tall + source, HALO)]
        for part, rows, ref, ref_other in zip(y_parts, y_rows, y_refs, y_others):
            frames[a][pl.ds(own, tall), rows, :] = keep(part["valid"], ref[a * tall : (a + 1) * tall])
            frames[a][pl.ds(place, HALO), rows, :] = keep(part["valid"], ref_other[pl.ds(a * tall + source, HALO)])
    zero = jnp.zeros((HALO, 128), F32)
    for t in range(tiles):
        for side in range(3):
            rows_ref[((2 - far) * 3 + side) * tiles + t] = zero
        rows_ref[4 * tiles + t] = own_refs[2][:, t * 128 : (t + 1) * 128]
        rows_ref[(far * 3 + 1) * tiles + t] = other[2 * per * tall + t]
        for part, side, ref, ref_other in zip(y_parts, y_side, y_refs, y_others):
            rows_ref[(3 + side) * tiles + t] = keep(part["valid"], ref[2 * tall + t])
            rows_ref[(far * 3 + side) * tiles + t] = keep(part["valid"], ref_other[2 * tall + t])
    for k, (out, ref) in enumerate(zip(z_outs, z_refs)):
        base = k * (groups * per + strips)
        y_base = k * (groups + strips)
        total = extent // HALO
        for s in range((tiles + 1) // 2):
            out[total + s] = jnp.zeros((4 * HALO, 128), F32)
        for g in range(groups):
            for r in range(per):
                out[own // HALO + g, HALO + 8 * r : HALO + 8 * r + 8, :] = ref[g * per + r]
            for part, rows, y_ref in zip(y_parts, y_rows, edge_refs):
                out[own // HALO + g, rows, :] = keep(part["valid"], y_ref[y_base + g])
        for r in range(per):
            out[place // HALO, HALO + 8 * r : HALO + 8 * r + 8, :] = z_other[base + source // HALO * per + r]
        for part, rows, y_ref in zip(y_parts, y_rows, edge_others):
            out[place // HALO, rows, :] = keep(part["valid"], y_ref[y_base + source // HALO])
        for strip in range(strips):
            for x_side in range(3):
                if x_side == 1:
                    middle = ref[groups * per + strip]
                    edges = [keep(p["valid"], r[y_base + groups + strip]) for p, r in zip(y_parts, edge_refs)]
                else:
                    here = far == x_side
                    middle = keep(here, z_other[base + groups * per + strip])
                    edges = [keep(p["valid"] & here, r[y_base + groups + strip]) for p, r in zip(y_parts, edge_others)]
                low, high = edges
                for j in range(min(8, tiles - 8 * strip)):
                    t = 8 * strip + j
                    for side, values in enumerate((low, middle, high)):
                        m = 16 * (t % 2) + x_side * 3 + side
                        out[total + t // 2, m : m + 1, :] = values[j : j + 1]


def down_kernel(mesh_shape, *refs):
    n_gx, n_gy, n_gz = mesh_shape
    gm, fw, za, zb = refs[:4]
    send, vm, gs, vs, ws, v1m, v1s, w1m, w1s, g1m, g1s, i1m, i1s = refs[4:17]
    tm, ts, um, us, small = refs[17:]
    extent, rows = fw.shape[0], fw.shape[1]
    tall, wide = extent - frame_extent(n_gx, 0), rows - 2 * HALO
    half, half_rows = extent // 2, rows // 2
    ix, own, _ = x_frame(n_gx, tall)
    groups = extent // HALO
    for ref in (gs, vm, vs, g1m, g1s, v1m, v1s):
        for x in (0, ref.shape[0] - 1):
            ref[x] = jnp.zeros(ref.shape[1:], F32)

    ends, sides = z_ends(n_gz), y_ends(n_gy, wide)

    def inside(depth, step):
        row, lane = iota((depth, 128), 0), iota((depth, 128), 1)
        edge = HALO // step
        low, high = ((e["valid"].astype(F32)) for e in sides)
        main = jnp.where(row < edge, K * low, jnp.where(row >= depth - edge, K * high, K))
        low, high = (e["valid"].astype(F32) for e in ends)
        return main, main * jnp.where(lane >= 120, low, jnp.where(lane < HALO, high, 0.0))

    def present(x, step):
        if n_gx <= 2:
            return None
        edge = HALO // step
        out = ((x < edge) & (ix == 0)) | ((x >= extent // step - edge) & (ix == n_gx - 1))
        return 1.0 - out.astype(F32)

    lane = iota((rows, 128), 1)
    halo_lanes = jnp.where(lane >= 120, ends[0]["valid"].astype(F32), 0.0) + jnp.where(lane < HALO, ends[1]["valid"].astype(F32), 0.0)
    first_half = lane % 16 < HALO

    def load(group):
        low, high = za[group], zb[group]
        both = (jnp.where(first_half, low, high), jnp.where(first_half, high, low))
        for i in range(HALO):
            x = group * HALO + i
            gs[x + 1, 8 : 8 + rows, :] = roll(both[0], 120 - 16 * i) * halo_lanes
            ws[x] = roll(both[1], 112 - 16 * i) * halo_lanes

    each(groups, load, 4)

    def smooth(g_refs, v_refs, factors, x, depth, step):
        main, side, main_n, side_n = neighbours(*g_refs, x + 1, 8, depth, step)
        here = present(x, step)
        for ref, value, near, factor in zip(v_refs, (main, side), (main_n, side_n), factors):
            ref[x + 1, 8 : 8 + depth, :] = 1.2 * value + (factor if here is None else factor * here) * near

    factors = inside(rows, 1)
    each(extent, lambda x: smooth((gm, gs), (vm, vs), factors, x, rows, 1), 24)

    def residual(x2):
        for row in range(0, rows, 8):
            totals = None
            for j in range(2):
                x = 2 * x2 + j
                main, side, main_n, side_n = neighbours(vm, vs, x + 1, 8 + row, 8, 1)
                w_main, w_side = fw[x, row : row + 8, :], ws[x, row : row + 8, :]
                r_main = w_main * ((1.0 / K) * gm[x + 1, 8 + row : 16 + row, :] - 6.0 * main + main_n)
                r_side = w_side * ((1.0 / K) * gs[x + 1, 8 + row : 16 + row, :] - 6.0 * side + side_n)
                values = (r_main, r_side, w_main, w_side)
                totals = values if j == 0 else tuple(a + b for a, b in zip(totals, values))
            for ref, value in zip((tm, ts, um, us), totals):
                ref[x2, row : row + 8, :] = value

    each(half, residual, half)
    src, dst = iota((128, 128), 0), iota((128, 128), 1)
    pair = src // 2 == dst // 2

    def coarsen(first):
        rows_of = [
            ref[first * 4 + i, pl.ds(0, half_rows, stride=2), :] + ref[first * 4 + i, pl.ds(1, half_rows, stride=2), :]
            for i in range(4)
            for ref in (tm, um, ts, us)
        ]
        sums = select_lanes(jnp.concatenate(rows_of, axis=0), pair)
        for i in range(4):
            x = first * 4 + i
            for j, (w_out, g_out, i_out) in enumerate(((w1m, g1m, i1m), (w1s, g1s, i1s))):
                at = (4 * i + 2 * j) * half_rows
                weights = 0.0625 * sums[at + half_rows : at + 2 * half_rows]
                inverses = inverse(weights)
                w_out[x] = weights
                i_out[x] = inverses
                g_out[x + 1, 8 : 8 + half_rows, :] = (0.125 * K) * sums[at : at + half_rows] * inverses

    each(half // 4, coarsen, 4)

    factors_1 = inside(half_rows, 2)
    each(half, lambda x: smooth((g1m, g1s), (v1m, v1s), factors_1, x, half_rows, 2), 16)

    base = own // 2
    first_row = 8 + HALO // 2
    quarter, quarter_rows = tall // 4, wide // 4
    for x2 in range(quarter):
        total_r = total_w = None
        for j in range(2):
            x = base + 2 * x2 + j + 1
            main, _, main_n, _ = neighbours(v1m, v1s, x, first_row, wide // 2, 2)
            weights = w1m[x - 1, pl.ds(first_row - 8, wide // 2), :]
            res = weights * ((1.0 / K) * g1m[x, pl.ds(first_row, wide // 2), :] - 6.0 * main + main_n)
            total_r = res if j == 0 else total_r + res
            total_w = weights if j == 0 else total_w + weights
        small[0, x2] = total_r
        small[1, x2] = total_w
    q = []
    for a, factor in ((0, 0.125), (1, 0.0625)):
        for x2 in range(quarter):
            ref = small.at[a, x2]
            both = ref[pl.ds(0, quarter_rows, stride=2), :] + ref[pl.ds(1, quarter_rows, stride=2), :]
            q.append(factor * both)
    stacked = jnp.concatenate([jnp.concatenate(q[:quarter], axis=0), jnp.concatenate(q[quarter:], axis=0)], axis=0)
    src, dst = iota((128, 128), 0), iota((128, 128), 1)
    cell = 4 * (dst % 32)
    compact = select_lanes(stacked, (src == cell) | (src == cell + 2))
    block = iota((quarter_rows, 128), 1) // 32
    gz = lax.axis_index("gz")
    out = []
    for a in range(2):
        packed = jnp.zeros((quarter_rows, 128), F32)
        for x2 in range(quarter):
            r = (a * quarter + x2) * quarter_rows
            packed = jnp.where(block == lax.rem(gz + x2, 4), compact[r : r + quarter_rows], packed)
        out.append(packed)
    message = jnp.concatenate(out, axis=0)

    def copy(d):
        send[d] = message

    each(send.shape[0], copy, 8)


def up_kernel(mesh_shape, *refs):
    n_gx, n_gy, n_gz = mesh_shape
    recv, rows_ref, za, zb, gm, fw, i0, vm, _, vs, ws, v1m, v1s, w1m, w1s, g1m, g1s, i1m, i1s, out = refs[:20]
    g2, w2, i2, v2, y2, e2, p2, t3, u3, g3, w3, i3, v3, y3, p3, b4, y1m, y1s, e1m, e1s, f1m, f1s, y0m, y0s = refs[20:]
    tall, wide = out.shape[0], out.shape[1]
    size_x, size_z = w2.shape[0], w2.shape[2]
    size_y = w2.shape[1]
    ix, own, _ = x_frame(n_gx, tall)
    iy, iz = lax.axis_index("gy"), lax.axis_index("gz")
    quarter, quarter_rows = tall // 4, wide // 4
    extent = frame_extent(n_gx, tall)
    half, half_rows = w1m.shape[0], w1m.shape[1]

    def clear(ref):
        count, depth, size = ref.shape
        zero = jnp.zeros((8, size), F32)
        for x in range(count):
            ref[x, 0:8, :] = zero
            ref[x, depth - 8 : depth, :] = zero
        for x in (0, count - 1):
            ref[x] = jnp.zeros((depth, size), F32)

    for ref in (g2, v2, y2, g3, v3, y3):
        clear(ref)
    e2[...] = jnp.zeros(e2.shape, F32)
    p3[...] = jnp.zeros(p3.shape, F32)

    lane = iota((quarter_rows, 128), 1)
    block = lane // 32
    for gx in range(n_gx):
        for gy in range(n_gy):
            for x in range(quarter):
                tiles_b, tiles_w = [], []
                for tile in range(size_z // 128):
                    picked = [jnp.zeros((quarter_rows, 128), F32)] * 2
                    for j in range(4):
                        gz = tile * 4 + j
                        d = (gx * n_gy + gy) * n_gz + gz
                        mask = block == (gz + x) % 4
                        for a in range(2):
                            piece = recv[d, a * quarter_rows : (a + 1) * quarter_rows, :]
                            picked[a] = jnp.where(mask, piece, picked[a])
                    tiles_b.append(roll(picked[0], -32 * x))
                    tiles_w.append(roll(picked[1], -32 * x))
                weights = joined(tiles_w)
                inverses = 1.0 / weights
                w2[gx * quarter + x, gy * quarter_rows : (gy + 1) * quarter_rows, :] = weights
                i2[gx * quarter + x, gy * quarter_rows : (gy + 1) * quarter_rows, :] = inverses
                g2[gx * quarter + x + 1, 8 + gy * quarter_rows : 8 + (gy + 1) * quarter_rows, :] = K * joined(tiles_b) * inverses

    def smooth(g, v, x, rows, step):
        main, near = global_neighbours(g, x + 1, 8, rows, step)
        v[x + 1, 8 : 8 + rows, :] = 1.2 * main + K * near

    def resid(g, v, w, x, rows, step):
        main, near = global_neighbours(v, x + 1, 8, rows, step)
        return w[x] * ((1.0 / K) * g[x + 1, 8 : 8 + rows, :] - 6.0 * main + near)

    each(size_x, lambda x: smooth(g2, v2, x, size_y, 1), 8)
    rows3, x3 = size_y // 2, size_x // 2

    def restrict_2(x):
        for t, part in enumerate(tiled(resid(g2, v2, w2, 2 * x, size_y, 1) + resid(g2, v2, w2, 2 * x + 1, size_y, 1))):
            t3[t] = part
        for t, part in enumerate(tiled(w2[2 * x] + w2[2 * x + 1])):
            u3[t] = part
        pairs = lambda ref: lane_pairs(row_pairs(ref, size_y), 1)
        weights = 0.0625 * pairs(u3)
        inverses = 1.0 / weights
        w3[x] = weights
        i3[x] = inverses
        g3[x + 1, 8 : 8 + rows3, :] = (0.125 * K) * pairs(t3) * inverses

    each(x3, restrict_2, 4)
    each(x3, lambda x: smooth(g3, v3, x, rows3, 2), 8)
    rows4, x4 = rows3 // 2, x3 // 2

    def restrict_3(x):
        for t, part in enumerate(tiled(resid(g3, v3, w3, 2 * x, rows3, 2) + resid(g3, v3, w3, 2 * x + 1, rows3, 2))):
            t3[t, 0:rows3, :] = part
        b4[x] = 0.125 * row_pairs(t3, rows3)

    each(x4, restrict_3, 4)

    tiles = rows_ref.shape[0] // 9
    coarse_z = size_z // 4
    per = 128 // coarse_z
    src, dst = iota((size_z, 128), 0), iota((size_z, 128), 1)
    values = b4[0] if x4 == 1 else jnp.concatenate([b4[x] for x in range(x4)], axis=0)
    cell = 4 * (dst % coarse_z)
    compact = select_lanes(values, (src == cell) | (src == cell + 2))
    place = iota((x4 * rows4, 128), 0) % per == iota((x4 * rows4, 128), 1) // coarse_z
    compact = jnp.where(place, compact, 0.0)
    vectors = [jnp.sum(compact[t * per : (t + 1) * per], axis=0, keepdims=True) for t in range(tiles)]
    ends = z_ends(n_gz)
    groups = extent // HALO
    fine = iota((HALO, size_z), 1) // 4
    fine_row = fine == iz * HALO + iota((HALO, size_z), 0)
    edge_row = iota((16, 128), 0)
    first_total = [None, None]
    for k, ref in enumerate((za, zb)):
        total = None
        for t in range(tiles):
            piece = ref[groups + t // 2, 16 * (t % 2) : 16 * (t % 2) + 16, :] * vectors[t]
            total = piece if total is None else total + piece
        first_total[k] = jnp.sum(total, axis=1, keepdims=True) * ends[k]["valid"].astype(F32)
    z_lane = iota((16, size_z), 1) // 4
    spread = None
    for k in range(2):
        piece = jnp.where(z_lane == iz * HALO + ends[k]["row"], first_total[k], 0.0)
        spread = piece if spread is None else spread + piece
    for m in range(9):
        total = None
        for t in range(tiles):
            piece = rows_ref[m * tiles + t] * vectors[t]
            total = piece if total is None else total + piece
        values = jnp.sum(total, axis=1, keepdims=True)
        line = jnp.sum(jnp.where(fine_row, values, 0.0), axis=0, keepdims=True) + spread[m : m + 1, :]
        row = 8 + 2 * (iy + (m % 3 - 1))
        for t, part in enumerate(tiled(line)):
            p3[ix + m // 3, t, pl.ds(row, 1), :] = part
            p3[ix + m // 3, t, pl.ds(row + 1, 1), :] = part

    def lift(y, v, w, p, x, px, rows, row):
        coarse = joined([p[px, t, row : row + rows, :] for t in range(p.shape[1])])
        y[x + 1, 8 : 8 + rows, :] = v[x + 1, 8 : 8 + rows, :] + w[x] * coarse

    def relax(y, g, inverses, x, rows, step):
        main, near = global_neighbours(y, x + 1, 8, rows, step)
        return (0.2 * main + g[x + 1, 8 : 8 + rows, :] + K * near) * inverses[x]

    each(x3, lambda x: lift(y3, v3, w3, p3, x, x // 2 + 1, rows3, 8), 8)

    def up_3(x):
        for t, e3 in enumerate(tiled(relax(y3, g3, i3, x, rows3, 2))):
            p2[x, t, pl.ds(0, rows3, stride=2), :] = e3
            p2[x, t, pl.ds(1, rows3, stride=2), :] = e3

    each(x3, up_3, 4)
    each(size_x, lambda x: lift(y2, v2, w2, p2, x, x // 2, size_y, 0), 8)

    def up_2(x):
        for t, part in enumerate(tiled(relax(y2, g2, i2, x, size_y, 1))):
            e2[x + 2, t, 8 : 8 + size_y, :] = part

    each(size_x, up_2, 8)

    src, dst = iota((size_z, 256), 0), iota((size_z, 256), 1)
    start = iz * 32
    cell = jnp.where(dst < 128, dst // 4, jnp.where(dst < 192, 32 + (dst - 128) // 4, -1 - (255 - dst) // 4))
    widen = src == start + cell
    n2 = extent // 4
    x_start = ix * quarter - own // 4
    y_start = 8 + iy * quarter_rows - HALO // 4
    spread = None
    for t in range(size_z // 128):
        stacked = jnp.concatenate([e2[x_start + 2 + i, t, pl.ds(y_start, 8), :] for i in range(n2)], axis=0)
        part = select_lanes(stacked, widen[t * 128 : (t + 1) * 128])
        spread = part if spread is None else spread + part
    for i in range(n2):
        for ref, part in ((e1m, spread[i * 8 : i * 8 + 8, :128]), (e1s, spread[i * 8 : i * 8 + 8, 128:])):
            ref[i, pl.ds(0, 8, stride=2), :] = part
            ref[i, pl.ds(1, 8, stride=2), :] = part

    for ref in (y1m, y1s):
        for x in (0, half + 1):
            ref[x] = jnp.zeros(ref.shape[1:], F32)
    inner = slice(8, 8 + half_rows)
    for x in range(half):
        y1m[x + 1, inner, :] = v1m[x + 1, inner, :] + w1m[x] * e1m[x // 2]
        y1s[x + 1, inner, :] = v1s[x + 1, inner, :] + w1s[x] * e1s[x // 2]

    def up_1(x):
        main, side, main_n, side_n = neighbours(y1m, y1s, x + 1, 8, half_rows, 2)
        for f, y, near, g, inverses in ((f1m, main, main_n, g1m, i1m), (f1s, side, side_n, g1s, i1s)):
            e1 = (0.2 * y + g[x + 1, inner, :] + K * near) * inverses[x]
            f[x, pl.ds(0, half_rows, stride=2), :] = e1
            f[x, pl.ds(1, half_rows, stride=2), :] = e1

    each(half, up_1, 12)
    base = own // 2
    extent_rows = fw.shape[1]
    for i in range(tall + 2):
        parent = jnp.clip(base + (i + 1) // 2 - 1, 0, half - 1)
        x = own + (i - 1)
        weights = fw[jnp.clip(x, 0, extent - 1)] if i in (0, tall + 1) else fw[x]
        value = vm[x + 1, 8 : 8 + extent_rows, :] + weights * f1m[parent]
        if i in (0, tall + 1):
            value = keep((x >= 0) & (x < extent), value)
        else:
            y0s[i - 1] = (
                vs[x + 1, 8 + HALO : 8 + HALO + wide, :] + ws[x, HALO : HALO + wide, :] * f1s[parent, HALO : HALO + wide, :]
            )
        y0m[i] = value

    def up_0(i):
        main = y0m[i + 1, pl.ds(HALO, wide), :]
        main_z, _ = z_sum(main, y0s[i], 1)
        near = xy_sum(y0m, i + 1, HALO, wide) + main_z
        out[i] = (0.2 * main + gm[own + i + 1, 8 + HALO : 8 + HALO + wide, :] + K * near) * i0[i]

    each(tall, up_0, 16)


def size_of(shape):
    return 4 * math.prod(shape)


def call(kernel, outs, scratch=(), resident=True, fetch=False):
    limit = 8 * 2**20 + sum(map(size_of, scratch)) + sum(size_of(s) for s in outs if size_of(s) > 2**20)
    run = pl.pallas_call(
        kernel,
        out_shape=[(pltpu.VMEM if resident and size_of(s) <= 2**20 else jax.ShapeDtypeStruct)(s, F32) for s in outs],
        scratch_shapes=[pltpu.VMEM(s, F32) for s in scratch],
        compiler_params=pltpu.CompilerParams(vmem_limit_bytes=min(limit, 56 * 2**20)),
    )

    def place(value):
        small = size_of(value.shape) <= 2**20 and not fetch
        return pltpu.with_memory_space_constraint(value, pltpu.VMEM if small else pltpu.HBM)

    return lambda *values: run(*map(place, values))


def plain_halo(mesh_shape, own, frames):
    n_gx = mesh_shape[0]
    tall = own[0].shape[0]
    extent, tiles = frames[1][0], own[2].shape[1] // 128
    inverses = 1.0 / own[1]
    own = (K * own[0] * inverses, *own[1:])
    parts = ()
    if n_gx > 1:
        odd = lax.axis_index("gx") % 2
        for first in range(2):
            start = jnp.where(odd == first, tall - HALO, 0)
            faces = [lax.dynamic_slice_in_dim(a, start, HALO, 0) for a in own[:2]] + [own[2]]
            parts += tuple(swap(a, "gx", first) for a in faces)
    slab = (2 * extent + 3 * tiles, HALO, 128)
    y_slabs = call(functools.partial(y_pack_kernel, mesh_shape), [slab, slab])(*own, *parts)
    y_parts = [ring(s, "gy", step) for s, step in zip(y_slabs, (1, -1))]
    fb, fw, matrix, z_a, z_b = call(functools.partial(z_pack_kernel, mesh_shape), frames)(*own, *parts, *y_parts)
    return fb, fw, matrix, ring(z_a, "gz", 1), ring(z_b, "gz", -1), inverses


def shared_halo(mesh_shape, own, frames):
    tall, wide = own[0].shape[:2]
    tiles = own[2].shape[1] // 128
    strips, groups, per = (tiles + 7) // 8, tall // HALO, wide // 8
    z_shape = (groups * per + strips, HALO, 128)
    y_shape = (2 * tall + tiles, HALO, 128)
    x_shape = (2 * per * tall + tiles, HALO, 128)
    outs = [z_shape, z_shape, y_shape, y_shape, x_shape] + [a.shape for a in own] + [own[0].shape]
    z_tail, z_head, y_tail, y_head, x_own, *here, inverses = call(face_kernel, outs, fetch=True)(*own)

    z_got = (ring(z_tail, "gz", 1), ring(z_head, "gz", -1))
    y_got = (ring(y_tail, "gy", 1), ring(y_head, "gy", -1))
    other = swap(x_own, "gx", 0)
    z_got = lax.optimization_barrier(z_got)
    edge = (2 * (groups + strips), HALO, 128)
    both = (2 * z_shape[0], HALO, 128)
    edge_tail, edge_head, z_both = call(functools.partial(y_edge_kernel, groups, per), [edge, edge, both])(*z_got)
    edge_got = (ring(edge_tail, "gy", 1), ring(edge_head, "gy", -1))
    z_other = swap(z_both, "gx", 0)
    y_other = [swap(y, "gx", 0) for y in y_got]
    edge_other = [swap(y, "gx", 0) for y in edge_got]
    made = call(functools.partial(frame_kernel, mesh_shape), frames)(
        *here, other, *z_got, z_other, *y_got, *y_other, *edge_got, *edge_other
    )
    return *made, inverses


def per_device(mesh_shape, sources, stiffness, coarse_inverse):
    n_gx, n_gy, n_gz = mesh_shape
    count = n_gx * n_gy * n_gz
    tall, wide, deep = stiffness.shape
    cells = coarse_inverse.shape[1]
    assert sources.shape[0] == 1 and deep == 128 and tall == 16 and wide == 16 and n_gz % 4 == 0 and cells % 128 == 0
    tiles = cells // 128
    extent = frame_extent(n_gx, tall)
    source = sources[0]
    own = (source, stiffness, coarse_inverse)
    rows = wide + 2 * HALO
    frame, padded = (extent, rows, 128), (extent + 2, rows + 16, 128)
    z_slab = (extent // HALO + (tiles + 1) // 2, rows, 128)
    frames = [padded, frame, (9 * tiles, HALO, 128), z_slab, z_slab]
    exchange = shared_halo if n_gx == 2 else plain_halo
    gm, fw, matrix, z_a, z_b, inverses = exchange(mesh_shape, own, frames)
    half, half_rows = extent // 2, rows // 2
    level1, plain1 = (half + 2, half_rows + 16, 128), (half, half_rows, 128)
    window, face = (tall + 2, rows, 128), (tall, wide, 128)
    message = (count, wide // 2, 128)
    outs = [message, padded, padded, padded, frame] + [level1] * 2 + [plain1] * 2 + [level1] * 2 + [plain1] * 2
    scratch = [(half, rows, 128)] * 4 + [(2, tall // 4, wide // 2, 128)]
    send, *state = call(functools.partial(down_kernel, mesh_shape), outs, scratch)(gm, fw, z_a, z_b)
    recv = lax.all_to_all(send, AXES, 0, 0, tiled=True)
    size_x, size_y, size_z = n_gx * tall // 4, n_gy * wide // 4, n_gz * deep // 4
    pad2 = (size_x + 2, size_y + 16, size_z)
    x3, rows3 = size_x // 2, size_y // 2
    pad3 = (x3 + 2, rows3 + 16, size_z)
    n2, lane_tiles = extent // 4, size_z // 128
    scratch = [
        pad2, *[(size_x, size_y, size_z)] * 2, pad2, pad2, (size_x + 4, lane_tiles, size_y + 16, 128), (x3, lane_tiles, size_y, 128),
        (lane_tiles, size_y, 128), (lane_tiles, size_y, 128), pad3, *[(x3, rows3, size_z)] * 2, pad3, pad3,
        (x3 // 2 + 2, lane_tiles, rows3 + 16, 128),
        (x3 // 2, rows3 // 2, size_z), level1, level1, (n2, 16, 128), (n2, 16, 128),
        (half, rows, 128), (half, rows, 128), window, face,
    ]
    (pressure,) = call(functools.partial(up_kernel, mesh_shape), [face], scratch, False)(
        recv, matrix, z_a, z_b, gm, fw, inverses, *state
    )
    return pressure[None]


def solution(mesh):
    mesh_shape = tuple(mesh.shape[a] for a in AXES)
    in_specs = (P(None, "gx", "gy", "gz"), P("gx", "gy", "gz"), P(AXES, None))
    return jax.shard_map(
        functools.partial(per_device, mesh_shape),
        mesh=mesh,
        in_specs=in_specs,
        out_specs=P(None, "gx", "gy", "gz"),
        check_vma=False,
    )
```

```python
import functools
import math

import jax
import jax.numpy as jnp
from jax import lax
from jax.experimental import pallas as pl
from jax.experimental.pallas import tpu as pltpu
from jax.sharding import PartitionSpec as P


damping = 0.8
K = damping / 6.0
AXES = ("gx", "gy", "gz")
HALO = 8
F32 = jnp.float32


def swap(values, axis, first):
    count = lax.axis_size(axis)
    partner = list(range(count))
    for i in range(first, count - 1, 2):
        partner[i], partner[i + 1] = i + 1, i
    return lax.ppermute(values, axis, list(enumerate(partner)))


def ring(values, axis, step):
    count = lax.axis_size(axis)
    return lax.ppermute(values, axis, [(i, (i + step) % count) for i in range(count)])


def iota(shape, dim):
    return lax.broadcasted_iota(jnp.int32, shape, dim)


def roll(values, amount):
    size = values.shape[-1]
    if isinstance(amount, int):
        amount = amount % size
        if amount == 0:
            return values
    return pltpu.roll(values, amount, values.ndim - 1)


def z_sum(main, side, step):
    lane = iota(main.shape, main.ndim - 1)
    size = main.shape[-1]
    main_up, side_up = roll(main, -step), roll(side, -step)
    main_dn, side_dn = roll(main, step), roll(side, step)
    last = lane >= size - step
    first = lane < step
    main_sum = jnp.where(last, side_up, main_up) + jnp.where(first, side_dn, main_dn)
    side_sum = jnp.where(last, main_up, side_up) + jnp.where(first, main_dn, side_dn)
    return main_sum, side_sum


def xy_sum(ref, x, row, rows):
    total = ref[x - 1, pl.ds(row, rows), :] + ref[x + 1, pl.ds(row, rows), :]
    return total + ref[x, pl.ds(row - 1, rows), :] + ref[x, pl.ds(row + 1, rows), :]


def neighbours(main_ref, side_ref, x, row, rows, step):
    main = main_ref[x, pl.ds(row, rows), :]
    side = side_ref[x, pl.ds(row, rows), :]
    main_z, side_z = z_sum(main, side, step)
    return main, side, xy_sum(main_ref, x, row, rows) + main_z, xy_sum(side_ref, x, row, rows) + side_z


def global_neighbours(ref, x, row, rows, step):
    main = ref[x, pl.ds(row, rows), :]
    lane = iota(main.shape, 1)
    size = main.shape[-1]
    up = jnp.where(lane >= size - step, 0.0, roll(main, -step))
    dn = jnp.where(lane < step, 0.0, roll(main, step))
    return main, xy_sum(ref, x, row, rows) + up + dn


def lane_pairs(values, step):
    lane = iota(values.shape, values.ndim - 1)
    return values + jnp.where((lane // step) % 2 == 0, roll(values, -step), roll(values, step))


def inverse(weights):
    return jnp.where(weights > 0.0, 1.0 / jnp.where(weights > 0.0, weights, 1.0), 0.0)


def select_lanes(values, chosen):
    first = values.astype(jnp.bfloat16)
    rest = values - first.astype(F32)
    second = rest.astype(jnp.bfloat16)
    third = (rest - second.astype(F32)).astype(jnp.bfloat16)
    matrix = chosen.astype(F32).astype(jnp.bfloat16)
    parts = [jnp.dot(p, matrix, preferred_element_type=F32) for p in (first, second, third)]
    return parts[0] + (parts[1] + parts[2])


def tiled(value):
    return [value[:, t * 128 : (t + 1) * 128] for t in range(value.shape[1] // 128)]


def joined(parts):
    return parts[0] if len(parts) == 1 else jnp.concatenate(parts, axis=1)


def row_pairs(ref, rows):
    return joined([ref[t, pl.ds(0, rows // 2, stride=2), :] + ref[t, pl.ds(1, rows // 2, stride=2), :] for t in range(ref.shape[0])])


def each(count, body, width=1):
    while count % width:
        width -= 1
    if count == width:
        for i in range(count):
            body(i)
        return

    def step(i, carry):
        for j in range(width):
            body(i * width + j)
        return carry

    lax.fori_loop(0, count // width, step, 0)


def pair_places(axis, count, own, tall):
    index = lax.axis_index(axis)
    odd = index % 2
    first = dict(place=jnp.where(odd == 0, own + tall, 0), high=odd == 0, valid=jnp.where(odd == 0, index + 1, index - 1) < count)
    other = jnp.where(odd == 0, index - 1, index + 1)
    second = dict(place=jnp.where(odd == 0, 0, own + tall), high=odd == 1, valid=(other >= 0) & (other < count))
    return index, odd, (first, second)


def x_frame(count, tall):
    index = lax.axis_index("gx")
    odd = index % 2
    if count == 1:
        return index, 0, ()
    own = HALO * odd if count == 2 else HALO
    _, _, (first, second) = pair_places("gx", count, own, tall)
    if count == 2:
        first["source"] = jnp.where(odd == 0, 0, tall - HALO)
        return index, own, (first,)
    first["source"] = second["source"] = 0
    return index, own, (first, second)


def y_ends(count, wide):
    index = lax.axis_index("gy")
    return (dict(valid=index > 0, place=0, high=0), dict(valid=index < count - 1, place=wide + HALO, high=1))


def inner_frames(padded, plain):
    extent, rows = plain.shape[0], plain.shape[1]
    for x in (0, extent + 1):
        padded[x] = jnp.zeros(padded.shape[1:], F32)
    return padded.at[pl.ds(1, extent), pl.ds(8, rows), :], plain


def frame_extent(count, tall):
    return tall + (0 if count == 1 else HALO if count == 2 else 2 * HALO)


def keep(valid, values):
    return jnp.where(valid, values, jnp.zeros_like(values))


def y_pack_kernel(mesh_shape, *refs):
    n_gx, _, _ = mesh_shape
    n_in = 3 * (1 + min(n_gx - 1, 2))
    own_refs, part_refs, outs = refs[:3], refs[3:n_in], refs[n_in:]
    tall, wide = own_refs[0].shape[0], own_refs[0].shape[1]
    extent = frame_extent(n_gx, tall)
    tiles = own_refs[2].shape[1] // 128
    _, own, parts = x_frame(n_gx, tall)
    for out, start in zip(outs, (wide - HALO, 0)):
        rows = pl.ds(start, HALO)
        for a in range(2):
            out[pl.ds(a * extent + own, tall)] = own_refs[a][:, rows, :]
            for part, ref in zip(parts, (part_refs[a : a + 1], part_refs[3 + a : 4 + a])):
                out[pl.ds(a * extent + part["place"], HALO)] = keep(part["valid"], ref[0][pl.ds(part["source"], HALO), rows, :])
        base = 2 * extent
        for side in (0, 2):
            for t in range(tiles):
                out[base + side * tiles + t] = jnp.zeros((HALO, 128), F32)
        for t in range(tiles):
            out[base + tiles + t] = own_refs[2][:, t * 128 : (t + 1) * 128]
            for part, ref in zip(parts, (part_refs[2:3], part_refs[5:6])):
                side = jnp.where(part["high"], 2, 0)
                out[base + side * tiles + t] = keep(part["valid"], ref[0][:, t * 128 : (t + 1) * 128])


def z_pack_kernel(mesh_shape, *refs):
    n_gx, n_gy, _ = mesh_shape
    n_in = 3 * (1 + min(n_gx - 1, 2))
    own_refs, part_refs = refs[:3], refs[3:n_in]
    y_refs = refs[n_in : n_in + 2]
    frames = inner_frames(*refs[n_in + 2 : n_in + 4])
    rows_ref, z_outs = refs[n_in + 4], refs[n_in + 5 :]
    tall, wide = own_refs[0].shape[0], own_refs[0].shape[1]
    extent = frame_extent(n_gx, tall)
    tiles = own_refs[2].shape[1] // 128
    _, own, parts = x_frame(n_gx, tall)
    y_parts = y_ends(n_gy, wide)
    for a in range(2):
        frames[a][pl.ds(own, tall), HALO : HALO + wide, :] = own_refs[a][...]
        for part, ref in zip(parts, (part_refs[a : a + 1], part_refs[3 + a : 4 + a])):
            frames[a][pl.ds(part["place"], HALO), HALO : HALO + wide, :] = keep(part["valid"], ref[0][pl.ds(part["source"], HALO)])
        for part, ref in zip(y_parts, y_refs):
            rows = pl.ds(part["place"], HALO)
            frames[a][:, rows, :] = keep(part["valid"], ref[a * extent : (a + 1) * extent])
    for t in range(tiles):
        for side in (0, 2):
            rows_ref[(side * 3 + 1) * tiles + t] = jnp.zeros((HALO, 128), F32)
        rows_ref[4 * tiles + t] = own_refs[2][:, t * 128 : (t + 1) * 128]
        for part, ref in zip(parts, (part_refs[2:3], part_refs[5:6])):
            side = jnp.where(part["high"], 2, 0)
            rows_ref[(side * 3 + 1) * tiles + t] = keep(part["valid"], ref[0][:, t * 128 : (t + 1) * 128])
        for x_side in range(3):
            for part, ref in zip(y_parts, y_refs):
                side = 2 * part["high"]
                rows_ref[(x_side * 3 + side) * tiles + t] = keep(part["valid"], ref[2 * extent + x_side * tiles + t])
    groups = extent // HALO
    for out, tail in zip(z_outs, (1, 0)):

        def put(group, packed):
            out[group] = packed

        pack_z(frames, put, tail)
        row = (HALO - 1) * tail
        for s in range((tiles + 1) // 2):
            out[groups + s] = jnp.zeros((4 * HALO, 128), F32)
        for t in range(tiles):
            for m in range(9):
                out[groups + t // 2, 16 * (t % 2) + m : 16 * (t % 2) + m + 1, :] = rows_ref[m * tiles + t, row : row + 1, :]


def z_ends(count):
    index = lax.axis_index("gz")
    return (dict(valid=index > 0, lane=120, row=-1), dict(valid=index < count - 1, lane=0, row=HALO))


def pack_z(frames, out, tail):
    rows = frames[0].shape[1]
    slot = iota((rows, 128), 1) // HALO
    for group in range(frames[0].shape[0] // HALO):
        packed = jnp.zeros((rows, 128), F32)
        for i in range(HALO):
            for a in range(2):
                at = (2 * i + a + 1 - tail) % 16
                piece = roll(frames[a][group * HALO + i], 8 * (tail + at))
                packed = jnp.where(slot == at, piece, packed)
        out(group, packed)


def face_kernel(*refs):
    source, weights, matrix, *outs = refs
    outs, y_outs, both, (b, w, own_matrix, own_inverse) = outs[:2], outs[2:4], outs[4], outs[5:]
    tall, wide = b.shape[0], b.shape[1]
    inverses = 1.0 / weights[...]
    own_inverse[...] = inverses
    b[...] = K * source[...] * inverses
    w[...] = weights[...]
    own_matrix[...] = matrix[...]
    tiles = matrix.shape[1] // 128
    strips = (tiles + 7) // 8
    per = wide // 8
    for out, tail in zip(outs, (1, 0)):

        def put(group, packed):
            for r in range(per):
                out[group * per + r] = packed[8 * r : 8 * r + 8]

        pack_z((b, w), put, tail)
        at = tall // HALO * per
        line = matrix[HALO - 1 : HALO, :] if tail else matrix[0:1, :]
        for strip in range(strips):
            out[at + strip] = jnp.zeros((8, 128), F32)
        for t in range(tiles):
            out[at + t // 8, t % 8 : t % 8 + 1, :] = line[:, t * 128 : (t + 1) * 128]
    for out, row in zip(y_outs, (wide - HALO, 0)):
        for a, ref in enumerate((b, w)):
            out[a * tall : (a + 1) * tall] = ref[:, row : row + HALO, :]
        for t in range(tiles):
            out[2 * tall + t] = matrix[:, t * 128 : (t + 1) * 128]
    at = 0
    for ref in (b, w):
        for r in range(per):
            both[at : at + tall] = ref[:, 8 * r : 8 * r + 8, :]
            at += tall
    for t in range(tiles):
        both[at + t] = matrix[:, t * 128 : (t + 1) * 128]


def y_edge_kernel(groups, per, *refs):
    z_refs, outs, both = refs[:2], refs[2:4], refs[4]
    size = z_refs[0].shape[0]
    strips = size - groups * per
    for out, r in zip(outs, (per - 1, 0)):
        for k, ref in enumerate(z_refs):
            at = k * (groups + strips)
            for group in range(groups):
                out[at + group] = ref[group * per + r]
            out[at + groups : at + groups + strips] = ref[groups * per : size]
    for k, ref in enumerate(z_refs):
        both[k * size : (k + 1) * size] = ref[...]


def frame_kernel(mesh_shape, *refs):
    n_gx, n_gy, _ = mesh_shape
    own_refs, other, z_refs, z_other = refs[:3], refs[3], refs[4:6], refs[6]
    y_refs, y_others, edge_refs, edge_others = refs[7:9], refs[9:11], refs[11:13], refs[13:15]
    frames, rows_ref, z_outs = inner_frames(*refs[15:17]), refs[17], refs[18:]
    tall, wide = own_refs[0].shape[0], own_refs[0].shape[1]
    extent = frame_extent(n_gx, tall)
    tiles = own_refs[2].shape[1] // 128
    strips, groups, per = (tiles + 7) // 8, tall // HALO, wide // 8
    _, own, parts = x_frame(n_gx, tall)
    place, source = parts[0]["place"], parts[0]["source"]
    y_parts = y_ends(n_gy, wide)
    far = jnp.where(parts[0]["high"], 2, 0)
    y_rows = [pl.ds(p["place"], HALO) for p in y_parts]
    y_side = [2 * p["high"] for p in y_parts]
    for a in range(2):
        frames[a][pl.ds(own, tall), HALO : HALO + wide, :] = own_refs[a][...]
        for r in range(per):
            rows = slice(HALO + 8 * r, HALO + 8 * r + 8)
            frames[a][pl.ds(place, HALO), rows, :] = other[pl.ds((a * per + r) * tall + source, HALO)]
        for part, rows, ref, ref_other in zip(y_parts, y_rows, y_refs, y_others):
            frames[a][pl.ds(own, tall), rows, :] = keep(part["valid"], ref[a * tall : (a + 1) * tall])
            frames[a][pl.ds(place, HALO), rows, :] = keep(part["valid"], ref_other[pl.ds(a * tall + source, HALO)])
    zero = jnp.zeros((HALO, 128), F32)
    for t in range(tiles):
        for side in range(3):
            rows_ref[((2 - far) * 3 + side) * tiles + t] = zero
        rows_ref[4 * tiles + t] = own_refs[2][:, t * 128 : (t + 1) * 128]
        rows_ref[(far * 3 + 1) * tiles + t] = other[2 * per * tall + t]
        for part, side, ref, ref_other in zip(y_parts, y_side, y_refs, y_others):
            rows_ref[(3 + side) * tiles + t] = keep(part["valid"], ref[2 * tall + t])
            rows_ref[(far * 3 + side) * tiles + t] = keep(part["valid"], ref_other[2 * tall + t])
    for k, (out, ref) in enumerate(zip(z_outs, z_refs)):
        base = k * (groups * per + strips)
        y_base = k * (groups + strips)
        total = extent // HALO
        for s in range((tiles + 1) // 2):
            out[total + s] = jnp.zeros((4 * HALO, 128), F32)
        for g in range(groups):
            for r in range(per):
                out[own // HALO + g, HALO + 8 * r : HALO + 8 * r + 8, :] = ref[g * per + r]
            for part, rows, y_ref in zip(y_parts, y_rows, edge_refs):
                out[own // HALO + g, rows, :] = keep(part["valid"], y_ref[y_base + g])
        for r in range(per):
            out[place // HALO, HALO + 8 * r : HALO + 8 * r + 8, :] = z_other[base + source // HALO * per + r]
        for part, rows, y_ref in zip(y_parts, y_rows, edge_others):
            out[place // HALO, rows, :] = keep(part["valid"], y_ref[y_base + source // HALO])
        for strip in range(strips):
            for x_side in range(3):
                if x_side == 1:
                    middle = ref[groups * per + strip]
                    edges = [keep(p["valid"], r[y_base + groups + strip]) for p, r in zip(y_parts, edge_refs)]
                else:
                    here = far == x_side
                    middle = keep(here, z_other[base + groups * per + strip])
                    edges = [keep(p["valid"] & here, r[y_base + groups + strip]) for p, r in zip(y_parts, edge_others)]
                low, high = edges
                for j in range(min(8, tiles - 8 * strip)):
                    t = 8 * strip + j
                    for side, values in enumerate((low, middle, high)):
                        m = 16 * (t % 2) + x_side * 3 + side
                        out[total + t // 2, m : m + 1, :] = values[j : j + 1]


def down_kernel(mesh_shape, *refs):
    n_gx, n_gy, n_gz = mesh_shape
    gm, fw, za, zb = refs[:4]
    send, vm, gs, vs, ws, v1m, v1s, w1m, w1s, g1m, g1s, i1m, i1s = refs[4:17]
    tm, ts, um, us, small = refs[17:]
    extent, rows = fw.shape[0], fw.shape[1]
    tall, wide = extent - frame_extent(n_gx, 0), rows - 2 * HALO
    half, half_rows = extent // 2, rows // 2
    ix, own, _ = x_frame(n_gx, tall)
    groups = extent // HALO
    for ref in (gs, vm, vs, g1m, g1s, v1m, v1s):
        for x in (0, ref.shape[0] - 1):
            ref[x] = jnp.zeros(ref.shape[1:], F32)

    ends, sides = z_ends(n_gz), y_ends(n_gy, wide)

    def inside(depth, step):
        row, lane = iota((depth, 128), 0), iota((depth, 128), 1)
        edge = HALO // step
        low, high = ((e["valid"].astype(F32)) for e in sides)
        main = jnp.where(row < edge, K * low, jnp.where(row >= depth - edge, K * high, K))
        low, high = (e["valid"].astype(F32) for e in ends)
        return main, main * jnp.where(lane >= 120, low, jnp.where(lane < HALO, high, 0.0))

    def present(x, step):
        if n_gx <= 2:
            return None
        edge = HALO // step
        out = ((x < edge) & (ix == 0)) | ((x >= extent // step - edge) & (ix == n_gx - 1))
        return 1.0 - out.astype(F32)

    lane = iota((rows, 128), 1)
    halo_lanes = jnp.where(lane >= 120, ends[0]["valid"].astype(F32), 0.0) + jnp.where(lane < HALO, ends[1]["valid"].astype(F32), 0.0)
    first_half = lane % 16 < HALO

    def load(group):
        low, high = za[group], zb[group]
        both = (jnp.where(first_half, low, high), jnp.where(first_half, high, low))
        for i in range(HALO):
            x = group * HALO + i
            gs[x + 1, 8 : 8 + rows, :] = roll(both[0], 120 - 16 * i) * halo_lanes
            ws[x] = roll(both[1], 112 - 16 * i) * halo_lanes

    each(groups, load, 4)

    def smooth(g_refs, v_refs, factors, x, depth, step):
        main, side, main_n, side_n = neighbours(*g_refs, x + 1, 8, depth, step)
        here = present(x, step)
        for ref, value, near, factor in zip(v_refs, (main, side), (main_n, side_n), factors):
            ref[x + 1, 8 : 8 + depth, :] = 1.2 * value + (factor if here is None else factor * here) * near

    factors = inside(rows, 1)
    each(extent, lambda x: smooth((gm, gs), (vm, vs), factors, x, rows, 1), 24)

    src, dst = iota((256, 256), 0), iota((256, 256), 1)
    beside = (src == (dst + 1) % 256) | (dst == (src + 1) % 256)

    def residual(first):
        layers = range(4 * first, 4 * first + 4)
        inner = slice(8, 8 + rows)
        lines = [jnp.concatenate([vm[x + 1, inner, :], vs[x + 1, inner, :]], axis=1) for x in layers]
        near = select_lanes(jnp.concatenate(lines, axis=0), beside)
        for i in range(2):
            for row in range(0, rows, 8):
                totals = None
                for j in range(2):
                    x, at = 4 * first + 2 * i + j, (2 * i + j) * rows + row
                    values = []
                    for k, (v, g, w) in enumerate(((vm, gm, fw), (vs, gs, ws))):
                        around = xy_sum(v, x + 1, 8 + row, 8) + near[at : at + 8, 128 * k : 128 * k + 128]
                        here, cells = slice(8 + row, 16 + row), w[x, row : row + 8, :]
                        values += [cells * ((1.0 / K) * g[x + 1, here, :] - 6.0 * v[x + 1, here, :] + around), cells]
                    totals = values if j == 0 else [a + b for a, b in zip(totals, values)]
                for ref, value in zip((tm, um, ts, us), totals):
                    ref[2 * first + i, row : row + 8, :] = value

    for first in range(half // 2):
        residual(first)
    src, dst = iota((128, 128), 0), iota((128, 128), 1)
    pair = src // 2 == dst // 2

    def coarsen(first):
        rows_of = [
            ref[first * 4 + i, pl.ds(0, half_rows, stride=2), :] + ref[first * 4 + i, pl.ds(1, half_rows, stride=2), :]
            for i in range(4)
            for ref in (tm, um, ts, us)
        ]
        sums = select_lanes(jnp.concatenate(rows_of, axis=0), pair)
        for i in range(4):
            x = first * 4 + i
            for j, (w_out, g_out, i_out) in enumerate(((w1m, g1m, i1m), (w1s, g1s, i1s))):
                at = (4 * i + 2 * j) * half_rows
                weights = 0.0625 * sums[at + half_rows : at + 2 * half_rows]
                inverses = inverse(weights)
                w_out[x] = weights
                i_out[x] = inverses
                g_out[x + 1, 8 : 8 + half_rows, :] = (0.125 * K) * sums[at : at + half_rows] * inverses

    each(half // 4, coarsen, 4)

    factors_1 = inside(half_rows, 2)
    each(half, lambda x: smooth((g1m, g1s), (v1m, v1s), factors_1, x, half_rows, 2), 16)

    base = own // 2
    first_row = 8 + HALO // 2
    quarter, quarter_rows = tall // 4, wide // 4
    for x2 in range(quarter):
        total_r = total_w = None
        for j in range(2):
            x = base + 2 * x2 + j + 1
            main, _, main_n, _ = neighbours(v1m, v1s, x, first_row, wide // 2, 2)
            weights = w1m[x - 1, pl.ds(first_row - 8, wide // 2), :]
            res = weights * ((1.0 / K) * g1m[x, pl.ds(first_row, wide // 2), :] - 6.0 * main + main_n)
            total_r = res if j == 0 else total_r + res
            total_w = weights if j == 0 else total_w + weights
        small[0, x2] = total_r
        small[1, x2] = total_w
    q = []
    for a, factor in ((0, 0.125), (1, 0.0625)):
        for x2 in range(quarter):
            ref = small.at[a, x2]
            both = ref[pl.ds(0, quarter_rows, stride=2), :] + ref[pl.ds(1, quarter_rows, stride=2), :]
            q.append(factor * both)
    stacked = jnp.concatenate([jnp.concatenate(q[:quarter], axis=0), jnp.concatenate(q[quarter:], axis=0)], axis=0)
    src, dst = iota((128, 128), 0), iota((128, 128), 1)
    cell = 4 * (dst % 32)
    compact = select_lanes(stacked, (src == cell) | (src == cell + 2))
    block = iota((quarter_rows, 128), 1) // 32
    gz = lax.axis_index("gz")
    out = []
    for a in range(2):
        packed = jnp.zeros((quarter_rows, 128), F32)
        for x2 in range(quarter):
            r = (a * quarter + x2) * quarter_rows
            packed = jnp.where(block == lax.rem(gz + x2, 4), compact[r : r + quarter_rows], packed)
        out.append(packed)
    message = jnp.concatenate(out, axis=0)

    def copy(d):
        send[d] = message

    each(send.shape[0], copy, 8)


def up_kernel(mesh_shape, *refs):
    n_gx, n_gy, n_gz = mesh_shape
    recv, rows_ref, za, zb, gm, fw, i0, vm, _, vs, ws, v1m, v1s, w1m, w1s, g1m, g1s, i1m, i1s, out = refs[:20]
    g2, w2, i2, v2, y2, e2, p2, t3, u3, g3, w3, i3, v3, y3, p3, b4, y1m, y1s, e1m, e1s, f1m, f1s, y0m, y0s = refs[20:]
    tall, wide = out.shape[0], out.shape[1]
    size_x, size_z = w2.shape[0], w2.shape[2]
    size_y = w2.shape[1]
    ix, own, _ = x_frame(n_gx, tall)
    iy, iz = lax.axis_index("gy"), lax.axis_index("gz")
    quarter, quarter_rows = tall // 4, wide // 4
    extent = frame_extent(n_gx, tall)
    half, half_rows = w1m.shape[0], w1m.shape[1]

    def clear(ref):
        count, depth, size = ref.shape
        zero = jnp.zeros((8, size), F32)
        for x in range(count):
            ref[x, 0:8, :] = zero
            ref[x, depth - 8 : depth, :] = zero
        for x in (0, count - 1):
            ref[x] = jnp.zeros((depth, size), F32)

    for ref in (g2, v2, y2, g3, v3, y3):
        clear(ref)
    e2[...] = jnp.zeros(e2.shape, F32)
    p3[...] = jnp.zeros(p3.shape, F32)

    lane = iota((quarter_rows, 128), 1)
    block = lane // 32
    for gx in range(n_gx):
        for gy in range(n_gy):
            for x in range(quarter):
                tiles_b, tiles_w = [], []
                for tile in range(size_z // 128):
                    picked = [jnp.zeros((quarter_rows, 128), F32)] * 2
                    for j in range(4):
                        gz = tile * 4 + j
                        d = (gx * n_gy + gy) * n_gz + gz
                        mask = block == (gz + x) % 4
                        for a in range(2):
                            piece = recv[d, a * quarter_rows : (a + 1) * quarter_rows, :]
                            picked[a] = jnp.where(mask, piece, picked[a])
                    tiles_b.append(roll(picked[0], -32 * x))
                    tiles_w.append(roll(picked[1], -32 * x))
                weights = joined(tiles_w)
                inverses = 1.0 / weights
                w2[gx * quarter + x, gy * quarter_rows : (gy + 1) * quarter_rows, :] = weights
                i2[gx * quarter + x, gy * quarter_rows : (gy + 1) * quarter_rows, :] = inverses
                g2[gx * quarter + x + 1, 8 + gy * quarter_rows : 8 + (gy + 1) * quarter_rows, :] = K * joined(tiles_b) * inverses

    def smooth(g, v, x, rows, step):
        main, near = global_neighbours(g, x + 1, 8, rows, step)
        v[x + 1, 8 : 8 + rows, :] = 1.2 * main + K * near

    def resid(g, v, w, x, rows, step):
        main, near = global_neighbours(v, x + 1, 8, rows, step)
        return w[x] * ((1.0 / K) * g[x + 1, 8 : 8 + rows, :] - 6.0 * main + near)

    each(size_x, lambda x: smooth(g2, v2, x, size_y, 1), 8)
    rows3, x3 = size_y // 2, size_x // 2

    def restrict_2(x):
        for t, part in enumerate(tiled(resid(g2, v2, w2, 2 * x, size_y, 1) + resid(g2, v2, w2, 2 * x + 1, size_y, 1))):
            t3[t] = part
        for t, part in enumerate(tiled(w2[2 * x] + w2[2 * x + 1])):
            u3[t] = part
        pairs = lambda ref: lane_pairs(row_pairs(ref, size_y), 1)
        weights = 0.0625 * pairs(u3)
        inverses = 1.0 / weights
        w3[x] = weights
        i3[x] = inverses
        g3[x + 1, 8 : 8 + rows3, :] = (0.125 * K) * pairs(t3) * inverses

    each(x3, restrict_2, 4)
    each(x3, lambda x: smooth(g3, v3, x, rows3, 2), 8)
    rows4, x4 = rows3 // 2, x3 // 2

    def restrict_3(x):
        for t, part in enumerate(tiled(resid(g3, v3, w3, 2 * x, rows3, 2) + resid(g3, v3, w3, 2 * x + 1, rows3, 2))):
            t3[t, 0:rows3, :] = part
        b4[x] = 0.125 * row_pairs(t3, rows3)

    each(x4, restrict_3, 4)

    tiles = rows_ref.shape[0] // 9
    coarse_z = size_z // 4
    per = 128 // coarse_z
    src, dst = iota((size_z, 128), 0), iota((size_z, 128), 1)
    values = b4[0] if x4 == 1 else jnp.concatenate([b4[x] for x in range(x4)], axis=0)
    cell = 4 * (dst % coarse_z)
    compact = select_lanes(values, (src == cell) | (src == cell + 2))
    place = iota((x4 * rows4, 128), 0) % per == iota((x4 * rows4, 128), 1) // coarse_z
    compact = jnp.where(place, compact, 0.0)
    vectors = [jnp.sum(compact[t * per : (t + 1) * per], axis=0, keepdims=True) for t in range(tiles)]
    ends = z_ends(n_gz)
    groups = extent // HALO
    fine = iota((HALO, size_z), 1) // 4
    fine_row = fine == iz * HALO + iota((HALO, size_z), 0)
    edge_row = iota((16, 128), 0)
    first_total = [None, None]
    for k, ref in enumerate((za, zb)):
        total = None
        for t in range(tiles):
            piece = ref[groups + t // 2, 16 * (t % 2) : 16 * (t % 2) + 16, :] * vectors[t]
            total = piece if total is None else total + piece
        first_total[k] = jnp.sum(total, axis=1, keepdims=True) * ends[k]["valid"].astype(F32)
    z_lane = iota((16, size_z), 1) // 4
    spread = None
    for k in range(2):
        piece = jnp.where(z_lane == iz * HALO + ends[k]["row"], first_total[k], 0.0)
        spread = piece if spread is None else spread + piece
    for m in range(9):
        total = None
        for t in range(tiles):
            piece = rows_ref[m * tiles + t] * vectors[t]
            total = piece if total is None else total + piece
        values = jnp.sum(total, axis=1, keepdims=True)
        line = jnp.sum(jnp.where(fine_row, values, 0.0), axis=0, keepdims=True) + spread[m : m + 1, :]
        row = 8 + 2 * (iy + (m % 3 - 1))
        for t, part in enumerate(tiled(line)):
            p3[ix + m // 3, t, pl.ds(row, 1), :] = part
            p3[ix + m // 3, t, pl.ds(row + 1, 1), :] = part

    def lift(y, v, w, p, x, px, rows, row):
        coarse = joined([p[px, t, row : row + rows, :] for t in range(p.shape[1])])
        y[x + 1, 8 : 8 + rows, :] = v[x + 1, 8 : 8 + rows, :] + w[x] * coarse

    def relax(y, g, inverses, x, rows, step):
        main, near = global_neighbours(y, x + 1, 8, rows, step)
        return (0.2 * main + g[x + 1, 8 : 8 + rows, :] + K * near) * inverses[x]

    each(x3, lambda x: lift(y3, v3, w3, p3, x, x // 2 + 1, rows3, 8), 8)

    def up_3(x):
        for t, e3 in enumerate(tiled(relax(y3, g3, i3, x, rows3, 2))):
            p2[x, t, pl.ds(0, rows3, stride=2), :] = e3
            p2[x, t, pl.ds(1, rows3, stride=2), :] = e3

    each(x3, up_3, 4)
    each(size_x, lambda x: lift(y2, v2, w2, p2, x, x // 2, size_y, 0), 8)

    def up_2(x):
        for t, part in enumerate(tiled(relax(y2, g2, i2, x, size_y, 1))):
            e2[x + 2, t, 8 : 8 + size_y, :] = part

    each(size_x, up_2, 8)

    src, dst = iota((size_z, 256), 0), iota((size_z, 256), 1)
    start = iz * 32
    cell = jnp.where(dst < 128, dst // 4, jnp.where(dst < 192, 32 + (dst - 128) // 4, -1 - (255 - dst) // 4))
    widen = src == start + cell
    n2 = extent // 4
    x_start = ix * quarter - own // 4
    y_start = 8 + iy * quarter_rows - HALO // 4
    spread = None
    for t in range(size_z // 128):
        stacked = jnp.concatenate([e2[x_start + 2 + i, t, pl.ds(y_start, 8), :] for i in range(n2)], axis=0)
        part = select_lanes(stacked, widen[t * 128 : (t + 1) * 128])
        spread = part if spread is None else spread + part
    for i in range(n2):
        for ref, part in ((e1m, spread[i * 8 : i * 8 + 8, :128]), (e1s, spread[i * 8 : i * 8 + 8, 128:])):
            ref[i, pl.ds(0, 8, stride=2), :] = part
            ref[i, pl.ds(1, 8, stride=2), :] = part

    for ref in (y1m, y1s):
        for x in (0, half + 1):
            ref[x] = jnp.zeros(ref.shape[1:], F32)
    inner = slice(8, 8 + half_rows)
    for x in range(half):
        y1m[x + 1, inner, :] = v1m[x + 1, inner, :] + w1m[x] * e1m[x // 2]
        y1s[x + 1, inner, :] = v1s[x + 1, inner, :] + w1s[x] * e1s[x // 2]

    def up_1(x):
        main, side, main_n, side_n = neighbours(y1m, y1s, x + 1, 8, half_rows, 2)
        for f, y, near, g, inverses in ((f1m, main, main_n, g1m, i1m), (f1s, side, side_n, g1s, i1s)):
            e1 = (0.2 * y + g[x + 1, inner, :] + K * near) * inverses[x]
            f[x, pl.ds(0, half_rows, stride=2), :] = e1
            f[x, pl.ds(1, half_rows, stride=2), :] = e1

    each(half, up_1, 12)
    base = own // 2
    extent_rows = fw.shape[1]
    for i in range(tall + 2):
        parent = jnp.clip(base + (i + 1) // 2 - 1, 0, half - 1)
        x = own + (i - 1)
        weights = fw[jnp.clip(x, 0, extent - 1)] if i in (0, tall + 1) else fw[x]
        value = vm[x + 1, 8 : 8 + extent_rows, :] + weights * f1m[parent]
        if i in (0, tall + 1):
            value = keep((x >= 0) & (x < extent), value)
        else:
            y0s[i - 1] = (
                vs[x + 1, 8 + HALO : 8 + HALO + wide, :] + ws[x, HALO : HALO + wide, :] * f1s[parent, HALO : HALO + wide, :]
            )
        y0m[i] = value

    def up_0(i):
        main = y0m[i + 1, pl.ds(HALO, wide), :]
        main_z, _ = z_sum(main, y0s[i], 1)
        near = xy_sum(y0m, i + 1, HALO, wide) + main_z
        out[i] = (0.2 * main + gm[own + i + 1, 8 + HALO : 8 + HALO + wide, :] + K * near) * i0[i]

    each(tall, up_0, 16)


def size_of(shape):
    return 4 * math.prod(shape)


def call(kernel, outs, scratch=(), resident=True, fetch=False):
    limit = 8 * 2**20 + sum(map(size_of, scratch)) + sum(size_of(s) for s in outs if size_of(s) > 2**20)
    run = pl.pallas_call(
        kernel,
        out_shape=[(pltpu.VMEM if resident and size_of(s) <= 2**20 else jax.ShapeDtypeStruct)(s, F32) for s in outs],
        scratch_shapes=[pltpu.VMEM(s, F32) for s in scratch],
        compiler_params=pltpu.CompilerParams(vmem_limit_bytes=min(limit, 56 * 2**20)),
    )

    def place(value):
        small = size_of(value.shape) <= 2**20 and not fetch
        return pltpu.with_memory_space_constraint(value, pltpu.VMEM if small else pltpu.HBM)

    return lambda *values: run(*map(place, values))


def plain_halo(mesh_shape, own, frames):
    n_gx = mesh_shape[0]
    tall = own[0].shape[0]
    extent, tiles = frames[1][0], own[2].shape[1] // 128
    inverses = 1.0 / own[1]
    own = (K * own[0] * inverses, *own[1:])
    parts = ()
    if n_gx > 1:
        odd = lax.axis_index("gx") % 2
        for first in range(2):
            start = jnp.where(odd == first, tall - HALO, 0)
            faces = [lax.dynamic_slice_in_dim(a, start, HALO, 0) for a in own[:2]] + [own[2]]
            parts += tuple(swap(a, "gx", first) for a in faces)
    slab = (2 * extent + 3 * tiles, HALO, 128)
    y_slabs = call(functools.partial(y_pack_kernel, mesh_shape), [slab, slab])(*own, *parts)
    y_parts = [ring(s, "gy", step) for s, step in zip(y_slabs, (1, -1))]
    fb, fw, matrix, z_a, z_b = call(functools.partial(z_pack_kernel, mesh_shape), frames)(*own, *parts, *y_parts)
    return fb, fw, matrix, ring(z_a, "gz", 1), ring(z_b, "gz", -1), inverses


def shared_halo(mesh_shape, own, frames):
    tall, wide = own[0].shape[:2]
    tiles = own[2].shape[1] // 128
    strips, groups, per = (tiles + 7) // 8, tall // HALO, wide // 8
    z_shape = (groups * per + strips, HALO, 128)
    y_shape = (2 * tall + tiles, HALO, 128)
    x_shape = (2 * per * tall + tiles, HALO, 128)
    outs = [z_shape, z_shape, y_shape, y_shape, x_shape] + [a.shape for a in own] + [own[0].shape]
    z_tail, z_head, y_tail, y_head, x_own, *here, inverses = call(face_kernel, outs, fetch=True)(*own)

    z_got = (ring(z_tail, "gz", 1), ring(z_head, "gz", -1))
    y_got = (ring(y_tail, "gy", 1), ring(y_head, "gy", -1))
    other = swap(x_own, "gx", 0)
    z_got = lax.optimization_barrier(z_got)
    edge = (2 * (groups + strips), HALO, 128)
    both = (2 * z_shape[0], HALO, 128)
    edge_tail, edge_head, z_both = call(functools.partial(y_edge_kernel, groups, per), [edge, edge, both])(*z_got)
    edge_got = (ring(edge_tail, "gy", 1), ring(edge_head, "gy", -1))
    z_other = swap(z_both, "gx", 0)
    y_other = [swap(y, "gx", 0) for y in y_got]
    edge_other = [swap(y, "gx", 0) for y in edge_got]
    made = call(functools.partial(frame_kernel, mesh_shape), frames)(
        *here, other, *z_got, z_other, *y_got, *y_other, *edge_got, *edge_other
    )
    return *made, inverses


def per_device(mesh_shape, sources, stiffness, coarse_inverse):
    n_gx, n_gy, n_gz = mesh_shape
    count = n_gx * n_gy * n_gz
    tall, wide, deep = stiffness.shape
    cells = coarse_inverse.shape[1]
    assert sources.shape[0] == 1 and deep == 128 and tall == 16 and wide == 16 and n_gz % 4 == 0 and cells % 128 == 0
    tiles = cells // 128
    extent = frame_extent(n_gx, tall)
    source = sources[0]
    own = (source, stiffness, coarse_inverse)
    rows = wide + 2 * HALO
    frame, padded = (extent, rows, 128), (extent + 2, rows + 16, 128)
    z_slab = (extent // HALO + (tiles + 1) // 2, rows, 128)
    frames = [padded, frame, (9 * tiles, HALO, 128), z_slab, z_slab]
    exchange = shared_halo if n_gx == 2 else plain_halo
    gm, fw, matrix, z_a, z_b, inverses = exchange(mesh_shape, own, frames)
    half, half_rows = extent // 2, rows // 2
    level1, plain1 = (half + 2, half_rows + 16, 128), (half, half_rows, 128)
    window, face = (tall + 2, rows, 128), (tall, wide, 128)
    message = (count, wide // 2, 128)
    outs = [message, padded, padded, padded, frame] + [level1] * 2 + [plain1] * 2 + [level1] * 2 + [plain1] * 2
    scratch = [(half, rows, 128)] * 4 + [(2, tall // 4, wide // 2, 128)]
    send, *state = call(functools.partial(down_kernel, mesh_shape), outs, scratch)(gm, fw, z_a, z_b)
    recv = lax.all_to_all(send, AXES, 0, 0, tiled=True)
    size_x, size_y, size_z = n_gx * tall // 4, n_gy * wide // 4, n_gz * deep // 4
    pad2 = (size_x + 2, size_y + 16, size_z)
    x3, rows3 = size_x // 2, size_y // 2
    pad3 = (x3 + 2, rows3 + 16, size_z)
    n2, lane_tiles = extent // 4, size_z // 128
    scratch = [
        pad2, *[(size_x, size_y, size_z)] * 2, pad2, pad2, (size_x + 4, lane_tiles, size_y + 16, 128), (x3, lane_tiles, size_y, 128),
        (lane_tiles, size_y, 128), (lane_tiles, size_y, 128), pad3, *[(x3, rows3, size_z)] * 2, pad3, pad3,
        (x3 // 2 + 2, lane_tiles, rows3 + 16, 128),
        (x3 // 2, rows3 // 2, size_z), level1, level1, (n2, 16, 128), (n2, 16, 128),
        (half, rows, 128), (half, rows, 128), window, face,
    ]
    (pressure,) = call(functools.partial(up_kernel, mesh_shape), [face], scratch, False)(
        recv, matrix, z_a, z_b, gm, fw, inverses, *state
    )
    return pressure[None]


def solution(mesh):
    mesh_shape = tuple(mesh.shape[a] for a in AXES)
    in_specs = (P(None, "gx", "gy", "gz"), P("gx", "gy", "gz"), P(AXES, None))
    return jax.shard_map(
        functools.partial(per_device, mesh_shape),
        mesh=mesh,
        in_specs=in_specs,
        out_specs=P(None, "gx", "gy", "gz"),
        check_vma=False,
    )
```
